512 devices in a mesh: seq: 128 (over x, z, core), head: 4 (over y).
Axes of the slice: x: 4, y: 4, z: 16, core: 2. Of those that a mesh axis runs over, the one named last changes fastest.
Arguments:
- values_in: bfloat16 [65536, 4096], P('seq', 'head'), may hold values from -6 to 6
- gate_in: bfloat16 [65536, 4096], P('seq', 'head'), may hold values from -6 to 6
- key_proj: bfloat16 [65536, 128], P('seq'), may hold values from -0.52734375 to 0.52734375
- query_proj: bfloat16 [65536, 128], P('seq'), may hold values from -6 to 6
- step_size: float32 [65536, 64], P('seq', 'head'), may hold values from 0.5 to 2
- log_decay: float32 [65536, 64], P('seq', 'head'), may hold values from -1.2 to 0
- skip_weight: float32 [64], P('head'), may hold values from 0.5 to 1.5
- norm_gain: float32 [4096], P('head'), may hold values from 0.5 to 1.5
- level_table: float32 [16, 64, 11], P(None, 'head'), may hold values from 0.25 to 2
- level_pick: int32 [65536], P('seq'), may hold values from 0 to 15
- doc_start: int32 [1024], P('seq'), may hold values 0 or 1
Outputs:
- layer_out: bfloat16 [65536, 4096], P('seq', 'head')
The draws below stay inside these ranges and needn't reach their ends.
All inputs are finite; a program needn't handle non-finite values. No bound on the sum of `doc_start` on one device may be relied on, other than what follows from the above.
Results may differ from the reference program's by a relative error of at most 0.012.
Values may be sent and summed in bfloat16 or wider, within the bound.
A program may use at most 64 MiB of HBM per device.

```python
import math
import jax
import jax.numpy as jnp
from jax import lax

H = 64
HEADDIM = 64
DSTATE = 128
STRETCH = 64
GROUPS = 16
TOK_DEV = 512
SEQUENCE_TOKENS = 65536
NCHUNK = 1024
STRETCH_BITS = 3
SPAN_BITS = 7
LEVELS = 11


def head_rank(key):
    return jax.random.permutation(jax.random.fold_in(key, 101), H)


def class_counts():
    return (max(1, H // 16), max(1, 3 * H // 16), max(1, H // 4))


def draw_log_decay(key, part):
    parallel_sequences = jax.random.split(jax.random.fold_in(key, 7), 8)
    rank = head_rank(key)
    very_count, fast_count, medium_count = class_counts()
    very_rate = jnp.exp(jax.random.uniform(parallel_sequences[0], (H,), minval=math.log(0.5), maxval=math.log(1.0)))
    fast_rate = jnp.exp(jax.random.uniform(parallel_sequences[1], (H,), minval=math.log(0.03), maxval=math.log(0.08)))
    medium_rate = jnp.exp(jax.random.uniform(parallel_sequences[7], (H,), minval=math.log(0.006), maxval=math.log(0.012)))
    slow_rate = jnp.exp(jax.random.uniform(parallel_sequences[2], (H,), minval=math.log(0.03), maxval=math.log(0.3))) * (math.log(10.0) / SEQUENCE_TOKENS)
    head_decay_speed = jnp.where(rank < very_count, very_rate, jnp.where(rank < very_count + fast_count, fast_rate, jnp.where(rank < very_count + fast_count + medium_count, medium_rate, slow_rate)))
    interval_multiplier = jnp.exp(jax.random.uniform(parallel_sequences[3], (SEQUENCE_TOKENS // TOK_DEV, H), minval=-math.log(2.0), maxval=math.log(2.0)))
    interval_multiplier = jnp.repeat(interval_multiplier, TOK_DEV, axis=0)
    noise_multiplier = jnp.exp(jax.random.uniform(parallel_sequences[4], (SEQUENCE_TOKENS, H), minval=-math.log(2.0), maxval=math.log(2.0)))
    outlier_position = jax.random.randint(parallel_sequences[5], (3,), 0, SEQUENCE_TOKENS)
    outlier_length = jax.random.uniform(parallel_sequences[6], (3,), minval=0.22, maxval=0.69)
    element_position = jnp.arange(SEQUENCE_TOKENS, dtype=jnp.int32)
    outlier_penalty = jnp.sum(jnp.where(element_position[:, None] == outlier_position[None, :], outlier_length[None, :], 0.0), axis=1)
    decay_logarithm = -(head_decay_speed[None, :] * interval_multiplier * noise_multiplier) - outlier_penalty[:, None]
    return jnp.maximum(decay_logarithm, -1.2).astype(jnp.float32)


def draw_values_in(key, part):
    parallel_sequences = jax.random.split(jax.random.fold_in(key, 11), 1)
    rank = head_rank(key)
    very_count, fast_count, medium_count = class_counts()
    slow_head = rank >= very_count + fast_count + medium_count
    span_large = jax.random.uniform(jax.random.fold_in(key, 103), (SEQUENCE_TOKENS // TOK_DEV,)) < 0.3
    span_scale = jnp.repeat(jnp.where(span_large, 1.0, 0.02), TOK_DEV)
    head_scale = jnp.where(slow_head[None, :], 2.0 / math.sqrt(SEQUENCE_TOKENS), span_scale[:, None])
    channel_scale = jnp.repeat(head_scale, HEADDIM, axis=1)
    base = jax.random.truncated_normal(parallel_sequences[0], -6.0, 6.0, (SEQUENCE_TOKENS, H * HEADDIM))
    return (base * channel_scale).astype(jnp.bfloat16)


def set_ends(values, key, low, largest):
    index_at = [jax.random.randint(jax.random.fold_in(key, axis), (), 0, length) for axis, length in enumerate(values.shape)]
    longest = values.shape.index(max(values.shape))
    next_to = index_at[:longest] + [(index_at[longest] + 1) % values.shape[longest]] + index_at[longest + 1:]
    return values.at[tuple(index_at)].set(low).at[tuple(next_to)].set(largest)


def levels(key, dims, shards, smallest, top_value):
    factor_of, own = 1.0, jax.random.fold_in(key, 6)
    for dim, blocks in shards:
        steps = jnp.exp(jax.random.uniform(jax.random.fold_in(own, dim), (blocks,), jnp.float32, smallest / len(shards), top_value / len(shards)))
        factor_of = factor_of * jnp.repeat(steps, dims[dim] // blocks).reshape([-1 if axis == dim else 1 for axis in range(len(dims))])
    return factor_of


def noise(stream_key, extent, scale, limit, pieces=(), kind=jnp.bfloat16):
    drawn = scale * jax.random.normal(stream_key, extent, jnp.float32)
    if pieces:
        drawn = drawn * levels(stream_key, extent, pieces, -0.22, 0.18)
    return jnp.clip(drawn, -limit, limit).astype(kind)


def setup_inputs(seed: int = 0) -> dict:
    streams_of = jax.random.split(jax.random.key(seed), 12)
    values_in = draw_values_in(jax.random.fold_in(streams_of[11], 71), 0)
    gate_in = noise(streams_of[1], (SEQUENCE_TOKENS, H * HEADDIM), 1.0, 6.0, ((0, 128), (1, 4)))
    key_proj = noise(streams_of[2], (SEQUENCE_TOKENS, DSTATE), 0.088, 0.52734375, ((0, 128),))
    query_proj = noise(streams_of[3], (SEQUENCE_TOKENS, DSTATE), 1.0, 6.0, ((0, 128),))
    step_size = jnp.clip(jnp.exp(math.log(2.0) - 1.3862944 * jax.random.uniform(streams_of[4], (SEQUENCE_TOKENS, H), jnp.float32) ** levels(streams_of[4], (SEQUENCE_TOKENS, H), ((0, 128), (1, 4)), -0.2, 0.2)), 0.5, 2.0)
    log_decay = draw_log_decay(jax.random.fold_in(streams_of[11], 71), 0)
    skip_weight = jnp.clip(0.5 + 1.0 * jax.random.uniform(streams_of[6], (H,), jnp.float32) ** levels(streams_of[6], (H,), ((0, 4),), -0.2, 0.2), 0.5, 1.5)
    norm_gain = jnp.clip(1.0 + 0.1 * jax.random.normal(streams_of[7], (H * HEADDIM,), jnp.float32), 0.5, 1.5)
    level_table = jnp.clip(jnp.exp(math.log(2.0) - 2.0794415 * jax.random.uniform(streams_of[8], (GROUPS, H, LEVELS), jnp.float32) ** levels(streams_of[8], (GROUPS, H, LEVELS), ((1, 4),), -0.2, 0.2)), 0.25, 2.0)
    level_pick = set_ends(jax.random.randint(streams_of[9], (SEQUENCE_TOKENS,), 0, GROUPS), jax.random.fold_in(streams_of[9], 1), 0, GROUPS - 1).astype(jnp.int32)
    doc_start = set_ends((jax.random.randint(streams_of[10], (NCHUNK,), 0, NCHUNK) < 2).astype(jnp.int32), jax.random.fold_in(streams_of[10], 1), 0, 1)
    return {"values_in": values_in, "gate_in": gate_in, "key_proj": key_proj, "query_proj": query_proj, "step_size": step_size, "log_decay": log_decay, "skip_weight": skip_weight, "norm_gain": norm_gain, "level_table": level_table, "level_pick": level_pick, "doc_start": doc_start}


epsilon = 1e-06

def level_of_pairs(row_count, stretch_len, low_bits):
    blocks = jnp.arange(row_count, dtype=jnp.int32) // stretch_len
    differ = jnp.bitwise_xor(blocks[:, None], blocks[None, :])
    level_index = jnp.zeros((row_count, row_count), jnp.int32)
    for bit_index in range(low_bits):
        level_index = level_index + (differ >= 1 << bit_index).astype(jnp.int32)
    return level_index

def reference(values_in, gate_in, key_proj, query_proj, step_size, log_decay, skip_weight, norm_gain, level_table, level_pick, doc_start):
    span_count = SEQUENCE_TOKENS // TOK_DEV
    per_span = TOK_DEV // STRETCH
    level_index = level_of_pairs(TOK_DEV, STRETCH, STRETCH_BITS)
    element_position = jnp.arange(TOK_DEV, dtype=jnp.int32)
    causal = element_position[:, None] >= element_position[None, :]
    level_weight = level_table[level_pick]
    bit_range = jnp.arange(SPAN_BITS, dtype=jnp.int32)

    def one_span(level_state, inputs):
        span_index, span_values, span_gate, span_keys, span_query, span_step, span_decay_log, span_weight, span_starts = inputs
        log_total = jnp.cumsum(span_decay_log, axis=0)
        doc_stretch = jnp.cumsum(span_starts)
        doc_count = jnp.broadcast_to(doc_stretch[:, None], (per_span, STRETCH)).reshape(TOK_DEV)
        visible = causal & (doc_count[:, None] == doc_count[None, :])
        select = jnp.zeros((H, TOK_DEV, TOK_DEV), jnp.float32)
        for level_id in range(STRETCH_BITS + 1):
            select = select + jnp.where(level_index[None] == level_id, jnp.transpose(span_weight[:, :, level_id])[:, :, None], 0.0)
        total_t = jnp.transpose(log_total)
        log_gap = jnp.where(visible[None], total_t[:, :, None] - total_t[:, None, :], -jnp.inf)
        scores = jnp.dot(span_query, span_keys.T, preferred_element_type=jnp.float32)
        mixing = (scores[None] * select * jnp.exp(log_gap)).astype(jnp.bfloat16)
        scaled_in = (span_step[:, :, None] * span_values.astype(jnp.float32)).astype(jnp.bfloat16)
        local_part = jnp.einsum('hts,shp->thp', mixing.astype(jnp.float32), scaled_in.astype(jnp.float32))
        remote_state = level_state.astype(jnp.bfloat16)
        reach_decay = jnp.exp(log_total) * (doc_count == 0).astype(jnp.float32)[:, None]
        projected = jnp.einsum('tn,bhpn->tbhp', span_query.astype(jnp.float32), remote_state.astype(jnp.float32))
        remote_weight = span_weight[:, :, 1 + STRETCH_BITS:1 + STRETCH_BITS + SPAN_BITS]
        remote_part = reach_decay[:, :, None] * jnp.einsum('thb,tbhp->thp', remote_weight, projected)
        combined = local_part + remote_part + skip_weight[None, :, None] * span_values.astype(jnp.float32)
        gated_out = combined * jax.nn.silu(span_gate.astype(jnp.float32))
        mean_square = lax.optimization_barrier(jnp.mean(gated_out * gated_out, axis=(1, 2), keepdims=True))
        result = (gated_out * lax.rsqrt(mean_square + epsilon) * norm_gain.reshape(H, HEADDIM)[None]).astype(jnp.bfloat16)
        end_log = log_total[TOK_DEV - 1]
        tail_decay = jnp.exp(end_log[None, :] - log_total) * (doc_count == doc_count[TOK_DEV - 1]).astype(jnp.float32)[:, None]
        carried_in = (tail_decay[:, :, None] * scaled_in.astype(jnp.float32)).astype(jnp.bfloat16)
        end_state = jnp.einsum('sn,shp->hpn', span_keys.astype(jnp.float32), carried_in.astype(jnp.float32))
        span_decay = jnp.exp(end_log) * (doc_count[TOK_DEV - 1] == 0).astype(jnp.float32)
        next_index = span_index + 1
        lowest = jnp.bitwise_and(next_index, -next_index)
        target = jnp.sum((jnp.left_shift(jnp.ones_like(bit_range), bit_range) < lowest).astype(jnp.int32))
        below_mask = (bit_range < target).astype(jnp.float32)[:, None, None, None]
        equal_mask = (bit_range == target).astype(jnp.float32)[:, None, None, None]
        above_mask = (bit_range > target).astype(jnp.float32)[:, None, None, None]
        decayed = span_decay[None, :, None, None] * level_state
        merged = lax.optimization_barrier(jnp.sum(below_mask * decayed, axis=0, keepdims=True)) + end_state[None]
        return (above_mask * decayed + equal_mask * merged, result)
    inputs = (jnp.arange(span_count, dtype=jnp.int32), values_in.reshape(span_count, TOK_DEV, H, HEADDIM), gate_in.reshape(span_count, TOK_DEV, H, HEADDIM), key_proj.reshape(span_count, TOK_DEV, DSTATE), query_proj.reshape(span_count, TOK_DEV, DSTATE), step_size.reshape(span_count, TOK_DEV, H), log_decay.reshape(span_count, TOK_DEV, H), level_weight.reshape(span_count, TOK_DEV, H, LEVELS), doc_start.reshape(span_count, per_span))
    start_state = jnp.zeros((SPAN_BITS, H, HEADDIM, DSTATE), jnp.float32)
    final_state, outputs = lax.scan(one_span, start_state, inputs)
    return outputs.reshape(SEQUENCE_TOKENS, H * HEADDIM)
```

```python
import functools
import math

import jax
import jax.numpy as jnp
from jax import lax
from jax.experimental import pallas as pl
from jax.experimental.pallas import tpu as pltpu
from jax.sharding import Mesh
from jax.sharding import PartitionSpec as P

H = 64
HEADDIM = 64
STRETCH = 64
SEQ = ("seq_0", "seq_1", "seq_2")


epsilon = 1e-06


def copy_for_each(array, axis):
    size = lax.axis_size(axis)
    return lax.all_to_all(
        jnp.broadcast_to(array[None], (size, *array.shape)), axis, 0, 0, tiled=True
    )


def over_copies(array, axis):
    everything = copy_for_each(array, axis)
    return jnp.sum(everything, axis=0)


def level_of_pairs(row_count, stretch_len, low_bits):
    blocks = jnp.arange(row_count, dtype=jnp.int32) // stretch_len
    differ = jnp.bitwise_xor(blocks[:, None], blocks[None, :])
    level_index = jnp.zeros((row_count, row_count), jnp.int32)
    for bit_index in range(low_bits):
        level_index = level_index + (differ >= 1 << bit_index).astype(jnp.int32)
    return level_index


MESH_ID = pl.DeviceIdType.MESH
SHARD = 32


def remote(src, dst, send, recv, where):
    return pltpu.make_async_remote_copy(
        src_ref=src, dst_ref=dst, send_sem=send, recv_sem=recv, device_id=where, device_id_type=MESH_ID
    )


def wait_bytes(ref, sem):
    pltpu.make_async_copy(ref, ref, sem).wait()


def lane_pick(rows, lane):
    lanes = lax.broadcasted_iota(jnp.int32, rows.shape, 1)
    return jnp.sum(jnp.where(lanes == lane, rows, 0.0), axis=1, keepdims=True)


def levels_base(size, bits):
    base, at = [], 0
    for j in range(bits):
        base.append(at)
        at += size >> (j + 1)
    return base, at


def exchange_kernel(
    nx, nz, e_ref, d_ref, rs_out, lead_out,
    pe, pd, a_half, dc, inz, dz, outz, drow, xr, dxr, outx, rs,
    pair_s, pair_r, z_s, z_r, x_s, x_r, lev_s, lev_r, fin_s, fin_r,
):
    bz, bx = nz.bit_length() - 1, nx.bit_length() - 1
    base_z, total_z = levels_base(nz, bz)
    base_x, _ = levels_base(nx, bx)
    my_x, my_z, my_c = lax.axis_index("seq_0"), lax.axis_index("seq_1"), lax.axis_index("seq_2")
    other = 1 - my_c
    half_heads = nz * SHARD // 64

    barrier = pltpu.get_barrier_semaphore()

    def greet_z(o, c):
        pl.semaphore_signal(barrier, inc=1, device_id={"seq_1": lax.rem(my_z + o, nz)}, device_id_type=MESH_ID)
        return c

    def greet_x(o, c):
        pl.semaphore_signal(barrier, inc=1, device_id={"seq_0": lax.rem(my_x + o, nx)}, device_id_type=MESH_ID)
        return c

    pl.semaphore_signal(barrier, inc=1, device_id={"seq_2": other}, device_id_type=MESH_ID)
    lax.fori_loop(1, nx, greet_x, 0)
    lax.fori_loop(1, nz, greet_z, 0)
    pl.semaphore_wait(barrier, nz + nx - 1)

    ce = remote(e_ref, pe, pair_s.at[0], pair_r.at[0], {"seq_2": other})
    cd = remote(d_ref, pd, pair_s.at[1], pair_r.at[1], {"seq_2": other})
    ce.start()
    cd.start()
    cd.wait()
    ce.wait()
    first = my_c == 0
    d_own, d_oth = d_ref[...], pd[...]
    d0 = jnp.where(first, d_own, d_oth)
    d1 = jnp.where(first, d_oth, d_own)
    dc[...] = d0 * d1
    for s in range(nz):
        own = e_ref[my_c, s].astype(jnp.float32)
        oth = pe[my_c, s].astype(jnp.float32)
        e0 = jnp.where(first, own, oth)
        e1 = jnp.where(first, oth, own)
        scale = lane_pick(d1, my_c * half_heads + s * SHARD // 64)
        a_half[s] = (e1 + scale * e0).astype(jnp.bfloat16)

    def send_z(o, c):
        to = lax.rem(my_z + o, nz)
        remote(a_half.at[to], inz.at[my_z], z_s.at[0], z_r.at[0], {"seq_1": to}).start()
        remote(dc, dz.at[my_z], z_s.at[1], z_r.at[1], {"seq_1": to}).start()
        return c

    lax.fori_loop(1, nz, send_z, 0)
    inz[my_z] = a_half[my_z]
    dz[my_z] = dc[...]
    wait_bytes(dz.at[pl.ds(0, nz - 1)], z_r.at[1])
    wait_bytes(inz.at[pl.ds(0, nz - 1)], z_r.at[0])

    my_head = my_c * half_heads + my_z * SHARD // 64
    rows_d = [dz[z] for z in range(nz)]
    state = [inz[z].astype(jnp.float32) for z in range(nz)]
    decay = [lane_pick(r, my_head) for r in rows_d]
    for j in range(bz):
        for m in range(0, nz >> j, 2):
            outz[base_z[j] + m // 2] = state[m].astype(jnp.bfloat16)
        state = [state[m + 1] + decay[m + 1] * state[m] for m in range(0, nz >> j, 2)]
        decay = [decay[m + 1] * decay[m] for m in range(0, nz >> j, 2)]
    outz[total_z] = state[0].astype(jnp.bfloat16)
    row_product = rows_d[0]
    for z in range(1, nz):
        row_product = row_product * rows_d[z]
    drow[...] = row_product

    def send_x(o, c):
        to = lax.rem(my_x + o, nx)
        remote(outz.at[total_z], xr.at[my_x], x_s.at[0], x_r.at[0], {"seq_0": to}).start()
        remote(drow, dxr.at[my_x], x_s.at[1], x_r.at[1], {"seq_0": to}).start()
        return c

    lax.fori_loop(1, nx, send_x, 0)
    xr[my_x] = outz[total_z]
    dxr[my_x] = drow[...]

    def bit(value, j):
        return lax.rem(value // (1 << j), 2) == 1

    def send_levels_z(o, c):
        to = lax.rem(my_z + o, nz)
        for j in range(bz):
            @pl.when(bit(to, j))
            def _():
                remote(
                    outz.at[base_z[j] + to // (1 << (j + 1))], rs.at[j, my_c, my_z], lev_s.at[j], lev_r.at[j], {"seq_1": to}
                ).start()
        return c

    lax.fori_loop(1, nz, send_levels_z, 0)
    for j in range(bz):
        @pl.when(bit(my_z, j))
        def _():
            rs[j, my_c, my_z] = outz[base_z[j] + my_z // (1 << (j + 1))]

    wait_bytes(dxr.at[pl.ds(0, nx - 1)], x_r.at[1])
    wait_bytes(xr.at[pl.ds(0, nx - 1)], x_r.at[0])
    rows_x = [dxr[x] for x in range(nx)]
    state = [xr[x].astype(jnp.float32) for x in range(nx)]
    decay = [lane_pick(r, my_head) for r in rows_x]
    for j in range(bx):
        for m in range(0, nx >> j, 2):
            outx[base_x[j] + m // 2] = state[m].astype(jnp.bfloat16)
        state = [state[m + 1] + decay[m + 1] * state[m] for m in range(0, nx >> j, 2)]
        decay = [decay[m + 1] * decay[m] for m in range(0, nx >> j, 2)]
    for j in range(bx):
        @pl.when(bit(my_x, j))
        def _():
            at = base_x[j] + my_x // (1 << (j + 1))

            def send_levels_x(o, c):
                to = lax.rem(my_z + o, nz)
                remote(outx.at[at], rs.at[bz + j, my_c, my_z], lev_s.at[bz + j], lev_r.at[bz + j], {"seq_1": to}).start()
                return c

            lax.fori_loop(1, nz, send_levels_x, 0)
            rs[bz + j, my_c, my_z] = outx[at]

    one = jnp.ones_like(d0)
    mine = jnp.where(first, one, d0)
    lead_out[0] = one
    for j in range(bz):
        low = my_z // (1 << j) * (1 << j)
        product = mine
        for z in range(nz):
            product = product * jnp.where((z >= low) & (z < my_z), rows_d[z], one)
        lead_out[1 + j] = product
    row_lead = mine
    for z in range(nz):
        row_lead = row_lead * jnp.where(z < my_z, rows_d[z], one)
    for j in range(bx):
        low = my_x // (1 << j) * (1 << j)
        product = row_lead
        for x in range(nx):
            product = product * jnp.where((x >= low) & (x < my_x), rows_x[x], one)
        lead_out[1 + bz + j] = product

    flags = [bit(my_z, j) for j in range(bz)] + [bit(my_x, j) for j in range(bx)]
    for v, flag in enumerate(flags):
        @pl.when(flag)
        def _():
            wait_bytes(rs.at[v, 0, pl.ds(0, nz - 1)], lev_r.at[v])
            remote(rs.at[v, my_c], rs.at[v, my_c], fin_s.at[v], fin_r.at[v], {"seq_2": other}).start()

    @pl.when(first)
    def _():
        rs_out[0] = jnp.zeros_like(rs_out[0])

    @pl.when(jnp.logical_not(first))
    def _():
        rs_out[0] = pe[...]

    for v, flag in enumerate(flags):
        @pl.when(flag)
        def _():
            remote(rs.at[v, my_c], rs.at[v, other], fin_s.at[v], fin_r.at[v], {"seq_2": other}).wait()
            rs_out[1 + v] = rs[v]

        @pl.when(jnp.logical_not(flag))
        def _():
            rs_out[1 + v] = jnp.zeros_like(rs[v])

    wait_bytes(a_half.at[pl.ds(0, nz - 1)], z_s.at[0])
    wait_bytes(dz.at[pl.ds(0, nz - 1)], z_s.at[1])
    wait_bytes(xr.at[pl.ds(0, nx - 1)], x_s.at[0])
    wait_bytes(dxr.at[pl.ds(0, nx - 1)], x_s.at[1])
    for j in range(bz):
        @pl.when(bit(my_z, j))
        def _():
            if nz // 2 > 1:
                wait_bytes(inz.at[pl.ds(0, nz // 2 - 1)], lev_s.at[j])

        @pl.when(jnp.logical_not(bit(my_z, j)))
        def _():
            wait_bytes(inz.at[pl.ds(0, nz // 2)], lev_s.at[j])
    for j in range(bx):
        @pl.when(bit(my_x, j))
        def _():
            wait_bytes(inz.at[pl.ds(0, nz - 1)], lev_s.at[bz + j])


def exchange(end_state, span_decay, nx, nz):
    rows, width = end_state.shape
    heads = span_decay.shape[0]
    levels = nz.bit_length() - 1 + nx.bit_length() - 1
    vmem = pl.BlockSpec(memory_space=pltpu.VMEM)
    bf, f32 = jnp.bfloat16, jnp.float32
    dma = pltpu.SemaphoreType.DMA
    states, leads = pl.pallas_call(
        functools.partial(exchange_kernel, nx, nz),
        name="exchange",
        out_shape=(
            jax.ShapeDtypeStruct((1 + levels, 2, nz, SHARD, width), bf),
            jax.ShapeDtypeStruct((1 + levels, 1, 128), f32),
        ),
        in_specs=[vmem, vmem],
        out_specs=(vmem, vmem),
        scratch_shapes=[
            pltpu.VMEM((2, nz, SHARD, width), bf),
            pltpu.VMEM((1, 128), f32),
            pltpu.VMEM((nz, SHARD, width), bf),
            pltpu.VMEM((1, 128), f32),
            pltpu.VMEM((nz, SHARD, width), bf),
            pltpu.VMEM((nz, 1, 128), f32),
            pltpu.VMEM((nz, SHARD, width), bf),
            pltpu.VMEM((1, 128), f32),
            pltpu.VMEM((nx, SHARD, width), bf),
            pltpu.VMEM((nx, 1, 128), f32),
            pltpu.VMEM((nx, SHARD, width), bf),
            pltpu.VMEM((levels, 2, nz, SHARD, width), bf),
            dma((2,)), dma((2,)), dma((2,)), dma((2,)), dma((2,)), dma((2,)),
            dma((levels,)), dma((levels,)), dma((levels,)), dma((levels,)),
        ],
        compiler_params=pltpu.CompilerParams(collective_id=0, has_side_effects=True, vmem_limit_bytes=48 << 20),
    )(end_state.reshape(2, nz, SHARD, width), jnp.pad(span_decay[None, :], ((0, 0), (0, 128 - heads))))
    return states.reshape(1 + levels, rows, width), leads[:, 0, :heads]


def local(
    values_in,
    gate_in,
    key_proj,
    query_proj,
    step_size,
    log_decay,
    skip_weight,
    norm_gain,
    level_table,
    level_pick,
    doc_start,
):
    tok_rows = values_in.shape[0]
    head_count = step_size.shape[1]
    head_width = HEADDIM
    state_width = key_proj.shape[1]
    per_span = doc_start.shape[0]
    low_bits = per_span.bit_length() - 1
    span_bits = lax.axis_size(SEQ).bit_length() - 1
    table_rows = level_table.shape[0]
    level_count = level_table.shape[2]
    one_hot = (level_pick[:, None] == jnp.arange(table_rows, dtype=jnp.int32)[None, :]).astype(
        jnp.float32
    )
    level_weight = jnp.dot(
        one_hot,
        level_table.reshape(table_rows, head_count * level_count),
        precision=lax.Precision.HIGHEST,
        preferred_element_type=jnp.float32,
    ).reshape(tok_rows, head_count, level_count)
    log_total = jnp.cumsum(log_decay, axis=0)
    doc_stretch = jnp.cumsum(doc_start)
    doc_count = jnp.broadcast_to(doc_stretch[:, None], (per_span, STRETCH)).reshape(tok_rows)
    scaled_in = (jnp.repeat(step_size, head_width, axis=1) * values_in.astype(jnp.float32)).astype(
        jnp.bfloat16
    )
    end_log = log_total[tok_rows - 1]
    tail_decay = (
        jnp.exp(end_log[None, :] - log_total)
        * (doc_count == doc_count[tok_rows - 1]).astype(jnp.float32)[:, None]
    )
    carried_in = (
        jnp.repeat(tail_decay, head_width, axis=1) * scaled_in.astype(jnp.float32)
    ).astype(jnp.bfloat16)
    end_state = jnp.einsum("sc,sn->cn", carried_in, key_proj, preferred_element_type=jnp.float32)
    span_decay = jnp.exp(end_log) * (doc_count[tok_rows - 1] == 0).astype(jnp.float32)
    states, leads = exchange(
        end_state.astype(jnp.bfloat16), span_decay, lax.axis_size("seq_0"), lax.axis_size("seq_1")
    )
    remote_state = states.reshape(span_bits, head_count, head_width, state_width)
    level_index = level_of_pairs(tok_rows, STRETCH, low_bits)
    element_position = jnp.arange(tok_rows, dtype=jnp.int32)
    visible = (element_position[:, None] >= element_position[None, :]) & (
        doc_count[:, None] == doc_count[None, :]
    )
    scores = jnp.einsum("tn,sn->ts", query_proj, key_proj, preferred_element_type=jnp.float32)
    level_weight = jnp.concatenate(
        [level_weight[:, :, : 1 + low_bits], level_weight[:, :, 1 + low_bits :] * leads.T[None]], axis=2
    )
    reach_decay = jnp.exp(log_total) * (doc_count == 0).astype(jnp.float32)[:, None]
    group_size = math.gcd(head_count, 4)
    group_count = head_count // group_size

    def head_group(inputs):
        group_log, group_weight, group_scaled, group_remote, group_reach = inputs
        select = jnp.zeros((group_size, tok_rows, tok_rows), jnp.float32)
        for level_id in range(low_bits + 1):
            select = select + jnp.where(
                level_index[None] == level_id,
                jnp.transpose(group_weight[:, :, level_id])[:, :, None],
                0.0,
            )
        log_rows = jnp.transpose(group_log)
        log_gap = jnp.where(visible[None], log_rows[:, :, None] - log_rows[:, None, :], -jnp.inf)
        mixing = (scores[None] * select * jnp.exp(log_gap)).astype(jnp.bfloat16)
        local_part = jnp.einsum(
            "hts,shp->thp",
            mixing,
            group_scaled.reshape(tok_rows, group_size, head_width),
            preferred_element_type=jnp.float32,
        )
        projected = jnp.einsum(
            "tn,bhpn->tbhp", query_proj, group_remote, preferred_element_type=jnp.float32
        )
        remote_weight = group_weight[:, :, 1 + low_bits : 1 + low_bits + span_bits]
        remote_part = group_reach[:, :, None] * jnp.einsum(
            "thb,tbhp->thp", remote_weight, projected, precision=lax.Precision.HIGHEST
        )
        return (local_part + remote_part).reshape(tok_rows, group_size * head_width)

    stacked = (
        log_total.reshape(tok_rows, group_count, group_size).transpose(1, 0, 2),
        level_weight.reshape(tok_rows, group_count, group_size, level_count).transpose(1, 0, 2, 3),
        scaled_in.reshape(tok_rows, group_count, group_size * head_width).transpose(1, 0, 2),
        remote_state.reshape(span_bits, group_count, group_size, head_width, state_width).transpose(
            1, 0, 2, 3, 4
        ),
        reach_decay.reshape(tok_rows, group_count, group_size).transpose(1, 0, 2),
    )
    group_parts = lax.map(head_group, stacked)
    both_parts = group_parts.transpose(1, 0, 2).reshape(tok_rows, head_count * head_width)
    combined = both_parts + jnp.repeat(skip_weight, head_width)[None, :] * values_in.astype(
        jnp.float32
    )
    gated_out = combined * jax.nn.silu(gate_in.astype(jnp.float32))
    square_sum = over_copies(jnp.sum(gated_out * gated_out, axis=1), "head")
    mean_square = square_sum / (H * HEADDIM)
    return (gated_out * lax.rsqrt(mean_square + epsilon)[:, None] * norm_gain[None, :]).astype(
        jnp.bfloat16
    )


def solution(mesh):
    split = Mesh(
        mesh.devices.reshape(4, 16, 2, mesh.shape["head"]), ("seq_0", "seq_1", "seq_2", "head")
    )
    placed = (
        P(SEQ, "head"),
        P(SEQ, "head"),
        P(SEQ, None),
        P(SEQ, None),
        P(SEQ, "head"),
        P(SEQ, "head"),
        P("head"),
        P("head"),
        P(None, "head", None),
        P(SEQ),
        P(SEQ),
    )
    return jax.shard_map(
        local, mesh=split, in_specs=placed, out_specs=P(SEQ, "head"), check_vma=False
    )
```

```python
import functools

import jax
import jax.numpy as jnp
from jax import lax
from jax.experimental import pallas as pl
from jax.experimental.pallas import tpu as pltpu
from jax.sharding import Mesh
from jax.sharding import PartitionSpec as P

HEADDIM = 64
STRETCH = 64
BLOCK = 256
SEQ = ("seq_0", "seq_1", "seq_2")
epsilon = 1e-06

MESH_ID = pl.DeviceIdType.MESH
SHARD = 32


def remote(src, dst, send, recv, where):
    return pltpu.make_async_remote_copy(
        src_ref=src, dst_ref=dst, send_sem=send, recv_sem=recv, device_id=where, device_id_type=MESH_ID
    )


def wait_bytes(ref, sem):
    pltpu.make_async_copy(ref, ref, sem).wait()


def lane_pick(rows, lane):
    lanes = lax.broadcasted_iota(jnp.int32, rows.shape, 1)
    return jnp.sum(jnp.where(lanes == lane, rows, 0.0), axis=1, keepdims=True)


def levels_base(size, bits):
    base, at = [], 0
    for j in range(bits):
        base.append(at)
        at += size >> (j + 1)
    return base, at


def bit(value, j):
    return lax.rem(value // (1 << j), 2) == 1


def nt_dot(a, b):
    return lax.dot_general(a, b, (((1,), (1,)), ((), ())), preferred_element_type=jnp.float32)


def layer_kernel(
    nx, nz, ny, val_hbm, gate_hbm, key_ref, query_ref, step_ref, log_ref, table_ref, pick_ref, doc_ref, skip_ref,
    gated_out, square_out,
    val_v, gate_v, val_t, scaled_t, var0, var1, var2, var3, rhs, acc_t, silu_t, steps, cuts, rows_s, rows_t,
    e_buf, d_buf, pe, pd, a_half, dc, inz, dz, outz, drow, xr, dxr, outx, rs, sq_own, sq,
    load_s, pair_s, pair_r, z_s, z_r, x_s, x_r, lev_s, lev_r, two_s, two_r, fin_s, fin_r, y_s, y_r,
):
    f32, bf = jnp.float32, jnp.bfloat16
    tok, ch = val_v.shape
    heads = ch // HEADDIM
    per_span = tok // STRETCH
    low_bits = per_span.bit_length() - 1
    bz, bx = nz.bit_length() - 1, nx.bit_length() - 1
    quads = nz // 4
    base_z, total_z = levels_base(nz, bz)
    base_x, _ = levels_base(nx, bx)
    my_x, my_z, my_c = lax.axis_index("seq_0"), lax.axis_index("seq_1"), lax.axis_index("seq_2")
    my_y = lax.axis_index("head")
    other = 1 - my_c
    half_heads = heads // 2

    def place(z):
        return lax.rem(z, 4) * quads + z // 4

    barrier = pltpu.get_barrier_semaphore()

    def greet(axis, mine, size):
        def step(o, c):
            pl.semaphore_signal(barrier, inc=1, device_id={axis: lax.rem(mine + o, size)}, device_id_type=MESH_ID)
            return c

        lax.fori_loop(1, size, step, 0)

    greet("seq_1", my_z, nz)
    greet("seq_0", my_x, nx)
    greet("head", my_y, ny)
    pl.semaphore_signal(barrier, inc=1, device_id={"seq_2": other}, device_id_type=MESH_ID)

    load_v = pltpu.make_async_copy(val_hbm, val_v, load_s.at[0])
    load_g = pltpu.make_async_copy(gate_hbm, gate_v, load_s.at[1])
    load_v.start()
    load_g.start()

    total = log_ref[...].T
    lane = lax.broadcasted_iota(jnp.int32, (heads, tok), 1)
    shift = 1
    while shift < tok:
        total = total + jnp.where(lane >= shift, pltpu.roll(total, shift, 1), 0.0)
        shift *= 2
    steps[...] = step_ref[...].T
    cuts[...] = total
    lane1 = lax.broadcasted_iota(jnp.int32, (1, tok), 1)
    count = doc_ref[0]
    docs = jnp.broadcast_to(count, (1, tok))
    for c in range(1, per_span):
        count = count + doc_ref[c]
        docs = jnp.where(lane1 >= c * STRETCH, count, docs)
    last = tok - 1
    end_log = total[:, last:]
    rows_s[0] = jnp.exp(end_log - total) * (docs == docs[:, last:]).astype(f32)
    square_mask = lax.broadcasted_iota(jnp.int32, (heads, 128), 0) == lax.broadcasted_iota(jnp.int32, (heads, 128), 1)
    end_decay = jnp.exp(end_log) * (docs[:, last:] == 0).astype(f32)
    d_buf[...] = jnp.sum(jnp.where(square_mask, end_decay, 0.0), axis=0, keepdims=True)

    load_v.wait()

    def end_pair(k, c):
        at = pl.multiple_of(k * 128, 128)
        v = val_v[:, pl.ds(at, 128)].astype(f32).T
        val_t[pl.ds(at, 128), :] = v.astype(bf)
        for i in range(2):
            h = 2 * k + i
            row = pl.ds(pl.multiple_of(h * HEADDIM, HEADDIM), HEADDIM)
            scaled = (v[i * HEADDIM : (i + 1) * HEADDIM] * steps[pl.ds(h, 1), :]).astype(bf)
            scaled_t[row, :] = scaled
            var0[row, :] = (scaled.astype(f32) * rows_s[0, pl.ds(h, 1), :]).astype(bf)
        return c

    lax.fori_loop(0, heads // 2, end_pair, 0)
    per = SHARD

    def end_dot(m, c):
        n = BLOCK // per
        part = jnp.dot(
            var0[pl.ds(pl.multiple_of(m * BLOCK, BLOCK), BLOCK), :], key_ref[...], preferred_element_type=f32
        ).astype(bf)
        for i in range(n):
            e_buf[m * n + i] = part[i * per : (i + 1) * per]
        return c

    lax.fori_loop(0, ch // BLOCK, end_dot, 0)

    pl.semaphore_wait(barrier, nz + nx + ny - 2)

    ce = remote(e_buf, pe, pair_s.at[0], pair_r.at[0], {"seq_2": other})
    cd = remote(d_buf, pd, pair_s.at[1], pair_r.at[1], {"seq_2": other})
    ce.start()
    cd.start()

    picks = jnp.broadcast_to(pick_ref[...], (heads, tok))
    levels = table_ref.shape[2]
    groups = table_ref.shape[0]
    for v in range(levels):
        w = jnp.zeros((heads, tok), f32)
        for g in range(groups):
            w = jnp.where(picks == g, table_ref[g, :, v : v + 1], w)
        rows_t[v] = w

    cd.wait()
    ce.wait()
    first = my_c == 0
    d_own, d_oth = d_buf[...], pd[...]
    d0 = jnp.where(first, d_own, d_oth)
    d1 = jnp.where(first, d_oth, d_own)
    dc[...] = d0 * d1

    def merge_pair(s, c):
        own = e_buf[my_c * nz + s].astype(f32)
        oth = pe[my_c * nz + s].astype(f32)
        e0 = jnp.where(first, own, oth)
        e1 = jnp.where(first, oth, own)
        scale = lane_pick(d1, my_c * half_heads + s * SHARD // HEADDIM)
        a_half[s] = (e1 + scale * e0).astype(bf)
        return c

    for s in range(nz):
        merge_pair(s, 0)

    def send_z(o, c):
        to = lax.rem(my_z + o, nz)
        remote(a_half.at[place(to)], inz.at[my_z], z_s.at[0], z_r.at[0], {"seq_1": to}).start()
        remote(dc, dz.at[my_z], z_s.at[1], z_r.at[1], {"seq_1": to}).start()
        return c

    lax.fori_loop(1, nz, send_z, 0)
    inz[my_z] = a_half[place(my_z)]
    dz[my_z] = dc[...]

    total = cuts[...]
    for v in range(low_bits + 1):
        width = STRETCH << max(v - 1, 0)
        mark, mark_doc = jnp.zeros((heads, tok), f32), jnp.zeros((1, tok), jnp.int32)
        if v == 0:
            for c in range(per_span):
                at = c * STRETCH + STRETCH // 2 - 1
                mark = jnp.where(lane >= c * STRETCH, total[:, at : at + 1], mark)
            rows_s[0] = jnp.exp(mark - total)
            rows_t[0] = rows_t[0] * jnp.exp(total - mark)
        else:
            for c in range(tok // (2 * width)):
                at = (2 * c + 1) * width - 1
                mark = jnp.where(lane >= 2 * c * width, total[:, at : at + 1], mark)
                mark_doc = jnp.where(lane1 >= 2 * c * width, docs[:, at : at + 1], mark_doc)
            upper = lane // width % 2 == 1
            same = (docs == mark_doc).astype(f32)
            rows_s[v] = jnp.where(upper, 0.0, jnp.exp(jnp.minimum(mark - total, 0.0)) * same)
            rows_t[v] = jnp.where(upper, rows_t[v] * jnp.exp(jnp.minimum(total - mark, 0.0)) * same, 0.0)
    reach = jnp.exp(total) * (docs == 0).astype(f32)
    for v in range(low_bits + 1, levels):
        rows_t[v] = rows_t[v] * reach

    source = lax.broadcasted_iota(jnp.int32, (BLOCK, BLOCK), 0)
    reader = lax.broadcasted_iota(jnp.int32, (BLOCK, BLOCK), 1)
    differ = jnp.bitwise_xor(source // STRETCH, reader // STRETCH)
    causal = source <= reader
    for b in range(tok // BLOCK):
        part = slice(b * BLOCK, (b + 1) * BLOCK)
        scores = jnp.where(causal, nt_dot(key_ref[part, :], query_ref[part, :]), 0.0)
        rhs[3 * b] = jnp.where(differ == 0, scores, 0.0).astype(bf)
        rhs[3 * b + 1] = jnp.where(differ == 1, scores, 0.0).astype(bf)
        rhs[3 * b + 2] = jnp.where(differ >= 2, scores, 0.0).astype(bf)
    rhs[6] = nt_dot(key_ref[:BLOCK, :], query_ref[BLOCK:, :]).astype(bf)

    def variants(h, c):
        row = pl.ds(pl.multiple_of(h * HEADDIM, HEADDIM), HEADDIM)
        scaled = scaled_t[row, :].astype(f32)
        var0[row, :] = (scaled * rows_s[0, pl.ds(h, 1), :]).astype(bf)
        var1[row, :] = (scaled * rows_s[1, pl.ds(h, 1), :]).astype(bf)
        var2[row, :] = (scaled * rows_s[2, pl.ds(h, 1), :]).astype(bf)
        var3[row, :] = (scaled[:, :BLOCK] * rows_s[3, pl.ds(h, 1), :BLOCK]).astype(bf)
        return c

    lax.fori_loop(0, heads, variants, 0)
    per_block = BLOCK // HEADDIM

    def inner(m, c):
        row = pl.ds(pl.multiple_of(m * BLOCK, BLOCK), BLOCK)
        for b in range(tok // BLOCK):
            part = slice(b * BLOCK, (b + 1) * BLOCK)
            products = [
                jnp.dot(var[row, part], rhs[3 * b + v], preferred_element_type=f32)
                for v, var in enumerate((var0, var1, var2))
            ]
            if b:
                products.append(jnp.dot(var3[row, :], rhs[6], preferred_element_type=f32))
            for i in range(per_block):
                h = m * per_block + i
                own = slice(i * HEADDIM, (i + 1) * HEADDIM)
                at = pl.ds(pl.multiple_of(h * HEADDIM, HEADDIM), HEADDIM)
                out = skip_ref[h] * val_t[at, part].astype(f32)
                for v, product in enumerate(products):
                    out = out + rows_t[v, pl.ds(h, 1), part] * product[own]
                acc_t[at, part] = out
        return c

    lax.fori_loop(0, ch // BLOCK, inner, 0)

    wait_bytes(dz.at[pl.ds(0, nz - 1)], z_r.at[1])
    wait_bytes(inz.at[pl.ds(0, nz - 1)], z_r.at[0])
    my_head = my_c * half_heads + place(my_z) * SHARD // HEADDIM
    rows_d = [dz[z] for z in range(nz)]
    state = [inz[z].astype(f32) for z in range(nz)]
    decay = [lane_pick(r, my_head) for r in rows_d]
    for j in range(bz):
        for m in range(0, nz >> j, 2):
            outz[base_z[j] + m // 2] = state[m].astype(bf)
        state = [state[m + 1] + decay[m + 1] * state[m] for m in range(0, nz >> j, 2)]
        decay = [decay[m + 1] * decay[m] for m in range(0, nz >> j, 2)]
    outz[total_z] = state[0].astype(bf)
    row_product = rows_d[0]
    for z in range(1, nz):
        row_product = row_product * rows_d[z]
    drow[...] = row_product

    def send_x(o, c):
        to = lax.rem(my_x + o, nx)
        remote(outz.at[total_z], xr.at[my_x], x_s.at[0], x_r.at[0], {"seq_0": to}).start()
        remote(drow, dxr.at[my_x], x_s.at[1], x_r.at[1], {"seq_0": to}).start()
        return c

    lax.fori_loop(1, nx, send_x, 0)
    xr[my_x] = outz[total_z]
    dxr[my_x] = drow[...]

    def send_levels_z(wanted):
        def step(o, c):
            to = lax.rem(my_z + o, nz)
            for j in wanted:
                @pl.when(bit(to, j))
                def _():
                    remote(
                        outz.at[base_z[j] + to // (1 << (j + 1))], rs.at[j, my_c, place(my_z)],
                        lev_s.at[j], lev_r.at[j], {"seq_1": to},
                    ).start()
            return c

        lax.fori_loop(1, nz, step, 0)
        for j in wanted:
            @pl.when(bit(my_z, j))
            def _():
                rs[j, my_c, place(my_z)] = outz[base_z[j] + my_z // (1 << (j + 1))]

    send_levels_z(range(bz // 2, bz))

    one = jnp.ones_like(d0)
    mine = jnp.where(first, one, d0)

    def weigh(v, lead):
        column = jnp.sum(jnp.where(square_mask, lead, 0.0), axis=1, keepdims=True)
        rows_t[v] = rows_t[v] * column

    for j in range(bz):
        low = my_z // (1 << j) * (1 << j)
        product = mine
        for z in range(nz):
            product = product * jnp.where((z >= low) & (z < my_z), rows_d[z], one)
        weigh(low_bits + 2 + j, product)
    row_lead = mine
    for z in range(nz):
        row_lead = row_lead * jnp.where(z < my_z, rows_d[z], one)

    wait_bytes(dxr.at[pl.ds(0, nx - 1)], x_r.at[1])
    wait_bytes(xr.at[pl.ds(0, nx - 1)], x_r.at[0])
    rows_x = [dxr[x] for x in range(nx)]
    state = [xr[x].astype(f32) for x in range(nx)]
    decay = [lane_pick(r, my_head) for r in rows_x]
    for j in range(bx):
        for m in range(0, nx >> j, 2):
            outx[base_x[j] + m // 2] = state[m].astype(bf)
        state = [state[m + 1] + decay[m + 1] * state[m] for m in range(0, nx >> j, 2)]
        decay = [decay[m + 1] * decay[m] for m in range(0, nx >> j, 2)]
    for j in range(bx):
        @pl.when(bit(my_x, j))
        def _():
            at = base_x[j] + my_x // (1 << (j + 1))
            for o in range(1, quads):
                to = lax.rem(my_z + 4 * o, nz)
                remote(
                    outx.at[at], rs.at[bz + j, my_c, place(my_z)], lev_s.at[bz + j], lev_r.at[bz + j], {"seq_1": to}
                ).start()
            rs[bz + j, my_c, place(my_z)] = outx[at]

    send_levels_z(range(bz // 2))
    for j in range(bx):
        low = my_x // (1 << j) * (1 << j)
        product = row_lead
        for x in range(nx):
            product = product * jnp.where((x >= low) & (x < my_x), rows_x[x], one)
        weigh(low_bits + 2 + bz + j, product)

    load_g.wait()

    def gate_pair(k, c):
        at = pl.multiple_of(k * 128, 128)
        g = gate_v[:, pl.ds(at, 128)].astype(f32)
        silu_t[pl.ds(at, 128), :] = (g / (1.0 + jnp.exp(-g))).T
        return c

    lax.fori_loop(0, heads // 2, gate_pair, 0)

    residue = lax.rem(my_z, 4) * quads
    for j in range(bx):
        @pl.when(bit(my_x, j))
        def _():
            if quads > 1:
                wait_bytes(rs.at[bz + j, 0, pl.ds(0, quads - 1)], lev_r.at[bz + j])
            for o in (1, nz - 1, 2):
                part = rs.at[bz + j, my_c, pl.ds(residue, quads)]
                remote(part, part, two_s.at[j], two_r.at[j], {"seq_1": lax.rem(my_z + o, nz)}).start()

    def apply(v, ref, rows):
        def step(m, c):
            for b in range(tok // BLOCK):
                part = slice(b * BLOCK, (b + 1) * BLOCK)
                block = ref(m)
                product = nt_dot(block, query_ref[part, :])
                for i in range(per_block):
                    h = m * per_block + i
                    at = pl.ds(pl.multiple_of(h * HEADDIM, HEADDIM), HEADDIM)
                    acc_t[at, part] += rows_t[v, pl.ds(h, 1), part] * product[i * HEADDIM : (i + 1) * HEADDIM]
            return c

        lax.fori_loop(rows[0], rows[1], step, 0)

    chunks = ch // BLOCK
    n = BLOCK // SHARD
    half_chunks = chunks // 2

    @pl.when(jnp.logical_not(first))
    def _():
        apply(low_bits + 1, lambda m: pe[pl.ds(m * n, n)].reshape(BLOCK, 128), (0, chunks))

    def swap(v):
        return remote(rs.at[v, my_c], rs.at[v, my_c], fin_s.at[v], fin_r.at[v], {"seq_2": other})

    def level_block(v):
        if half_chunks:
            return lambda m: rs[v, m // half_chunks, pl.ds(lax.rem(m, half_chunks) * n, n)].reshape(BLOCK, 128)
        return lambda m: jnp.concatenate([rs[v, 0].reshape(BLOCK // 2, 128), rs[v, 1].reshape(BLOCK // 2, 128)])

    for j in reversed(range(bz)):
        @pl.when(bit(my_z, j))
        def _():
            wait_bytes(rs.at[j, 0, pl.ds(0, nz - 1)], lev_r.at[j])
            swap(j).start()

    for j in reversed(range(bz)):
        @pl.when(bit(my_z, j))
        def _():
            swap(j).wait()
            apply(low_bits + 2 + j, level_block(j), (0, chunks))

    for j in range(bx):
        @pl.when(bit(my_x, j))
        def _():
            wait_bytes(rs.at[bz + j, 0, pl.ds(0, 3 * quads)], two_r.at[j])
            swap(bz + j).start()

    for j in range(bx):
        @pl.when(bit(my_x, j))
        def _():
            v = bz + j
            if half_chunks:
                apply(low_bits + 2 + v, level_block(v), (my_c * half_chunks, (my_c + 1) * half_chunks))
                swap(v).wait()
                apply(low_bits + 2 + v, level_block(v), (other * half_chunks, (other + 1) * half_chunks))
            else:
                swap(v).wait()
                apply(low_bits + 2 + v, level_block(v), (0, chunks))

    def gate_rows(k, squares):
        row = pl.ds(pl.multiple_of(k * 128, 128), 128)
        g = acc_t[row, :] * silu_t[row, :]
        acc_t[row, :] = g
        return squares + jnp.sum(g * g, axis=0, keepdims=True)

    sq_own[...] = lax.fori_loop(0, heads // 2, gate_rows, jnp.zeros((1, tok), f32))

    def send_y(o, c):
        remote(sq_own, sq.at[my_y], y_s, y_r, {"head": lax.rem(my_y + o, ny)}).start()
        return c

    lax.fori_loop(1, ny, send_y, 0)
    sq[my_y] = sq_own[...]

    def back(k, c):
        at = pl.multiple_of(k * 128, 128)
        gated_out[:, pl.ds(at, 128)] = acc_t[pl.ds(at, 128), :].T
        return c

    lax.fori_loop(0, heads // 2, back, 0)

    wait_bytes(a_half.at[pl.ds(0, nz - 1)], z_s.at[0])
    wait_bytes(dz.at[pl.ds(0, nz - 1)], z_s.at[1])
    wait_bytes(xr.at[pl.ds(0, nx - 1)], x_s.at[0])
    wait_bytes(dxr.at[pl.ds(0, nx - 1)], x_s.at[1])
    for j in range(bz):
        @pl.when(bit(my_z, j))
        def _():
            if nz // 2 > 1:
                wait_bytes(inz.at[pl.ds(0, nz // 2 - 1)], lev_s.at[j])

        @pl.when(jnp.logical_not(bit(my_z, j)))
        def _():
            wait_bytes(inz.at[pl.ds(0, nz // 2)], lev_s.at[j])
    for j in range(bx):
        @pl.when(bit(my_x, j))
        def _():
            if quads > 1:
                wait_bytes(inz.at[pl.ds(0, quads - 1)], lev_s.at[bz + j])
            wait_bytes(rs.at[bz + j, 0, pl.ds(0, 3 * quads)], two_s.at[j])
    if ny > 1:
        wait_bytes(sq.at[pl.ds(0, ny - 1)], y_s)
        wait_bytes(sq.at[pl.ds(0, ny - 1)], y_r)
    squares = sq[0]
    for y in range(1, ny):
        squares = squares + sq[y]
    square_out[...] = squares


def local(
    values_in, gate_in, key_proj, query_proj, step_size, log_decay, skip_weight, norm_gain, level_table, level_pick, doc_start,
):
    nx, nz, ny = lax.axis_size("seq_0"), lax.axis_size("seq_1"), lax.axis_size("head")
    tok, ch = values_in.shape
    heads = step_size.shape[1]
    width = key_proj.shape[1]
    levels_out = nz.bit_length() - 1 + nx.bit_length() - 1
    bx = nx.bit_length() - 1
    table_levels = level_table.shape[2]
    bf, f32 = jnp.bfloat16, jnp.float32
    vmem = pl.BlockSpec(memory_space=pltpu.VMEM)
    smem = pl.BlockSpec(memory_space=pltpu.SMEM)
    hbm = pl.BlockSpec(memory_space=pl.ANY)
    dma = pltpu.SemaphoreType.DMA
    V = pltpu.VMEM
    gated, squares = pl.pallas_call(
        functools.partial(layer_kernel, nx, nz, ny),
        name="layer",
        out_shape=(jax.ShapeDtypeStruct((tok, ch), f32), jax.ShapeDtypeStruct((1, tok), f32)),
        in_specs=[hbm, hbm, vmem, vmem, vmem, vmem, vmem, vmem, smem, smem],
        out_specs=(vmem, vmem),
        scratch_shapes=[
            V((tok, ch), bf), V((tok, ch), bf), V((ch, tok), bf), V((ch, tok), bf),
            V((ch, tok), bf), V((ch, tok), bf), V((ch, tok), bf), V((ch, BLOCK), bf),
            V((7, BLOCK, BLOCK), bf), V((ch, tok), f32), V((ch, tok), f32),
            V((heads, tok), f32), V((heads, tok), f32), V((4, heads, tok), f32), V((table_levels, heads, tok), f32),
            V((2 * nz, SHARD, width), bf), V((1, 128), f32), V((2 * nz, SHARD, width), bf), V((1, 128), f32),
            V((nz, SHARD, width), bf), V((1, 128), f32), V((nz, SHARD, width), bf), V((nz, 1, 128), f32),
            V((nz, SHARD, width), bf), V((1, 128), f32), V((nx, SHARD, width), bf), V((nx, 1, 128), f32),
            V((nx, SHARD, width), bf), V((levels_out, 2, nz, SHARD, width), bf),
            V((1, tok), f32), V((ny, 1, tok), f32),
            dma((2,)), dma((2,)), dma((2,)), dma((2,)), dma((2,)), dma((2,)), dma((2,)),
            dma((levels_out,)), dma((levels_out,)), dma((bx,)), dma((bx,)), dma((levels_out,)), dma((levels_out,)),
            dma, dma,
        ],
        compiler_params=pltpu.CompilerParams(collective_id=0, has_side_effects=True, vmem_limit_bytes=50 << 20),
    )(
        values_in, gate_in, key_proj, query_proj, step_size, log_decay, level_table, level_pick.reshape(1, tok),
        doc_start, skip_weight,
    )
    mean_square = squares[0] / (ch * ny)
    return (gated * lax.rsqrt(mean_square + epsilon)[:, None] * norm_gain[None, :]).astype(bf)


def solution(mesh):
    split = Mesh(
        mesh.devices.reshape(4, 16, 2, mesh.shape["head"]), ("seq_0", "seq_1", "seq_2", "head")
    )
    return on_mesh(split)


def on_mesh(split):
    placed = (
        P(SEQ, "head"),
        P(SEQ, "head"),
        P(SEQ, None),
        P(SEQ, None),
        P(SEQ, "head"),
        P(SEQ, "head"),
        P("head"),
        P("head"),
        P(None, "head", None),
        P(SEQ),
        P(SEQ),
    )
    return jax.shard_map(local, mesh=split, in_specs=placed, out_specs=P(SEQ, "head"), check_vma=False)
```

```python
import functools

import jax
import jax.numpy as jnp
from jax import lax
from jax.experimental import pallas as pl
from jax.experimental.pallas import tpu as pltpu
from jax.sharding import Mesh
from jax.sharding import PartitionSpec as P

HEADDIM = 64
STRETCH = 64
BLOCK = 256
SEQ = ("seq_0", "seq_1", "seq_2")
epsilon = 1e-06

MESH_ID = pl.DeviceIdType.MESH
SHARD = 32


def remote(src, dst, send, recv, where):
    return pltpu.make_async_remote_copy(
        src_ref=src, dst_ref=dst, send_sem=send, recv_sem=recv, device_id=where, device_id_type=MESH_ID
    )


def wait_bytes(ref, sem):
    pltpu.make_async_copy(ref, ref, sem).wait()


def lane_pick(rows, lane):
    lanes = lax.broadcasted_iota(jnp.int32, rows.shape, 1)
    return jnp.sum(jnp.where(lanes == lane, rows, 0.0), axis=1, keepdims=True)


def levels_base(size, bits):
    base, at = [], 0
    for j in range(bits):
        base.append(at)
        at += size >> (j + 1)
    return base, at


def bit(value, j):
    return lax.rem(value // (1 << j), 2) == 1


def nt_dot(a, b):
    return lax.dot_general(a, b, (((1,), (1,)), ((), ())), preferred_element_type=jnp.float32)


def layer_kernel(
    nx, nz, ny, val_hbm, gate_hbm, key_hbm, query_hbm, step_hbm, log_hbm, table_hbm, pick_hbm, doc_hbm, skip_hbm,
    gated_out, square_out,
    key_ref, query_ref, log_ref, table_ref, pick_ref, doc_ref, skip_ref,
    val_v, gate_v, val_t, scaled_t, var0, var1, var2, var3, rhs, acc_t, silu_t, steps, cuts, rows_s, rows_t,
    e_buf, d_buf, pe, pd, a_half, dc, inz, dz, outz, drow, xr, dxr, outx, rs, sq_own, sq,
    load_s, pair_s, pair_r, z_s, z_r, x_s, x_r, lev_s, lev_r, two_s, two_r, fin_s, fin_r, y_s, y_r,
):
    f32, bf = jnp.float32, jnp.bfloat16
    tok, ch = val_v.shape
    heads = ch // HEADDIM
    per_span = tok // STRETCH
    low_bits = per_span.bit_length() - 1
    bz, bx = nz.bit_length() - 1, nx.bit_length() - 1
    quads = nz // 4
    base_z, total_z = levels_base(nz, bz)
    base_x, _ = levels_base(nx, bx)
    my_x, my_z, my_c = lax.axis_index("seq_0"), lax.axis_index("seq_1"), lax.axis_index("seq_2")
    my_y = lax.axis_index("head")
    other = 1 - my_c
    half_heads = heads // 2

    def place(z):
        return lax.rem(z, 4) * quads + z // 4

    barrier = pltpu.get_barrier_semaphore()

    def greet(axis, mine, size):
        def step(o, c):
            pl.semaphore_signal(barrier, inc=1, device_id={axis: lax.rem(mine + o, size)}, device_id_type=MESH_ID)
            return c

        lax.fori_loop(1, size, step, 0)

    greet("seq_1", my_z, nz)
    greet("seq_0", my_x, nx)
    greet("head", my_y, ny)
    pl.semaphore_signal(barrier, inc=1, device_id={"seq_2": other}, device_id_type=MESH_ID)

    loads = [
        pltpu.make_async_copy(src, dst, load_s.at[i])
        for i, (src, dst) in enumerate((
            (log_hbm, log_ref), (doc_hbm, doc_ref), (val_hbm, val_v), (step_hbm, steps), (key_hbm, key_ref),
            (query_hbm, query_ref), (table_hbm, table_ref), (pick_hbm, pick_ref), (skip_hbm, skip_ref), (gate_hbm, gate_v),
        ))
    ]
    for load in loads:
        load.start()
    loads[0].wait()
    loads[1].wait()

    total = log_ref[...]
    lane = lax.broadcasted_iota(jnp.int32, (heads, tok), 1)
    shift = 1
    while shift < tok:
        total = total + jnp.where(lane >= shift, pltpu.roll(total, shift, 1), 0.0)
        shift *= 2
    cuts[...] = total
    lane1 = lax.broadcasted_iota(jnp.int32, (1, tok), 1)
    count = doc_ref[0]
    docs = jnp.broadcast_to(count, (1, tok))
    for c in range(1, per_span):
        count = count + doc_ref[c]
        docs = jnp.where(lane1 >= c * STRETCH, count, docs)
    last = tok - 1
    end_log = total[:, last:]
    rows_s[0] = jnp.exp(end_log - total) * (docs == docs[:, last:]).astype(f32)
    square_mask = lax.broadcasted_iota(jnp.int32, (heads, 128), 0) == lax.broadcasted_iota(jnp.int32, (heads, 128), 1)
    end_decay = jnp.exp(end_log) * (docs[:, last:] == 0).astype(f32)
    d_buf[...] = jnp.sum(jnp.where(square_mask, end_decay, 0.0), axis=0, keepdims=True)

    for load in loads[2:5]:
        load.wait()

    def end_pair(k, c):
        at = pl.multiple_of(k * 128, 128)
        v = val_v[:, pl.ds(at, 128)].astype(f32).T
        val_t[pl.ds(at, 128), :] = v.astype(bf)
        for i in range(2):
            h = 2 * k + i
            row = pl.ds(pl.multiple_of(h * HEADDIM, HEADDIM), HEADDIM)
            scaled = (v[i * HEADDIM : (i + 1) * HEADDIM] * steps[pl.ds(h, 1), :]).astype(bf)
            scaled_t[row, :] = scaled
            var0[row, :] = (scaled.astype(f32) * rows_s[0, pl.ds(h, 1), :]).astype(bf)
        return c

    lax.fori_loop(0, heads // 2, end_pair, 0)
    per = SHARD

    def end_dot(m, c):
        n = BLOCK // per
        part = jnp.dot(
            var0[pl.ds(pl.multiple_of(m * BLOCK, BLOCK), BLOCK), :], key_ref[...], preferred_element_type=f32
        ).astype(bf)
        for i in range(n):
            e_buf[m * n + i] = part[i * per : (i + 1) * per]
        return c

    lax.fori_loop(0, ch // BLOCK, end_dot, 0)

    pl.semaphore_wait(barrier, nz + nx + ny - 2)

    ce = remote(e_buf, pe, pair_s.at[0], pair_r.at[0], {"seq_2": other})
    cd = remote(d_buf, pd, pair_s.at[1], pair_r.at[1], {"seq_2": other})
    ce.start()
    cd.start()

    for load in loads[5:9]:
        load.wait()
    picks = jnp.broadcast_to(pick_ref[...], (heads, tok))
    levels, groups, _ = table_ref.shape
    for v in range(levels):
        w = jnp.zeros((heads, tok), f32)
        columns = table_ref[v].T
        for g in range(groups):
            w = jnp.where(picks == g, columns[:, g : g + 1], w)
        rows_t[v] = w

    cd.wait()
    ce.wait()
    first = my_c == 0
    d_own, d_oth = d_buf[...], pd[...]
    d0 = jnp.where(first, d_own, d_oth)
    d1 = jnp.where(first, d_oth, d_own)
    dc[...] = d0 * d1

    def merge_pair(s, c):
        own = e_buf[my_c * nz + s].astype(f32)
        oth = pe[my_c * nz + s].astype(f32)
        e0 = jnp.where(first, own, oth)
        e1 = jnp.where(first, oth, own)
        scale = lane_pick(d1, my_c * half_heads + s * SHARD // HEADDIM)
        a_half[s] = (e1 + scale * e0).astype(bf)
        return c

    for s in range(nz):
        merge_pair(s, 0)

    def send_z(o, c):
        to = lax.rem(my_z + o, nz)
        remote(a_half.at[place(to)], inz.at[my_z], z_s.at[0], z_r.at[0], {"seq_1": to}).start()
        remote(dc, dz.at[my_z], z_s.at[1], z_r.at[1], {"seq_1": to}).start()
        return c

    lax.fori_loop(1, nz, send_z, 0)
    inz[my_z] = a_half[place(my_z)]
    dz[my_z] = dc[...]

    total = cuts[...]
    for v in range(low_bits + 1):
        width = STRETCH << max(v - 1, 0)
        mark, mark_doc = jnp.zeros((heads, tok), f32), jnp.zeros((1, tok), jnp.int32)
        if v == 0:
            for c in range(per_span):
                at = c * STRETCH + STRETCH // 2 - 1
                mark = jnp.where(lane >= c * STRETCH, total[:, at : at + 1], mark)
            rows_s[0] = jnp.exp(mark - total)
            rows_t[0] = rows_t[0] * jnp.exp(total - mark)
        else:
            for c in range(tok // (2 * width)):
                at = (2 * c + 1) * width - 1
                mark = jnp.where(lane >= 2 * c * width, total[:, at : at + 1], mark)
                mark_doc = jnp.where(lane1 >= 2 * c * width, docs[:, at : at + 1], mark_doc)
            upper = lane // width % 2 == 1
            same = (docs == mark_doc).astype(f32)
            rows_s[v] = jnp.where(upper, 0.0, jnp.exp(jnp.minimum(mark - total, 0.0)) * same)
            rows_t[v] = jnp.where(upper, rows_t[v] * jnp.exp(jnp.minimum(total - mark, 0.0)) * same, 0.0)
    reach = jnp.exp(total) * (docs == 0).astype(f32)
    for v in range(low_bits + 1, levels):
        rows_t[v] = rows_t[v] * reach

    source = lax.broadcasted_iota(jnp.int32, (BLOCK, BLOCK), 0)
    reader = lax.broadcasted_iota(jnp.int32, (BLOCK, BLOCK), 1)
    differ = jnp.bitwise_xor(source // STRETCH, reader // STRETCH)
    causal = source <= reader
    for b in range(tok // BLOCK):
        part = slice(b * BLOCK, (b + 1) * BLOCK)
        scores = jnp.where(causal, nt_dot(key_ref[part, :], query_ref[part, :]), 0.0)
        rhs[3 * b] = jnp.where(differ == 0, scores, 0.0).astype(bf)
        rhs[3 * b + 1] = jnp.where(differ == 1, scores, 0.0).astype(bf)
        rhs[3 * b + 2] = jnp.where(differ >= 2, scores, 0.0).astype(bf)
    rhs[6] = nt_dot(key_ref[:BLOCK, :], query_ref[BLOCK:, :]).astype(bf)

    def variants(h, c):
        row = pl.ds(pl.multiple_of(h * HEADDIM, HEADDIM), HEADDIM)
        scaled = scaled_t[row, :].astype(f32)
        var0[row, :] = (scaled * rows_s[0, pl.ds(h, 1), :]).astype(bf)
        var1[row, :] = (scaled * rows_s[1, pl.ds(h, 1), :]).astype(bf)
        var2[row, :] = (scaled * rows_s[2, pl.ds(h, 1), :]).astype(bf)
        var3[row, :] = (scaled[:, :BLOCK] * rows_s[3, pl.ds(h, 1), :BLOCK]).astype(bf)
        return c

    lax.fori_loop(0, heads, variants, 0)
    per_block = BLOCK // HEADDIM

    def inner(m, c):
        row = pl.ds(pl.multiple_of(m * BLOCK, BLOCK), BLOCK)
        for b in range(tok // BLOCK):
            part = slice(b * BLOCK, (b + 1) * BLOCK)
            products = [
                jnp.dot(var[row, part], rhs[3 * b + v], preferred_element_type=f32)
                for v, var in enumerate((var0, var1, var2))
            ]
            if b:
                products.append(jnp.dot(var3[row, :], rhs[6], preferred_element_type=f32))
            for i in range(per_block):
                h = m * per_block + i
                own = slice(i * HEADDIM, (i + 1) * HEADDIM)
                at = pl.ds(pl.multiple_of(h * HEADDIM, HEADDIM), HEADDIM)
                out = skip_ref[h] * val_t[at, part].astype(f32)
                for v, product in enumerate(products):
                    out = out + rows_t[v, pl.ds(h, 1), part] * product[own]
                acc_t[at, part] = out
        return c

    lax.fori_loop(0, ch // BLOCK, inner, 0)

    wait_bytes(dz.at[pl.ds(0, nz - 1)], z_r.at[1])
    wait_bytes(inz.at[pl.ds(0, nz - 1)], z_r.at[0])
    my_head = my_c * half_heads + place(my_z) * SHARD // HEADDIM
    rows_d = [dz[z] for z in range(nz)]
    state = [inz[z].astype(f32) for z in range(nz)]
    decay = [lane_pick(r, my_head) for r in rows_d]
    for j in range(bz):
        for m in range(0, nz >> j, 2):
            outz[base_z[j] + m // 2] = state[m].astype(bf)
        state = [state[m + 1] + decay[m + 1] * state[m] for m in range(0, nz >> j, 2)]
        decay = [decay[m + 1] * decay[m] for m in range(0, nz >> j, 2)]
    outz[total_z] = state[0].astype(bf)
    row_product = rows_d[0]
    for z in range(1, nz):
        row_product = row_product * rows_d[z]
    drow[...] = row_product

    def send_x(o, c):
        to = lax.rem(my_x + o, nx)
        remote(outz.at[total_z], xr.at[my_x], x_s.at[0], x_r.at[0], {"seq_0": to}).start()
        remote(drow, dxr.at[my_x], x_s.at[1], x_r.at[1], {"seq_0": to}).start()
        return c

    lax.fori_loop(1, nx, send_x, 0)
    xr[my_x] = outz[total_z]
    dxr[my_x] = drow[...]

    def send_levels_z(wanted):
        def step(o, c):
            to = lax.rem(my_z + o, nz)
            for j in wanted:
                @pl.when(bit(to, j))
                def _():
                    remote(
                        outz.at[base_z[j] + to // (1 << (j + 1))], rs.at[j, my_c, place(my_z)],
                        lev_s.at[j], lev_r.at[j], {"seq_1": to},
                    ).start()
            return c

        lax.fori_loop(1, nz, step, 0)
        for j in wanted:
            @pl.when(bit(my_z, j))
            def _():
                rs[j, my_c, place(my_z)] = outz[base_z[j] + my_z // (1 << (j + 1))]

    send_levels_z(range(bz // 2, bz))

    one = jnp.ones_like(d0)
    mine = jnp.where(first, one, d0)

    def weigh(v, lead):
        column = jnp.sum(jnp.where(square_mask, lead, 0.0), axis=1, keepdims=True)
        rows_t[v] = rows_t[v] * column

    for j in range(bz):
        low = my_z // (1 << j) * (1 << j)
        product = mine
        for z in range(nz):
            product = product * jnp.where((z >= low) & (z < my_z), rows_d[z], one)
        weigh(low_bits + 2 + j, product)
    row_lead = mine
    for z in range(nz):
        row_lead = row_lead * jnp.where(z < my_z, rows_d[z], one)

    wait_bytes(dxr.at[pl.ds(0, nx - 1)], x_r.at[1])
    wait_bytes(xr.at[pl.ds(0, nx - 1)], x_r.at[0])
    rows_x = [dxr[x] for x in range(nx)]
    state = [xr[x].astype(f32) for x in range(nx)]
    decay = [lane_pick(r, my_head) for r in rows_x]
    for j in range(bx):
        for m in range(0, nx >> j, 2):
            outx[base_x[j] + m // 2] = state[m].astype(bf)
        state = [state[m + 1] + decay[m + 1] * state[m] for m in range(0, nx >> j, 2)]
        decay = [decay[m + 1] * decay[m] for m in range(0, nx >> j, 2)]
    for j in range(bx):
        @pl.when(bit(my_x, j))
        def _():
            at = base_x[j] + my_x // (1 << (j + 1))
            for o in range(1, quads):
                to = lax.rem(my_z + 4 * o, nz)
                remote(
                    outx.at[at], rs.at[bz + j, my_c, place(my_z)], lev_s.at[bz + j], lev_r.at[bz + j], {"seq_1": to}
                ).start()
            rs[bz + j, my_c, place(my_z)] = outx[at]

    send_levels_z(range(bz // 2))
    for j in range(bx):
        low = my_x // (1 << j) * (1 << j)
        product = row_lead
        for x in range(nx):
            product = product * jnp.where((x >= low) & (x < my_x), rows_x[x], one)
        weigh(low_bits + 2 + bz + j, product)

    loads[9].wait()

    def gate_pair(k, c):
        at = pl.multiple_of(k * 128, 128)
        g = gate_v[:, pl.ds(at, 128)].astype(f32)
        silu_t[pl.ds(at, 128), :] = (g / (1.0 + jnp.exp(-g))).T
        return c

    lax.fori_loop(0, heads // 2, gate_pair, 0)

    residue = lax.rem(my_z, 4) * quads
    for j in range(bx):
        @pl.when(bit(my_x, j))
        def _():
            if quads > 1:
                wait_bytes(rs.at[bz + j, 0, pl.ds(0, quads - 1)], lev_r.at[bz + j])
            for o in (1, nz - 1, 2):
                part = rs.at[bz + j, my_c, pl.ds(residue, quads)]
                remote(part, part, two_s.at[j], two_r.at[j], {"seq_1": lax.rem(my_z + o, nz)}).start()

    def apply(v, ref, rows):
        def step(m, c):
            for b in range(tok // BLOCK):
                part = slice(b * BLOCK, (b + 1) * BLOCK)
                block = ref(m)
                product = nt_dot(block, query_ref[part, :])
                for i in range(per_block):
                    h = m * per_block + i
                    at = pl.ds(pl.multiple_of(h * HEADDIM, HEADDIM), HEADDIM)
                    acc_t[at, part] += rows_t[v, pl.ds(h, 1), part] * product[i * HEADDIM : (i + 1) * HEADDIM]
            return c

        lax.fori_loop(rows[0], rows[1], step, 0)

    chunks = ch // BLOCK
    n = BLOCK // SHARD
    half_chunks = chunks // 2

    @pl.when(jnp.logical_not(first))
    def _():
        apply(low_bits + 1, lambda m: pe[pl.ds(m * n, n)].reshape(BLOCK, 128), (0, chunks))

    def swap(v):
        return remote(rs.at[v, my_c], rs.at[v, my_c], fin_s.at[v], fin_r.at[v], {"seq_2": other})

    def level_block(v):
        if half_chunks:
            return lambda m: rs[v, m // half_chunks, pl.ds(lax.rem(m, half_chunks) * n, n)].reshape(BLOCK, 128)
        return lambda m: jnp.concatenate([rs[v, 0].reshape(BLOCK // 2, 128), rs[v, 1].reshape(BLOCK // 2, 128)])

    for j in reversed(range(bz)):
        @pl.when(bit(my_z, j))
        def _():
            wait_bytes(rs.at[j, 0, pl.ds(0, nz - 1)], lev_r.at[j])
            swap(j).start()

    for j in reversed(range(bz)):
        @pl.when(bit(my_z, j))
        def _():
            swap(j).wait()
            apply(low_bits + 2 + j, level_block(j), (0, chunks))

    for j in range(bx):
        @pl.when(bit(my_x, j))
        def _():
            wait_bytes(rs.at[bz + j, 0, pl.ds(0, 3 * quads)], two_r.at[j])
            swap(bz + j).start()

    for j in range(bx):
        @pl.when(bit(my_x, j))
        def _():
            v = bz + j
            if half_chunks:
                apply(low_bits + 2 + v, level_block(v), (my_c * half_chunks, (my_c + 1) * half_chunks))
                swap(v).wait()
                apply(low_bits + 2 + v, level_block(v), (other * half_chunks, (other + 1) * half_chunks))
            else:
                swap(v).wait()
                apply(low_bits + 2 + v, level_block(v), (0, chunks))

    def gate_rows(k, squares):
        row = pl.ds(pl.multiple_of(k * 128, 128), 128)
        g = acc_t[row, :] * silu_t[row, :]
        acc_t[row, :] = g
        return squares + jnp.sum(g * g, axis=0, keepdims=True)

    sq_own[...] = lax.fori_loop(0, heads // 2, gate_rows, jnp.zeros((1, tok), f32))

    def send_y(o, c):
        remote(sq_own, sq.at[my_y], y_s, y_r, {"head": lax.rem(my_y + o, ny)}).start()
        return c

    lax.fori_loop(1, ny, send_y, 0)
    sq[my_y] = sq_own[...]

    def back(k, c):
        at = pl.multiple_of(k * 128, 128)
        gated_out[:, pl.ds(at, 128)] = acc_t[pl.ds(at, 128), :].T.astype(bf)
        return c

    lax.fori_loop(0, heads // 2, back, 0)

    wait_bytes(a_half.at[pl.ds(0, nz - 1)], z_s.at[0])
    wait_bytes(dz.at[pl.ds(0, nz - 1)], z_s.at[1])
    wait_bytes(xr.at[pl.ds(0, nx - 1)], x_s.at[0])
    wait_bytes(dxr.at[pl.ds(0, nx - 1)], x_s.at[1])
    for j in range(bz):
        @pl.when(bit(my_z, j))
        def _():
            if nz // 2 > 1:
                wait_bytes(inz.at[pl.ds(0, nz // 2 - 1)], lev_s.at[j])

        @pl.when(jnp.logical_not(bit(my_z, j)))
        def _():
            wait_bytes(inz.at[pl.ds(0, nz // 2)], lev_s.at[j])
    for j in range(bx):
        @pl.when(bit(my_x, j))
        def _():
            if quads > 1:
                wait_bytes(inz.at[pl.ds(0, quads - 1)], lev_s.at[bz + j])
            wait_bytes(rs.at[bz + j, 0, pl.ds(0, 3 * quads)], two_s.at[j])
    if ny > 1:
        wait_bytes(sq.at[pl.ds(0, ny - 1)], y_s)
        wait_bytes(sq.at[pl.ds(0, ny - 1)], y_r)
    squares = sq[0]
    for y in range(1, ny):
        squares = squares + sq[y]
    square_out[...] = squares


def local(
    values_in, gate_in, key_proj, query_proj, step_size, log_decay, skip_weight, norm_gain, level_table, level_pick, doc_start,
):
    nx, nz, ny = lax.axis_size("seq_0"), lax.axis_size("seq_1"), lax.axis_size("head")
    tok, ch = values_in.shape
    heads = step_size.shape[1]
    width = key_proj.shape[1]
    levels_out = nz.bit_length() - 1 + nx.bit_length() - 1
    bx = nx.bit_length() - 1
    table_levels = level_table.shape[2]
    bf, f32 = jnp.bfloat16, jnp.float32
    vmem = pl.BlockSpec(memory_space=pltpu.VMEM)
    hbm = pl.BlockSpec(memory_space=pltpu.HBM)
    dma = pltpu.SemaphoreType.DMA
    V = pltpu.VMEM
    gated, squares = pl.pallas_call(
        functools.partial(layer_kernel, nx, nz, ny),
        name="layer",
        out_shape=(jax.ShapeDtypeStruct((tok, ch), bf), jax.ShapeDtypeStruct((1, tok), f32)),
        in_specs=[hbm] * 10,
        out_specs=(vmem, vmem),
        scratch_shapes=[
            V((tok, width), bf), V((tok, width), bf), V((heads, tok), f32), V((table_levels, level_table.shape[0], heads), f32),
            V((1, tok), jnp.int32), pltpu.SMEM((doc_start.shape[0],), jnp.int32), pltpu.SMEM((heads,), f32),
            V((tok, ch), bf), V((tok, ch), bf), V((ch, tok), bf), V((ch, tok), bf),
            V((ch, tok), bf), V((ch, tok), bf), V((ch, tok), bf), V((ch, BLOCK), bf),
            V((7, BLOCK, BLOCK), bf), V((ch, tok), f32), V((ch, tok), f32),
            V((heads, tok), f32), V((heads, tok), f32), V((4, heads, tok), f32), V((table_levels, heads, tok), f32),
            V((2 * nz, SHARD, width), bf), V((1, 128), f32), V((2 * nz, SHARD, width), bf), V((1, 128), f32),
            V((nz, SHARD, width), bf), V((1, 128), f32), V((nz, SHARD, width), bf), V((nz, 1, 128), f32),
            V((nz, SHARD, width), bf), V((1, 128), f32), V((nx, SHARD, width), bf), V((nx, 1, 128), f32),
            V((nx, SHARD, width), bf), V((levels_out, 2, nz, SHARD, width), bf),
            V((1, tok), f32), V((ny, 1, tok), f32),
            dma((10,)), dma((2,)), dma((2,)), dma((2,)), dma((2,)), dma((2,)), dma((2,)),
            dma((levels_out,)), dma((levels_out,)), dma((bx,)), dma((bx,)), dma((levels_out,)), dma((levels_out,)),
            dma, dma,
        ],
        compiler_params=pltpu.CompilerParams(collective_id=0, has_side_effects=True, vmem_limit_bytes=67043328),
    )(
        values_in, gate_in, key_proj, query_proj, step_size.T, log_decay.T, level_table.transpose(2, 0, 1),
        level_pick.reshape(1, tok), doc_start, skip_weight,
    )
    mean_square = squares[0] / (ch * ny)
    return (gated * lax.rsqrt(mean_square + epsilon)[:, None] * norm_gain[None, :]).astype(bf)


def solution(mesh):
    split = Mesh(
        mesh.devices.reshape(4, 16, 2, mesh.shape["head"]), ("seq_0", "seq_1", "seq_2", "head")
    )
    return on_mesh(split)


def on_mesh(split):
    placed = (
        P(SEQ, "head"),
        P(SEQ, "head"),
        P(SEQ, None),
        P(SEQ, None),
        P(SEQ, "head"),
        P(SEQ, "head"),
        P("head"),
        P("head"),
        P(None, "head", None),
        P(SEQ),
        P(SEQ),
    )
    return jax.shard_map(local, mesh=split, in_specs=placed, out_specs=P(SEQ, "head"), check_vma=False)
```

```python
import functools

import jax
import jax.numpy as jnp
from jax import lax
from jax.experimental import pallas as pl
from jax.experimental.pallas import tpu as pltpu
from jax.sharding import Mesh
from jax.sharding import PartitionSpec as P

HEADDIM = 64
STRETCH = 64
BLOCK = 256
SEQ = ("seq_0", "seq_1", "seq_2")
epsilon = 1e-06

MESH_ID = pl.DeviceIdType.MESH
SHARD = 32


def remote(src, dst, send, recv, where):
    return pltpu.make_async_remote_copy(
        src_ref=src, dst_ref=dst, send_sem=send, recv_sem=recv, device_id=where, device_id_type=MESH_ID
    )


def wait_bytes(ref, sem):
    pltpu.make_async_copy(ref, ref, sem).wait()


def lane_pick(rows, lane):
    lanes = lax.broadcasted_iota(jnp.int32, rows.shape, 1)
    return jnp.sum(jnp.where(lanes == lane, rows, 0.0), axis=1, keepdims=True)


def levels_base(size, bits):
    base, at = [], 0
    for j in range(bits):
        base.append(at)
        at += size >> (j + 1)
    return base, at


def bit(value, j):
    return lax.rem(value // (1 << j), 2) == 1


def nt_dot(a, b):
    return lax.dot_general(a, b, (((1,), (1,)), ((), ())), preferred_element_type=jnp.float32)


def layer_kernel(
    nx, nz, ny, val_hbm, gate_hbm, key_hbm, query_hbm, step_hbm, log_hbm, table_hbm, pick_hbm, doc_hbm, skip_hbm,
    gated_out, square_out,
    key_ref, query_ref, log_ref, table_ref, pick_ref, doc_ref, skip_ref,
    val_v, gate_v, val_t, scaled_t, var0, var1, var2, var3, rhs, acc_t, silu_t, steps, cuts, rows_s, rows_t,
    e_buf, d_buf, pe, pd, a_half, dc, inz, dz, outz, drow, xr, dxr, outx, rs, sq_own, sq,
    load_s, pair_s, pair_r, z_s, z_r, x_s, x_r, lev_s, lev_r, two_s, two_r, fin_s, fin_r, y_s, y_r,
):
    f32, bf = jnp.float32, jnp.bfloat16
    tok, ch = val_v.shape
    heads = ch // HEADDIM
    per_span = tok // STRETCH
    low_bits = per_span.bit_length() - 1
    bz, bx = nz.bit_length() - 1, nx.bit_length() - 1
    quads = nz // 4
    base_z, total_z = levels_base(nz, bz)
    base_x, _ = levels_base(nx, bx)
    my_x, my_z, my_c = lax.axis_index("seq_0"), lax.axis_index("seq_1"), lax.axis_index("seq_2")
    my_y = lax.axis_index("head")
    other = 1 - my_c
    half_heads = heads // 2

    def far_first(i, size):
        return size // 2 + (i + 1) // 2 * (1 - 2 * lax.rem(i, 2))

    def place(z):
        return lax.rem(z, 4) * quads + z // 4

    barrier = pltpu.get_barrier_semaphore()

    def greet(axis, mine, size):
        def step(o, c):
            pl.semaphore_signal(barrier, inc=1, device_id={axis: lax.rem(mine + o, size)}, device_id_type=MESH_ID)
            return c

        lax.fori_loop(1, size, step, 0)

    greet("seq_1", my_z, nz)
    greet("seq_0", my_x, nx)
    greet("head", my_y, ny)
    pl.semaphore_signal(barrier, inc=1, device_id={"seq_2": other}, device_id_type=MESH_ID)

    loads = [
        pltpu.make_async_copy(src, dst, load_s.at[i])
        for i, (src, dst) in enumerate((
            (log_hbm, log_ref), (doc_hbm, doc_ref), (val_hbm, val_v), (step_hbm, steps), (key_hbm, key_ref),
            (query_hbm, query_ref), (table_hbm, table_ref), (pick_hbm, pick_ref), (skip_hbm, skip_ref), (gate_hbm, gate_v),
        ))
    ]
    for load in loads:
        load.start()
    loads[0].wait()
    loads[1].wait()

    total = log_ref[...]
    lane = lax.broadcasted_iota(jnp.int32, (heads, tok), 1)
    shift = 1
    while shift < tok:
        total = total + jnp.where(lane >= shift, pltpu.roll(total, shift, 1), 0.0)
        shift *= 2
    cuts[...] = total
    lane1 = lax.broadcasted_iota(jnp.int32, (1, tok), 1)
    count = doc_ref[0]
    docs = jnp.broadcast_to(count, (1, tok))
    for c in range(1, per_span):
        count = count + doc_ref[c]
        docs = jnp.where(lane1 >= c * STRETCH, count, docs)
    last = tok - 1
    end_log = total[:, last:]
    rows_s[0] = jnp.exp(end_log - total) * (docs == docs[:, last:]).astype(f32)
    square_mask = lax.broadcasted_iota(jnp.int32, (heads, 128), 0) == lax.broadcasted_iota(jnp.int32, (heads, 128), 1)
    end_decay = jnp.exp(end_log) * (docs[:, last:] == 0).astype(f32)
    d_buf[...] = jnp.sum(jnp.where(square_mask, end_decay, 0.0), axis=0, keepdims=True)

    for load in loads[2:5]:
        load.wait()

    def end_pair(k, c):
        at = pl.multiple_of(k * 128, 128)
        v = val_v[:, pl.ds(at, 128)].astype(f32).T
        val_t[pl.ds(at, 128), :] = v.astype(bf)
        for i in range(2):
            h = 2 * k + i
            row = pl.ds(pl.multiple_of(h * HEADDIM, HEADDIM), HEADDIM)
            scaled = (v[i * HEADDIM : (i + 1) * HEADDIM] * steps[pl.ds(h, 1), :]).astype(bf)
            scaled_t[row, :] = scaled
            var0[row, :] = (scaled.astype(f32) * rows_s[0, pl.ds(h, 1), :]).astype(bf)
        return c

    lax.fori_loop(0, heads // 2, end_pair, 0)
    per = SHARD

    def end_dot(m, c):
        n = BLOCK // per
        part = jnp.dot(
            var0[pl.ds(pl.multiple_of(m * BLOCK, BLOCK), BLOCK), :], key_ref[...], preferred_element_type=f32
        ).astype(bf)
        for i in range(n):
            e_buf[m * n + i] = part[i * per : (i + 1) * per]
        return c

    lax.fori_loop(0, ch // BLOCK, end_dot, 0)

    pl.semaphore_wait(barrier, nz + nx + ny - 2)

    ce = remote(e_buf, pe, pair_s.at[0], pair_r.at[0], {"seq_2": other})
    cd = remote(d_buf, pd, pair_s.at[1], pair_r.at[1], {"seq_2": other})
    ce.start()
    cd.start()

    for load in loads[5:9]:
        load.wait()
    picks = jnp.broadcast_to(pick_ref[...], (heads, tok))
    levels, groups, _ = table_ref.shape
    for v in range(levels):
        w = jnp.zeros((heads, tok), f32)
        columns = table_ref[v].T
        for g in range(groups):
            w = jnp.where(picks == g, columns[:, g : g + 1], w)
        rows_t[v] = w

    cd.wait()
    ce.wait()
    first = my_c == 0
    d_own, d_oth = d_buf[...], pd[...]
    d0 = jnp.where(first, d_own, d_oth)
    d1 = jnp.where(first, d_oth, d_own)
    dc[...] = d0 * d1

    def merge_pair(s, c):
        own = e_buf[my_c * nz + s].astype(f32)
        oth = pe[my_c * nz + s].astype(f32)
        e0 = jnp.where(first, own, oth)
        e1 = jnp.where(first, oth, own)
        scale = lane_pick(d1, my_c * half_heads + s * SHARD // HEADDIM)
        a_half[s] = (e1 + scale * e0).astype(bf)
        return c

    for s in range(nz):
        merge_pair(s, 0)

    def send_z(i, c):
        to = lax.rem(my_z + far_first(i, nz), nz)
        remote(a_half.at[place(to)], inz.at[my_z], z_s.at[0], z_r.at[0], {"seq_1": to}).start()
        remote(dc, dz.at[my_z], z_s.at[1], z_r.at[1], {"seq_1": to}).start()
        return c

    lax.fori_loop(0, nz - 1, send_z, 0)
    step_up = remote(a_half, rs.at[0, my_c], lev_s.at[0], lev_r.at[0], {"seq_1": lax.rem(my_z + 1, nz)})

    @pl.when(jnp.logical_not(bit(my_z, 0)))
    def _():
        step_up.start()

    inz[my_z] = a_half[place(my_z)]
    dz[my_z] = dc[...]

    total = cuts[...]
    for v in range(low_bits + 1):
        width = STRETCH << max(v - 1, 0)
        mark, mark_doc = jnp.zeros((heads, tok), f32), jnp.zeros((1, tok), jnp.int32)
        if v == 0:
            for c in range(per_span):
                at = c * STRETCH + STRETCH // 2 - 1
                mark = jnp.where(lane >= c * STRETCH, total[:, at : at + 1], mark)
            rows_s[0] = jnp.exp(mark - total)
            rows_t[0] = rows_t[0] * jnp.exp(total - mark)
        else:
            for c in range(tok // (2 * width)):
                at = (2 * c + 1) * width - 1
                mark = jnp.where(lane >= 2 * c * width, total[:, at : at + 1], mark)
                mark_doc = jnp.where(lane1 >= 2 * c * width, docs[:, at : at + 1], mark_doc)
            upper = lane // width % 2 == 1
            same = (docs == mark_doc).astype(f32)
            rows_s[v] = jnp.where(upper, 0.0, jnp.exp(jnp.minimum(mark - total, 0.0)) * same)
            rows_t[v] = jnp.where(upper, rows_t[v] * jnp.exp(jnp.minimum(total - mark, 0.0)) * same, 0.0)
    reach = jnp.exp(total) * (docs == 0).astype(f32)
    for v in range(low_bits + 1, levels):
        rows_t[v] = rows_t[v] * reach

    source = lax.broadcasted_iota(jnp.int32, (BLOCK, BLOCK), 0)
    reader = lax.broadcasted_iota(jnp.int32, (BLOCK, BLOCK), 1)
    differ = jnp.bitwise_xor(source // STRETCH, reader // STRETCH)
    causal = source <= reader
    for b in range(tok // BLOCK):
        part = slice(b * BLOCK, (b + 1) * BLOCK)
        scores = jnp.where(causal, nt_dot(key_ref[part, :], query_ref[part, :]), 0.0)
        rhs[3 * b] = jnp.where(differ == 0, scores, 0.0).astype(bf)
        rhs[3 * b + 1] = jnp.where(differ == 1, scores, 0.0).astype(bf)
        rhs[3 * b + 2] = jnp.where(differ >= 2, scores, 0.0).astype(bf)
    rhs[6] = nt_dot(key_ref[:BLOCK, :], query_ref[BLOCK:, :]).astype(bf)

    def variants(h, c):
        row = pl.ds(pl.multiple_of(h * HEADDIM, HEADDIM), HEADDIM)
        scaled = scaled_t[row, :].astype(f32)
        var0[row, :] = (scaled * rows_s[0, pl.ds(h, 1), :]).astype(bf)
        var1[row, :] = (scaled * rows_s[1, pl.ds(h, 1), :]).astype(bf)
        var2[row, :] = (scaled * rows_s[2, pl.ds(h, 1), :]).astype(bf)
        var3[row, :] = (scaled[:, :BLOCK] * rows_s[3, pl.ds(h, 1), :BLOCK]).astype(bf)
        return c

    lax.fori_loop(0, heads, variants, 0)
    per_block = BLOCK // HEADDIM

    def inner(m, c):
        row = pl.ds(pl.multiple_of(m * BLOCK, BLOCK), BLOCK)
        for b in range(tok // BLOCK):
            part = slice(b * BLOCK, (b + 1) * BLOCK)
            products = [
                jnp.dot(var[row, part], rhs[3 * b + v], preferred_element_type=f32)
                for v, var in enumerate((var0, var1, var2))
            ]
            if b:
                products.append(jnp.dot(var3[row, :], rhs[6], preferred_element_type=f32))
            for i in range(per_block):
                h = m * per_block + i
                own = slice(i * HEADDIM, (i + 1) * HEADDIM)
                at = pl.ds(pl.multiple_of(h * HEADDIM, HEADDIM), HEADDIM)
                out = skip_ref[h] * val_t[at, part].astype(f32)
                for v, product in enumerate(products):
                    out = out + rows_t[v, pl.ds(h, 1), part] * product[own]
                acc_t[at, part] = out
        return c

    lax.fori_loop(0, ch // BLOCK, inner, 0)

    wait_bytes(dz.at[pl.ds(0, nz - 1)], z_r.at[1])
    wait_bytes(inz.at[pl.ds(0, nz - 1)], z_r.at[0])
    my_head = my_c * half_heads + place(my_z) * SHARD // HEADDIM
    rows_d = [dz[z] for z in range(nz)]
    state = [inz[z].astype(f32) for z in range(nz)]
    decay = [lane_pick(r, my_head) for r in rows_d]
    for j in range(bz):
        for m in range(0, nz >> j, 2):
            outz[base_z[j] + m // 2] = state[m].astype(bf)
        state = [state[m + 1] + decay[m + 1] * state[m] for m in range(0, nz >> j, 2)]
        decay = [decay[m + 1] * decay[m] for m in range(0, nz >> j, 2)]
    outz[total_z] = state[0].astype(bf)
    row_product = rows_d[0]
    for z in range(1, nz):
        row_product = row_product * rows_d[z]
    drow[...] = row_product

    def send_x(i, c):
        to = lax.rem(my_x + far_first(i, nx), nx)
        remote(outz.at[total_z], xr.at[my_x], x_s.at[0], x_r.at[0], {"seq_0": to}).start()
        remote(drow, dxr.at[my_x], x_s.at[1], x_r.at[1], {"seq_0": to}).start()
        return c

    lax.fori_loop(0, nx - 1, send_x, 0)
    xr[my_x] = outz[total_z]
    dxr[my_x] = drow[...]

    near = 2
    quarter = my_z // 4

    def send_levels_quad():
        for j in range(near, bz):
            for o in sorted(range(1, quads), key=lambda o: -min(o, quads - o)):
                to = lax.rem(my_z + 4 * o, nz)
                @pl.when(bit(to, j))
                def _():
                    remote(
                        outz.at[base_z[j] + to // (1 << (j + 1))], rs.at[j, my_c, place(my_z)],
                        lev_s.at[j], lev_r.at[j], {"seq_1": to},
                    ).start()

            @pl.when(bit(my_z, j))
            def _():
                rs[j, my_c, place(my_z)] = outz[base_z[j] + my_z // (1 << (j + 1))]

    def pass_levels_quad():
        for j in range(near, bz):
            @pl.when(bit(my_z, j))
            def _():
                wait_bytes(rs.at[j, 0, pl.ds(0, quads - 1)], lev_r.at[j])
                for o in range(1, 4):
                    part = rs.at[j, my_c, pl.ds(lax.rem(my_z, 4) * quads, quads)]
                    to = quarter * 4 + lax.rem(my_z + o, 4)
                    remote(part, part, two_s.at[bx + j - near], two_r.at[bx + j - near], {"seq_1": to}).start()

    def send_levels_z(wanted):
        def step(i, c):
            to = lax.rem(my_z + far_first(i, nz), nz)
            for j in wanted:
                @pl.when(bit(to, j))
                def _():
                    remote(
                        outz.at[base_z[j] + to // (1 << (j + 1))], rs.at[j, my_c, place(my_z)],
                        lev_s.at[j], lev_r.at[j], {"seq_1": to},
                    ).start()
            return c

        lax.fori_loop(0, nz - 1, step, 0)
        for j in wanted:
            @pl.when(bit(my_z, j))
            def _():
                rs[j, my_c, place(my_z)] = outz[base_z[j] + my_z // (1 << (j + 1))]

    send_levels_quad()

    one = jnp.ones_like(d0)
    mine = jnp.where(first, one, d0)

    def weigh(v, lead):
        column = jnp.sum(jnp.where(square_mask, lead, 0.0), axis=1, keepdims=True)
        rows_t[v] = rows_t[v] * column

    for j in range(bz):
        low = my_z // (1 << j) * (1 << j)
        product = mine
        for z in range(nz):
            product = product * jnp.where((z >= low) & (z < my_z), rows_d[z], one)
        weigh(low_bits + 2 + j, product)
    row_lead = mine
    for z in range(nz):
        row_lead = row_lead * jnp.where(z < my_z, rows_d[z], one)

    wait_bytes(dxr.at[pl.ds(0, nx - 1)], x_r.at[1])
    wait_bytes(xr.at[pl.ds(0, nx - 1)], x_r.at[0])
    rows_x = [dxr[x] for x in range(nx)]
    state = [xr[x].astype(f32) for x in range(nx)]
    decay = [lane_pick(r, my_head) for r in rows_x]
    for j in range(bx):
        for m in range(0, nx >> j, 2):
            outx[base_x[j] + m // 2] = state[m].astype(bf)
        state = [state[m + 1] + decay[m + 1] * state[m] for m in range(0, nx >> j, 2)]
        decay = [decay[m + 1] * decay[m] for m in range(0, nx >> j, 2)]
    for j in range(bx):
        @pl.when(bit(my_x, j))
        def _():
            at = base_x[j] + my_x // (1 << (j + 1))
            for o in sorted(range(1, quads), key=lambda o: -min(o, quads - o)):
                to = lax.rem(my_z + 4 * o, nz)
                remote(
                    outx.at[at], rs.at[bz + j, my_c, place(my_z)], lev_s.at[bz + j], lev_r.at[bz + j], {"seq_1": to}
                ).start()
            rs[bz + j, my_c, place(my_z)] = outx[at]

    send_levels_z(range(1, near))
    for j in range(bx):
        low = my_x // (1 << j) * (1 << j)
        product = row_lead
        for x in range(nx):
            product = product * jnp.where((x >= low) & (x < my_x), rows_x[x], one)
        weigh(low_bits + 2 + bz + j, product)

    loads[9].wait()

    def gate_pair(k, c):
        at = pl.multiple_of(k * 128, 128)
        g = gate_v[:, pl.ds(at, 128)].astype(f32)
        silu_t[pl.ds(at, 128), :] = (g / (1.0 + jnp.exp(-g))).T
        return c

    lax.fori_loop(0, heads // 2, gate_pair, 0)

    pass_levels_quad()
    residue = lax.rem(my_z, 4) * quads
    for j in range(bx):
        @pl.when(bit(my_x, j))
        def _():
            if quads > 1:
                wait_bytes(rs.at[bz + j, 0, pl.ds(0, quads - 1)], lev_r.at[bz + j])
            for o in (2 if j % 2 == 0 else nz - 2, 1, nz - 1):
                part = rs.at[bz + j, my_c, pl.ds(residue, quads)]
                remote(part, part, two_s.at[j], two_r.at[j], {"seq_1": lax.rem(my_z + o, nz)}).start()

    def apply(v, ref, rows):
        def step(m, c):
            for b in range(tok // BLOCK):
                part = slice(b * BLOCK, (b + 1) * BLOCK)
                block = ref(m)
                product = nt_dot(block, query_ref[part, :])
                for i in range(per_block):
                    h = m * per_block + i
                    at = pl.ds(pl.multiple_of(h * HEADDIM, HEADDIM), HEADDIM)
                    acc_t[at, part] += rows_t[v, pl.ds(h, 1), part] * product[i * HEADDIM : (i + 1) * HEADDIM]
            return c

        lax.fori_loop(rows[0], rows[1], step, 0)

    chunks = ch // BLOCK
    n = BLOCK // SHARD
    half_chunks = chunks // 2

    @pl.when(jnp.logical_not(first))
    def _():
        apply(low_bits + 1, lambda m: pe[pl.ds(m * n, n)].reshape(BLOCK, 128), (0, chunks))

    def swap(v):
        return remote(rs.at[v, my_c], rs.at[v, my_c], fin_s.at[v], fin_r.at[v], {"seq_2": other})

    def level_block(v):
        if half_chunks:
            return lambda m: rs[v, m // half_chunks, pl.ds(lax.rem(m, half_chunks) * n, n)].reshape(BLOCK, 128)
        return lambda m: jnp.concatenate([rs[v, 0].reshape(BLOCK // 2, 128), rs[v, 1].reshape(BLOCK // 2, 128)])

    def arrive_z(j):
        @pl.when(bit(my_z, j))
        def _():
            if j == 0:
                wait_bytes(rs.at[0, 0], lev_r.at[0])
            elif j < near:
                wait_bytes(rs.at[j, 0, pl.ds(0, nz - 1)], lev_r.at[j])
            else:
                wait_bytes(rs.at[j, 0, pl.ds(0, 3 * quads)], two_r.at[bx + j - near])
            swap(j).start()

    def apply_z(j):
        @pl.when(bit(my_z, j))
        def _():
            swap(j).wait()
            apply(low_bits + 2 + j, level_block(j), (0, chunks))

    early = [0] + list(range(near, bz))
    for j in early:
        arrive_z(j)
    for j in early:
        apply_z(j)
    for j in range(bx):
        @pl.when(bit(my_x, j))
        def _():
            wait_bytes(rs.at[bz + j, 0, pl.ds(0, 3 * quads)], two_r.at[j])
            swap(bz + j).start()
    for j in range(1, near):
        arrive_z(j)
    if half_chunks:
        for j in range(bx):
            @pl.when(bit(my_x, j))
            def _():
                v = bz + j
                apply(low_bits + 2 + v, level_block(v), (my_c * half_chunks, (my_c + 1) * half_chunks))
    for j in range(1, near):
        apply_z(j)
    for j in range(bx):
        @pl.when(bit(my_x, j))
        def _():
            v = bz + j
            swap(v).wait()
            if half_chunks:
                apply(low_bits + 2 + v, level_block(v), (other * half_chunks, (other + 1) * half_chunks))
            else:
                apply(low_bits + 2 + v, level_block(v), (0, chunks))

    def gate_rows(k, squares):
        row = pl.ds(pl.multiple_of(k * 128, 128), 128)
        g = acc_t[row, :] * silu_t[row, :]
        acc_t[row, :] = g
        return squares + jnp.sum(g * g, axis=0, keepdims=True)

    sq_own[...] = lax.fori_loop(0, heads // 2, gate_rows, jnp.zeros((1, tok), f32))

    def send_y(o, c):
        remote(sq_own, sq.at[my_y], y_s, y_r, {"head": lax.rem(my_y + o, ny)}).start()
        return c

    lax.fori_loop(1, ny, send_y, 0)
    sq[my_y] = sq_own[...]

    def back(k, c):
        at = pl.multiple_of(k * 128, 128)
        gated_out[:, pl.ds(at, 128)] = acc_t[pl.ds(at, 128), :].T.astype(bf)
        return c

    lax.fori_loop(0, heads // 2, back, 0)

    wait_bytes(a_half.at[pl.ds(0, nz - 1)], z_s.at[0])
    wait_bytes(dz.at[pl.ds(0, nz - 1)], z_s.at[1])
    wait_bytes(xr.at[pl.ds(0, nx - 1)], x_s.at[0])
    wait_bytes(dxr.at[pl.ds(0, nx - 1)], x_s.at[1])
    for j in range(near, bz):
        reached = (bit(my_z, j)).astype(jnp.int32)
        for count in range(quads // 2 - 1, quads // 2 + 1):
            @pl.when((quads // 2 - reached == count) & (count > 0))
            def _():
                wait_bytes(inz.at[pl.ds(0, max(count, 1))], lev_s.at[j])

        @pl.when(bit(my_z, j))
        def _():
            wait_bytes(rs.at[j, 0, pl.ds(0, 3 * quads)], two_s.at[bx + j - near])
    @pl.when(jnp.logical_not(bit(my_z, 0)))
    def _():
        wait_bytes(a_half, lev_s.at[0])

    for j in range(1, near):
        @pl.when(bit(my_z, j))
        def _():
            if nz // 2 > 1:
                wait_bytes(inz.at[pl.ds(0, nz // 2 - 1)], lev_s.at[j])

        @pl.when(jnp.logical_not(bit(my_z, j)))
        def _():
            wait_bytes(inz.at[pl.ds(0, nz // 2)], lev_s.at[j])
    for j in range(bx):
        @pl.when(bit(my_x, j))
        def _():
            if quads > 1:
                wait_bytes(inz.at[pl.ds(0, quads - 1)], lev_s.at[bz + j])
            wait_bytes(rs.at[bz + j, 0, pl.ds(0, 3 * quads)], two_s.at[j])
    if ny > 1:
        wait_bytes(sq.at[pl.ds(0, ny - 1)], y_s)
        wait_bytes(sq.at[pl.ds(0, ny - 1)], y_r)
    squares = sq[0]
    for y in range(1, ny):
        squares = squares + sq[y]
    square_out[...] = squares


def local(
    values_in, gate_in, key_proj, query_proj, step_size, log_decay, skip_weight, norm_gain, level_table, level_pick, doc_start,
):
    nx, nz, ny = lax.axis_size("seq_0"), lax.axis_size("seq_1"), lax.axis_size("head")
    tok, ch = values_in.shape
    heads = step_size.shape[1]
    width = key_proj.shape[1]
    levels_out = nz.bit_length() - 1 + nx.bit_length() - 1
    bx = nx.bit_length() - 1
    table_levels = level_table.shape[2]
    bf, f32 = jnp.bfloat16, jnp.float32
    vmem = pl.BlockSpec(memory_space=pltpu.VMEM)
    hbm = pl.BlockSpec(memory_space=pltpu.HBM)
    dma = pltpu.SemaphoreType.DMA
    V = pltpu.VMEM
    gated, squares = pl.pallas_call(
        functools.partial(layer_kernel, nx, nz, ny),
        name="layer",
        out_shape=(jax.ShapeDtypeStruct((tok, ch), bf), jax.ShapeDtypeStruct((1, tok), f32)),
        in_specs=[hbm] * 10,
        out_specs=(vmem, vmem),
        scratch_shapes=[
            V((tok, width), bf), V((tok, width), bf), V((heads, tok), f32), V((table_levels, level_table.shape[0], heads), f32),
            V((1, tok), jnp.int32), pltpu.SMEM((doc_start.shape[0],), jnp.int32), pltpu.SMEM((heads,), f32),
            V((tok, ch), bf), V((tok, ch), bf), V((ch, tok), bf), V((ch, tok), bf),
            V((ch, tok), bf), V((ch, tok), bf), V((ch, tok), bf), V((ch, BLOCK), bf),
            V((7, BLOCK, BLOCK), bf), V((ch, tok), f32), V((ch, tok), f32),
            V((heads, tok), f32), V((heads, tok), f32), V((4, heads, tok), f32), V((table_levels, heads, tok), f32),
            V((2 * nz, SHARD, width), bf), V((1, 128), f32), V((2 * nz, SHARD, width), bf), V((1, 128), f32),
            V((nz, SHARD, width), bf), V((1, 128), f32), V((nz, SHARD, width), bf), V((nz, 1, 128), f32),
            V((nz, SHARD, width), bf), V((1, 128), f32), V((nx, SHARD, width), bf), V((nx, 1, 128), f32),
            V((nx, SHARD, width), bf), V((levels_out, 2, nz, SHARD, width), bf),
            V((1, tok), f32), V((ny, 1, tok), f32),
            dma((10,)), dma((2,)), dma((2,)), dma((2,)), dma((2,)), dma((2,)), dma((2,)),
            dma((levels_out,)), dma((levels_out,)), dma((2 * levels_out,)), dma((2 * levels_out,)), dma((levels_out,)), dma((levels_out,)),
            dma, dma,
        ],
        compiler_params=pltpu.CompilerParams(collective_id=0, has_side_effects=True, vmem_limit_bytes=67043328),
    )(
        values_in, gate_in, key_proj, query_proj, step_size.T, log_decay.T, level_table.transpose(2, 0, 1),
        level_pick.reshape(1, tok), doc_start, skip_weight,
    )
    mean_square = squares[0] / (ch * ny)
    return (gated * lax.rsqrt(mean_square + epsilon)[:, None] * norm_gain[None, :]).astype(bf)


def solution(mesh):
    split = Mesh(
        mesh.devices.reshape(4, 16, 2, mesh.shape["head"]), ("seq_0", "seq_1", "seq_2", "head")
    )
    return on_mesh(split)


def on_mesh(split):
    placed = (
        P(SEQ, "head"),
        P(SEQ, "head"),
        P(SEQ, None),
        P(SEQ, None),
        P(SEQ, "head"),
        P(SEQ, "head"),
        P("head"),
        P("head"),
        P(None, "head", None),
        P(SEQ),
        P(SEQ),
    )
    return jax.shard_map(local, mesh=split, in_specs=placed, out_specs=P(SEQ, "head"), check_vma=False)
```

```python
import functools

import jax
import jax.numpy as jnp
from jax import lax
from jax.experimental import pallas as pl
from jax.experimental.pallas import tpu as pltpu
from jax.sharding import Mesh
from jax.sharding import PartitionSpec as P

HEADDIM = 64
STRETCH = 64
BLOCK = 256
SEQ = ("seq_0", "seq_1", "seq_2")
epsilon = 1e-06

MESH_ID = pl.DeviceIdType.MESH
SHARD = 32


def remote(src, dst, send, recv, where):
    return pltpu.make_async_remote_copy(
        src_ref=src, dst_ref=dst, send_sem=send, recv_sem=recv, device_id=where, device_id_type=MESH_ID
    )


def wait_bytes(ref, sem):
    pltpu.make_async_copy(ref, ref, sem).wait()


def lane_pick(rows, lane):
    lanes = lax.broadcasted_iota(jnp.int32, rows.shape, 1)
    return jnp.sum(jnp.where(lanes == lane, rows, 0.0), axis=1, keepdims=True)


def levels_base(size, bits):
    base, at = [], 0
    for j in range(bits):
        base.append(at)
        at += size >> (j + 1)
    return base, at


def bit(value, j):
    return lax.rem(value // (1 << j), 2) == 1


def nt_dot(a, b):
    return lax.dot_general(a, b, (((1,), (1,)), ((), ())), preferred_element_type=jnp.float32)


def layer_kernel(
    nx, nz, ny, val_hbm, gate_hbm, key_hbm, query_hbm, step_hbm, log_hbm, table_hbm, pick_hbm, doc_hbm, skip_hbm,
    gated_out, square_out,
    key_ref, query_ref, log_ref, table_ref, pick_ref, doc_ref, skip_ref,
    val_v, gate_v, val_t, scaled_t, var0, var1, var2, var3, rhs, acc_t, silu_t, steps, cuts, rows_s, rows_t,
    e_buf, d_buf, pe, pd, a_half, dc, inz, dz, outz, drow, xr, dxr, outx, rs, sq_own, sq,
    load_s, pair_s, pair_r, z_s, z_r, x_s, x_r, lev_s, lev_r, two_s, two_r, row_r, fin_s, fin_r, y_s, y_r, out_s,
):
    f32, bf = jnp.float32, jnp.bfloat16
    tok, ch = val_v.shape
    heads = ch // HEADDIM
    per_span = tok // STRETCH
    low_bits = per_span.bit_length() - 1
    bz, bx = nz.bit_length() - 1, nx.bit_length() - 1
    quads = nz // 4
    base_z, total_z = levels_base(nz, bz)
    base_x, _ = levels_base(nx, bx)
    my_x, my_z, my_c = lax.axis_index("seq_0"), lax.axis_index("seq_1"), lax.axis_index("seq_2")
    my_y = lax.axis_index("head")
    other = 1 - my_c
    half_heads = heads // 2

    def far_first(i, size):
        return size // 2 + (i + 1) // 2 * (1 - 2 * lax.rem(i, 2))

    def place(z):
        return lax.rem(z, 4) * quads + z // 4

    barrier = pltpu.get_barrier_semaphore()

    def greet(axis, mine, size):
        def step(o, c):
            pl.semaphore_signal(barrier, inc=1, device_id={axis: lax.rem(mine + o, size)}, device_id_type=MESH_ID)
            return c

        lax.fori_loop(1, size, step, 0)

    greet("seq_1", my_z, nz)
    greet("seq_0", my_x, nx)
    greet("head", my_y, ny)
    pl.semaphore_signal(barrier, inc=1, device_id={"seq_2": other}, device_id_type=MESH_ID)

    loads = [
        pltpu.make_async_copy(src, dst, load_s.at[i])
        for i, (src, dst) in enumerate((
            (log_hbm, log_ref), (doc_hbm, doc_ref), (val_hbm, val_v), (step_hbm, steps), (key_hbm, key_ref),
            (query_hbm, query_ref), (table_hbm, table_ref), (pick_hbm, pick_ref), (skip_hbm, skip_ref), (gate_hbm, gate_v),
        ))
    ]
    for load in loads:
        load.start()
    loads[0].wait()
    loads[1].wait()

    total = log_ref[...]
    lane = lax.broadcasted_iota(jnp.int32, (heads, tok), 1)
    shift = 1
    while shift < tok:
        total = total + jnp.where(lane >= shift, pltpu.roll(total, shift, 1), 0.0)
        shift *= 2
    cuts[...] = total
    lane1 = lax.broadcasted_iota(jnp.int32, (1, tok), 1)
    count = doc_ref[0]
    docs = jnp.broadcast_to(count, (1, tok))
    for c in range(1, per_span):
        count = count + doc_ref[c]
        docs = jnp.where(lane1 >= c * STRETCH, count, docs)
    last = tok - 1
    end_log = total[:, last:]
    rows_s[0] = jnp.exp(end_log - total) * (docs == docs[:, last:]).astype(f32)
    square_mask = lax.broadcasted_iota(jnp.int32, (heads, 128), 0) == lax.broadcasted_iota(jnp.int32, (heads, 128), 1)
    end_decay = jnp.exp(end_log) * (docs[:, last:] == 0).astype(f32)
    d_buf[...] = jnp.sum(jnp.where(square_mask, end_decay, 0.0), axis=0, keepdims=True)

    for load in loads[2:5]:
        load.wait()

    def end_pair(k, c):
        at = pl.multiple_of(k * 128, 128)
        v = val_v[:, pl.ds(at, 128)].astype(f32).T
        val_t[pl.ds(at, 128), :] = v.astype(bf)
        for i in range(2):
            h = 2 * k + i
            row = pl.ds(pl.multiple_of(h * HEADDIM, HEADDIM), HEADDIM)
            scaled = (v[i * HEADDIM : (i + 1) * HEADDIM] * steps[pl.ds(h, 1), :]).astype(bf)
            scaled_t[row, :] = scaled
            var0[row, :] = (scaled.astype(f32) * rows_s[0, pl.ds(h, 1), :]).astype(bf)
        return c

    lax.fori_loop(0, heads // 2, end_pair, 0)
    per = SHARD

    def end_dot(m, c):
        n = BLOCK // per
        part = jnp.dot(
            var0[pl.ds(pl.multiple_of(m * BLOCK, BLOCK), BLOCK), :], key_ref[...], preferred_element_type=f32
        ).astype(bf)
        for i in range(n):
            e_buf[m * n + i] = part[i * per : (i + 1) * per]
        return c

    lax.fori_loop(0, ch // BLOCK, end_dot, 0)

    pl.semaphore_wait(barrier, nz + nx + ny - 2)

    ce = remote(e_buf, pe, pair_s.at[0], pair_r.at[0], {"seq_2": other})
    cd = remote(d_buf, pd, pair_s.at[1], pair_r.at[1], {"seq_2": other})
    ce.start()
    cd.start()

    for load in loads[5:9]:
        load.wait()
    picks = jnp.broadcast_to(pick_ref[...], (heads, tok))
    levels, groups, _ = table_ref.shape
    for v in range(levels):
        w = jnp.zeros((heads, tok), f32)
        columns = table_ref[v].T
        for g in range(groups):
            w = jnp.where(picks == g, columns[:, g : g + 1], w)
        rows_t[v] = w

    cd.wait()
    first = my_c == 0
    d_own, d_oth = d_buf[...], pd[...]
    d0 = jnp.where(first, d_own, d_oth)
    d1 = jnp.where(first, d_oth, d_own)
    dc[...] = d0 * d1
    scales = [lane_pick(d1, my_c * half_heads + h) for h in range(half_heads)]
    ce.wait()

    def merge_pair(s, c):
        own = e_buf[my_c * nz + s].astype(f32)
        oth = pe[my_c * nz + s].astype(f32)
        e0 = jnp.where(first, own, oth)
        e1 = jnp.where(first, oth, own)
        a_half[s] = (e1 + scales[s * SHARD // HEADDIM] * e0).astype(bf)
        return c

    for s in range(nz):
        merge_pair(s, 0)

    def send_z(i, c):
        to = lax.rem(my_z + far_first(i, nz), nz)
        remote(a_half.at[place(to)], inz.at[my_z], z_s.at[0], z_r.at[0], {"seq_1": to}).start()
        remote(dc, dz.at[my_z], z_s.at[1], z_r.at[1], {"seq_1": to}).start()
        return c

    lax.fori_loop(0, nz - 1, send_z, 0)
    step_up = remote(a_half, rs.at[0, my_c], lev_s.at[0], lev_r.at[0], {"seq_1": lax.rem(my_z + 1, nz)})

    @pl.when(jnp.logical_not(bit(my_z, 0)))
    def _():
        step_up.start()

    inz[my_z] = a_half[place(my_z)]
    dz[my_z] = dc[...]

    total = cuts[...]
    for v in range(low_bits + 1):
        width = STRETCH << max(v - 1, 0)
        mark, mark_doc = jnp.zeros((heads, tok), f32), jnp.zeros((1, tok), jnp.int32)
        if v == 0:
            for c in range(per_span):
                at = c * STRETCH + STRETCH // 2 - 1
                mark = jnp.where(lane >= c * STRETCH, total[:, at : at + 1], mark)
            rows_s[0] = jnp.exp(mark - total)
            rows_t[0] = rows_t[0] * jnp.exp(total - mark)
        else:
            for c in range(tok // (2 * width)):
                at = (2 * c + 1) * width - 1
                mark = jnp.where(lane >= 2 * c * width, total[:, at : at + 1], mark)
                mark_doc = jnp.where(lane1 >= 2 * c * width, docs[:, at : at + 1], mark_doc)
            upper = lane // width % 2 == 1
            same = (docs == mark_doc).astype(f32)
            rows_s[v] = jnp.where(upper, 0.0, jnp.exp(jnp.minimum(mark - total, 0.0)) * same)
            rows_t[v] = jnp.where(upper, rows_t[v] * jnp.exp(jnp.minimum(total - mark, 0.0)) * same, 0.0)
    reach = jnp.exp(total) * (docs == 0).astype(f32)
    for v in range(low_bits + 1, levels):
        rows_t[v] = rows_t[v] * reach

    source = lax.broadcasted_iota(jnp.int32, (BLOCK, BLOCK), 0)
    reader = lax.broadcasted_iota(jnp.int32, (BLOCK, BLOCK), 1)
    differ = jnp.bitwise_xor(source // STRETCH, reader // STRETCH)
    causal = source <= reader
    for b in range(tok // BLOCK):
        part = slice(b * BLOCK, (b + 1) * BLOCK)
        scores = jnp.where(causal, nt_dot(key_ref[part, :], query_ref[part, :]), 0.0)
        rhs[3 * b] = jnp.where(differ == 0, scores, 0.0).astype(bf)
        rhs[3 * b + 1] = jnp.where(differ == 1, scores, 0.0).astype(bf)
        rhs[3 * b + 2] = jnp.where(differ >= 2, scores, 0.0).astype(bf)
    rhs[6] = nt_dot(key_ref[:BLOCK, :], query_ref[BLOCK:, :]).astype(bf)

    def variants(h, c):
        row = pl.ds(pl.multiple_of(h * HEADDIM, HEADDIM), HEADDIM)
        scaled = scaled_t[row, :].astype(f32)
        var0[row, :] = (scaled * rows_s[0, pl.ds(h, 1), :]).astype(bf)
        var1[row, :] = (scaled * rows_s[1, pl.ds(h, 1), :]).astype(bf)
        var2[row, :] = (scaled * rows_s[2, pl.ds(h, 1), :]).astype(bf)
        var3[row, :] = (scaled[:, :BLOCK] * rows_s[3, pl.ds(h, 1), :BLOCK]).astype(bf)
        return c

    lax.fori_loop(0, heads, variants, 0)
    per_block = BLOCK // HEADDIM

    def inner(m, c):
        row = pl.ds(pl.multiple_of(m * BLOCK, BLOCK), BLOCK)
        for b in range(tok // BLOCK):
            part = slice(b * BLOCK, (b + 1) * BLOCK)
            products = [
                jnp.dot(var[row, part], rhs[3 * b + v], preferred_element_type=f32)
                for v, var in enumerate((var0, var1, var2))
            ]
            if b:
                products.append(jnp.dot(var3[row, :], rhs[6], preferred_element_type=f32))
            for i in range(per_block):
                h = m * per_block + i
                own = slice(i * HEADDIM, (i + 1) * HEADDIM)
                at = pl.ds(pl.multiple_of(h * HEADDIM, HEADDIM), HEADDIM)
                out = skip_ref[h] * val_t[at, part].astype(f32)
                for v, product in enumerate(products):
                    out = out + rows_t[v, pl.ds(h, 1), part] * product[own]
                acc_t[at, part] = out
        return c

    lax.fori_loop(0, ch // BLOCK, inner, 0)

    wait_bytes(dz.at[pl.ds(0, nz - 1)], z_r.at[1])
    my_head = my_c * half_heads + place(my_z) * SHARD // HEADDIM
    rows_d = [dz[z] for z in range(nz)]
    decay = [[lane_pick(r, my_head) for r in rows_d]]
    for j in range(bz):
        decay.append([decay[j][m + 1] * decay[j][m] for m in range(0, nz >> j, 2)])
    row_product = rows_d[0]
    for z in range(1, nz):
        row_product = row_product * rows_d[z]
    drow[...] = row_product

    def send_x_decay(i, c):
        to = lax.rem(my_x + far_first(i, nx), nx)
        remote(drow, dxr.at[my_x], x_s.at[1], x_r.at[1], {"seq_0": to}).start()
        return c

    lax.fori_loop(0, nx - 1, send_x_decay, 0)
    dxr[my_x] = drow[...]
    wait_bytes(inz.at[pl.ds(0, nz - 1)], z_r.at[0])
    state = [[inz[z].astype(f32) for z in range(nz)]]
    for j in range(bz):
        state.append([state[j][m + 1] + decay[j][m + 1] * state[j][m] for m in range(0, nz >> j, 2)])
    outz[total_z] = state[bz][0].astype(bf)
    for j in range(bz):
        for m in range(0, nz >> j, 2):
            outz[base_z[j] + m // 2] = state[j][m].astype(bf)

    def send_x(i, c):
        to = lax.rem(my_x + far_first(i, nx), nx)
        remote(outz.at[total_z], xr.at[my_x], x_s.at[0], x_r.at[0], {"seq_0": to}).start()
        return c

    lax.fori_loop(0, nx - 1, send_x, 0)
    xr[my_x] = outz[total_z]
    near = 2

    def pass_row(j, o):
        shard = rs.at[bz + j, my_c, lax.rem(my_z, 4) * quads + lax.rem(my_z // 4 + quads - o, quads)]
        if o:
            wait_bytes(shard, row_r.at[j * quads + o])
        for to in (2 if j % 2 == 0 else nz - 2, 1, nz - 1):
            remote(shard, shard, two_s.at[j], two_r.at[j], {"seq_1": lax.rem(my_z + to, nz)}).start()
    quarter = my_z // 4

    def send_levels_quad():
        for j in range(near, bz):
            for o in sorted(range(1, quads), key=lambda o: -min(o, quads - o)):
                to = lax.rem(my_z + 4 * o, nz)
                @pl.when(bit(to, j))
                def _():
                    remote(
                        outz.at[base_z[j] + to // (1 << (j + 1))], rs.at[j, my_c, place(my_z)],
                        lev_s.at[j], lev_r.at[j], {"seq_1": to},
                    ).start()

            @pl.when(bit(my_z, j))
            def _():
                rs[j, my_c, place(my_z)] = outz[base_z[j] + my_z // (1 << (j + 1))]

    def pass_levels_quad():
        for j in range(near, bz):
            @pl.when(bit(my_z, j))
            def _():
                wait_bytes(rs.at[j, 0, pl.ds(0, quads - 1)], lev_r.at[j])
                for o in range(1, 4):
                    part = rs.at[j, my_c, pl.ds(lax.rem(my_z, 4) * quads, quads)]
                    to = quarter * 4 + lax.rem(my_z + o, 4)
                    remote(part, part, two_s.at[bx + j - near], two_r.at[bx + j - near], {"seq_1": to}).start()

    def send_levels_z(wanted):
        def step(i, c):
            to = lax.rem(my_z + far_first(i, nz), nz)
            for j in wanted:
                @pl.when(bit(to, j))
                def _():
                    remote(
                        outz.at[base_z[j] + to // (1 << (j + 1))], rs.at[j, my_c, place(my_z)],
                        lev_s.at[j], lev_r.at[j], {"seq_1": to},
                    ).start()
            return c

        lax.fori_loop(0, nz - 1, step, 0)
        for j in wanted:
            @pl.when(bit(my_z, j))
            def _():
                rs[j, my_c, place(my_z)] = outz[base_z[j] + my_z // (1 << (j + 1))]

    send_levels_quad()

    one = jnp.ones_like(d0)
    mine = jnp.where(first, one, d0)

    def weigh(v, lead):
        column = jnp.sum(jnp.where(square_mask, lead, 0.0), axis=1, keepdims=True)
        rows_t[v] = rows_t[v] * column

    for j in range(bz):
        low = my_z // (1 << j) * (1 << j)
        product = mine
        for z in range(nz):
            product = product * jnp.where((z >= low) & (z < my_z), rows_d[z], one)
        weigh(low_bits + 2 + j, product)
    row_lead = mine
    for z in range(nz):
        row_lead = row_lead * jnp.where(z < my_z, rows_d[z], one)

    wait_bytes(dxr.at[pl.ds(0, nx - 1)], x_r.at[1])
    rows_x = [dxr[x] for x in range(nx)]
    decay = [lane_pick(r, my_head) for r in rows_x]
    wait_bytes(xr.at[pl.ds(0, nx - 1)], x_r.at[0])
    state = [xr[x].astype(f32) for x in range(nx)]
    for j in range(bx):
        for m in range(0, nx >> j, 2):
            outx[base_x[j] + m // 2] = state[m].astype(bf)
        state = [state[m + 1] + decay[m + 1] * state[m] for m in range(0, nx >> j, 2)]
        decay = [decay[m + 1] * decay[m] for m in range(0, nx >> j, 2)]
    for j in range(bx):
        @pl.when(bit(my_x, j))
        def _():
            at = base_x[j] + my_x // (1 << (j + 1))
            for o in sorted(range(1, quads), key=lambda o: -min(o, quads - o)):
                to = lax.rem(my_z + 4 * o, nz)
                remote(
                    outx.at[at], rs.at[bz + j, my_c, place(my_z)], lev_s.at[bz + j], row_r.at[j * quads + o], {"seq_1": to}
                ).start()
            rs[bz + j, my_c, place(my_z)] = outx[at]
            pass_row(j, 0)

    send_levels_z(range(1, near))
    for j in range(bx):
        low = my_x // (1 << j) * (1 << j)
        product = row_lead
        for x in range(nx):
            product = product * jnp.where((x >= low) & (x < my_x), rows_x[x], one)
        weigh(low_bits + 2 + bz + j, product)

    loads[9].wait()

    def gate_pair(k, c):
        at = pl.multiple_of(k * 128, 128)
        g = gate_v[:, pl.ds(at, 128)].astype(f32)
        silu_t[pl.ds(at, 128), :] = (g / (1.0 + jnp.exp(-g))).T
        return c

    lax.fori_loop(0, heads // 2, gate_pair, 0)

    pass_levels_quad()
    for o in sorted(range(1, quads), key=lambda o: min(o, quads - o)):
        for j in range(bx):
            @pl.when(bit(my_x, j))
            def _():
                pass_row(j, o)

    def apply(v, ref, rows):
        def step(m, c):
            for b in range(tok // BLOCK):
                part = slice(b * BLOCK, (b + 1) * BLOCK)
                block = ref(m)
                product = nt_dot(block, query_ref[part, :])
                for i in range(per_block):
                    h = m * per_block + i
                    at = pl.ds(pl.multiple_of(h * HEADDIM, HEADDIM), HEADDIM)
                    acc_t[at, part] += rows_t[v, pl.ds(h, 1), part] * product[i * HEADDIM : (i + 1) * HEADDIM]
            return c

        lax.fori_loop(rows[0], rows[1], step, 0)

    chunks = ch // BLOCK
    n = BLOCK // SHARD
    half_chunks = chunks // 2

    @pl.when(jnp.logical_not(first))
    def _():
        apply(low_bits + 1, lambda m: pe[pl.ds(m * n, n)].reshape(BLOCK, 128), (0, chunks))

    def swap(v):
        return remote(rs.at[v, my_c], rs.at[v, my_c], fin_s.at[v], fin_r.at[v], {"seq_2": other})

    def level_block(v):
        if half_chunks:
            return lambda m: rs[v, m // half_chunks, pl.ds(lax.rem(m, half_chunks) * n, n)].reshape(BLOCK, 128)
        return lambda m: jnp.concatenate([rs[v, 0].reshape(BLOCK // 2, 128), rs[v, 1].reshape(BLOCK // 2, 128)])

    def arrive_z(j):
        @pl.when(bit(my_z, j))
        def _():
            if j == 0:
                wait_bytes(rs.at[0, 0], lev_r.at[0])
            elif j < near:
                wait_bytes(rs.at[j, 0, pl.ds(0, nz - 1)], lev_r.at[j])
            else:
                wait_bytes(rs.at[j, 0, pl.ds(0, 3 * quads)], two_r.at[bx + j - near])
            swap(j).start()

    def apply_z(j):
        @pl.when(bit(my_z, j))
        def _():
            swap(j).wait()
            apply(low_bits + 2 + j, level_block(j), (0, chunks))

    early = [0] + list(range(near, bz))
    for j in early:
        arrive_z(j)
    for j in early:
        apply_z(j)
    for j in range(bx):
        @pl.when(bit(my_x, j))
        def _():
            wait_bytes(rs.at[bz + j, 0, pl.ds(0, 3 * quads)], two_r.at[j])
            swap(bz + j).start()
    for j in range(1, near):
        arrive_z(j)
    if half_chunks:
        for j in range(bx):
            @pl.when(bit(my_x, j))
            def _():
                v = bz + j
                apply(low_bits + 2 + v, level_block(v), (my_c * half_chunks, (my_c + 1) * half_chunks))
    for j in range(1, near):
        apply_z(j)
    for j in range(bx):
        @pl.when(bit(my_x, j))
        def _():
            v = bz + j
            swap(v).wait()
            if half_chunks:
                apply(low_bits + 2 + v, level_block(v), (other * half_chunks, (other + 1) * half_chunks))
            else:
                apply(low_bits + 2 + v, level_block(v), (0, chunks))

    def gate_rows(k, squares):
        row = pl.ds(pl.multiple_of(k * 128, 128), 128)
        g = acc_t[row, :] * silu_t[row, :]
        acc_t[row, :] = g
        return squares + jnp.sum(g * g, axis=0, keepdims=True)

    sq_own[...] = lax.fori_loop(0, heads // 2, gate_rows, jnp.zeros((1, tok), f32))

    def send_y(o, c):
        remote(sq_own, sq.at[my_y], y_s, y_r, {"head": lax.rem(my_y + o, ny)}).start()
        return c

    lax.fori_loop(1, ny, send_y, 0)
    sq[my_y] = sq_own[...]

    for k in range(heads // 2):
        part = pl.ds(k * 128, 128)
        val_v[:, part] = acc_t[part, :].T.astype(bf)
        if k:
            part = pl.ds(k * 128 - 128, 128)
            pltpu.make_async_copy(val_v.at[:, part], gated_out.at[:, part], out_s).start()

    part = pl.ds(ch - 128, 128)
    pltpu.make_async_copy(val_v.at[:, part], gated_out.at[:, part], out_s).start()

    wait_bytes(a_half.at[pl.ds(0, nz - 1)], z_s.at[0])
    wait_bytes(dz.at[pl.ds(0, nz - 1)], z_s.at[1])
    wait_bytes(xr.at[pl.ds(0, nx - 1)], x_s.at[0])
    wait_bytes(dxr.at[pl.ds(0, nx - 1)], x_s.at[1])
    for j in range(near, bz):
        reached = (bit(my_z, j)).astype(jnp.int32)
        for count in range(quads // 2 - 1, quads // 2 + 1):
            @pl.when((quads // 2 - reached == count) & (count > 0))
            def _():
                wait_bytes(inz.at[pl.ds(0, max(count, 1))], lev_s.at[j])

        @pl.when(bit(my_z, j))
        def _():
            wait_bytes(rs.at[j, 0, pl.ds(0, 3 * quads)], two_s.at[bx + j - near])
    @pl.when(jnp.logical_not(bit(my_z, 0)))
    def _():
        wait_bytes(a_half, lev_s.at[0])

    for j in range(1, near):
        @pl.when(bit(my_z, j))
        def _():
            if nz // 2 > 1:
                wait_bytes(inz.at[pl.ds(0, nz // 2 - 1)], lev_s.at[j])

        @pl.when(jnp.logical_not(bit(my_z, j)))
        def _():
            wait_bytes(inz.at[pl.ds(0, nz // 2)], lev_s.at[j])
    for j in range(bx):
        @pl.when(bit(my_x, j))
        def _():
            if quads > 1:
                wait_bytes(inz.at[pl.ds(0, quads - 1)], lev_s.at[bz + j])
            wait_bytes(rs.at[bz + j, 0, pl.ds(0, 3 * quads)], two_s.at[j])
    if ny > 1:
        wait_bytes(sq.at[pl.ds(0, ny - 1)], y_s)
        wait_bytes(sq.at[pl.ds(0, ny - 1)], y_r)
    squares = sq[0]
    for y in range(1, ny):
        squares = squares + sq[y]
    wait_bytes(val_v, out_s)
    square_out[...] = squares


def finish_kernel(count, gated_hbm, square_hbm, gain_hbm, out_hbm, gated, done, squares, gain, small_s, in_s, out_s):
    tok, ch = gated.shape
    rows = tok // 8
    small = [
        pltpu.make_async_copy(square_hbm, squares, small_s.at[0]), pltpu.make_async_copy(gain_hbm, gain, small_s.at[1]),
    ]
    parts = [pl.ds(k * rows, rows) for k in range(8)]
    loads = [pltpu.make_async_copy(gated_hbm.at[part], gated.at[part], in_s.at[k]) for k, part in enumerate(parts)]
    stores = [pltpu.make_async_copy(done.at[part], out_hbm.at[part], out_s.at[k]) for k, part in enumerate(parts)]
    for copy in small + loads:
        copy.start()
    for copy in small:
        copy.wait()
    scale = lax.rsqrt(squares[...] / count + epsilon)
    column = jnp.broadcast_to(scale, (128, tok)).T[:, :1]
    weight = gain[...]
    for k, part in enumerate(parts):
        loads[k].wait()
        done[part, :] = (gated[part, :].astype(jnp.float32) * column[k * rows : (k + 1) * rows] * weight).astype(jnp.bfloat16)
        if k:
            stores[k - 1].start()
    stores[7].start()
    for copy in stores:
        copy.wait()


def local(
    values_in, gate_in, key_proj, query_proj, step_size, log_decay, skip_weight, norm_gain, level_table, level_pick, doc_start,
):
    nx, nz, ny = lax.axis_size("seq_0"), lax.axis_size("seq_1"), lax.axis_size("head")
    tok, ch = values_in.shape
    heads = step_size.shape[1]
    width = key_proj.shape[1]
    levels_out = nz.bit_length() - 1 + nx.bit_length() - 1
    bx = nx.bit_length() - 1
    table_levels = level_table.shape[2]
    bf, f32 = jnp.bfloat16, jnp.float32
    vmem = pl.BlockSpec(memory_space=pltpu.VMEM)
    hbm = pl.BlockSpec(memory_space=pltpu.HBM)
    dma = pltpu.SemaphoreType.DMA
    V = pltpu.VMEM
    gated, squares = pl.pallas_call(
        functools.partial(layer_kernel, nx, nz, ny),
        name="layer",
        out_shape=(jax.ShapeDtypeStruct((tok, ch), bf), jax.ShapeDtypeStruct((1, tok), f32)),
        in_specs=[hbm] * 10,
        out_specs=(hbm, vmem),
        scratch_shapes=[
            V((tok, width), bf), V((tok, width), bf), V((heads, tok), f32), V((table_levels, level_table.shape[0], heads), f32),
            V((1, tok), jnp.int32), pltpu.SMEM((doc_start.shape[0],), jnp.int32), pltpu.SMEM((heads,), f32),
            V((tok, ch), bf), V((tok, ch), bf), V((ch, tok), bf), V((ch, tok), bf),
            V((ch, tok), bf), V((ch, tok), bf), V((ch, tok), bf), V((ch, BLOCK), bf),
            V((7, BLOCK, BLOCK), bf), V((ch, tok), f32), V((ch, tok), f32),
            V((heads, tok), f32), V((heads, tok), f32), V((4, heads, tok), f32), V((table_levels, heads, tok), f32),
            V((2 * nz, SHARD, width), bf), V((1, 128), f32), V((2 * nz, SHARD, width), bf), V((1, 128), f32),
            V((nz, SHARD, width), bf), V((1, 128), f32), V((nz, SHARD, width), bf), V((nz, 1, 128), f32),
            V((nz, SHARD, width), bf), V((1, 128), f32), V((nx, SHARD, width), bf), V((nx, 1, 128), f32),
            V((nx, SHARD, width), bf), V((levels_out, 2, nz, SHARD, width), bf),
            V((1, tok), f32), V((ny, 1, tok), f32),
            dma((10,)), dma((2,)), dma((2,)), dma((2,)), dma((2,)), dma((2,)), dma((2,)),
            dma((levels_out,)), dma((levels_out,)), dma((2 * levels_out,)), dma((2 * levels_out,)), dma((bx * nz // 4,)), dma((levels_out,)), dma((levels_out,)),
            dma, dma, dma,
        ],
        compiler_params=pltpu.CompilerParams(collective_id=0, has_side_effects=True, vmem_limit_bytes=67043328),
    )(
        values_in, gate_in, key_proj, query_proj, step_size.T, log_decay.T, level_table.transpose(2, 0, 1),
        level_pick.reshape(1, tok), doc_start, skip_weight,
    )
    return pl.pallas_call(
        functools.partial(finish_kernel, ch * ny),
        name="finish",
        out_shape=jax.ShapeDtypeStruct((tok, ch), bf),
        in_specs=[hbm] * 3,
        out_specs=hbm,
        scratch_shapes=[V((tok, ch), bf), V((tok, ch), bf), V((1, tok), f32), V((1, ch), f32), dma((2,)), dma((8,)), dma((8,))],
        compiler_params=pltpu.CompilerParams(vmem_limit_bytes=67043328),
    )(gated, squares, norm_gain.reshape(1, ch))


def solution(mesh):
    split = Mesh(
        mesh.devices.reshape(4, 16, 2, mesh.shape["head"]), ("seq_0", "seq_1", "seq_2", "head")
    )
    return on_mesh(split)


def on_mesh(split):
    placed = (
        P(SEQ, "head"),
        P(SEQ, "head"),
        P(SEQ, None),
        P(SEQ, None),
        P(SEQ, "head"),
        P(SEQ, "head"),
        P("head"),
        P("head"),
        P(None, "head", None),
        P(SEQ),
        P(SEQ),
    )
    return jax.shard_map(local, mesh=split, in_specs=placed, out_specs=P(SEQ, "head"), check_vma=False)
```

```python
import functools

import jax
import jax.numpy as jnp
from jax import lax
from jax.experimental import pallas as pl
from jax.experimental.pallas import tpu as pltpu
from jax.sharding import Mesh
from jax.sharding import PartitionSpec as P

HEADDIM = 64
STRETCH = 64
BLOCK = 256
SEQ = ("seq_0", "seq_1", "seq_2")
epsilon = 1e-06

MESH_ID = pl.DeviceIdType.MESH
SHARD = 32


def remote(src, dst, send, recv, where):
    return pltpu.make_async_remote_copy(
        src_ref=src, dst_ref=dst, send_sem=send, recv_sem=recv, device_id=where, device_id_type=MESH_ID
    )


def wait_bytes(ref, sem):
    pltpu.make_async_copy(ref, ref, sem).wait()


def lane_pick(rows, lane):
    lanes = lax.broadcasted_iota(jnp.int32, rows.shape, 1)
    return jnp.sum(jnp.where(lanes == lane, rows, 0.0), axis=1, keepdims=True)


def levels_base(size, bits):
    base, at = [], 0
    for j in range(bits):
        base.append(at)
        at += size >> (j + 1)
    return base, at


def bit(value, j):
    return lax.rem(value // (1 << j), 2) == 1


def nt_dot(a, b):
    return lax.dot_general(a, b, (((1,), (1,)), ((), ())), preferred_element_type=jnp.float32)


def layer_kernel(
    nx, nz, ny, val_hbm, gate_hbm, key_hbm, query_hbm, step_hbm, log_hbm, table_hbm, pick_hbm, doc_hbm, skip_hbm,
    gated_out, square_out,
    key_ref, query_ref, log_ref, table_ref, pick_ref, doc_ref, skip_ref,
    val_v, gate_v, val_t, scaled_t, var0, var1, var2, var3, rhs, acc_t, silu_t, steps, cuts, rows_s, rows_t,
    e_buf, d_buf, pe, pd, a_half, dc, inz, dz, outz, drow, xr, dxr, outx, rs, sq_own, sq,
    load_s, pair_s, pair_r, z_s, z_r, x_s, x_r, lev_s, lev_r, two_s, two_r, row_r, fin_s, fin_r, y_s, y_r, out_s,
):
    f32, bf = jnp.float32, jnp.bfloat16
    tok, ch = val_v.shape
    heads = ch // HEADDIM
    per_span = tok // STRETCH
    low_bits = per_span.bit_length() - 1
    bz, bx = nz.bit_length() - 1, nx.bit_length() - 1
    quads = nz // 4
    base_z, total_z = levels_base(nz, bz)
    base_x, _ = levels_base(nx, bx)
    my_x, my_z, my_c = lax.axis_index("seq_0"), lax.axis_index("seq_1"), lax.axis_index("seq_2")
    my_y = lax.axis_index("head")
    other = 1 - my_c
    half_heads = heads // 2

    def far_first(i, size):
        return size // 2 + (i + 1) // 2 * (1 - 2 * lax.rem(i, 2))

    def place(z):
        return lax.rem(z, 4) * quads + z // 4

    barrier = pltpu.get_barrier_semaphore()

    def greet(axis, mine, size):
        def step(o, c):
            pl.semaphore_signal(barrier, inc=1, device_id={axis: lax.rem(mine + o, size)}, device_id_type=MESH_ID)
            return c

        lax.fori_loop(1, size, step, 0)

    greet("seq_1", my_z, nz)
    greet("seq_0", my_x, nx)
    greet("head", my_y, ny)
    pl.semaphore_signal(barrier, inc=1, device_id={"seq_2": other}, device_id_type=MESH_ID)

    loads = [
        pltpu.make_async_copy(src, dst, load_s.at[i])
        for i, (src, dst) in enumerate((
            (log_hbm, log_ref), (doc_hbm, doc_ref), (val_hbm, val_v), (step_hbm, steps), (key_hbm, key_ref),
            (query_hbm, query_ref), (table_hbm, table_ref), (pick_hbm, pick_ref), (skip_hbm, skip_ref), (gate_hbm, gate_v),
        ))
    ]
    for load in loads:
        load.start()
    loads[0].wait()
    loads[1].wait()

    total = log_ref[...]
    lane = lax.broadcasted_iota(jnp.int32, (heads, tok), 1)
    shift = 1
    while shift < tok:
        total = total + jnp.where(lane >= shift, pltpu.roll(total, shift, 1), 0.0)
        shift *= 2
    cuts[...] = total
    lane1 = lax.broadcasted_iota(jnp.int32, (1, tok), 1)
    count = doc_ref[0]
    docs = jnp.broadcast_to(count, (1, tok))
    for c in range(1, per_span):
        count = count + doc_ref[c]
        docs = jnp.where(lane1 >= c * STRETCH, count, docs)
    last = tok - 1
    end_log = total[:, last:]
    rows_s[0] = jnp.exp(end_log - total) * (docs == docs[:, last:]).astype(f32)
    square_mask = lax.broadcasted_iota(jnp.int32, (heads, 128), 0) == lax.broadcasted_iota(jnp.int32, (heads, 128), 1)
    end_decay = jnp.exp(end_log) * (docs[:, last:] == 0).astype(f32)
    d_buf[...] = jnp.sum(jnp.where(square_mask, end_decay, 0.0), axis=0, keepdims=True)

    for load in loads[2:5]:
        load.wait()

    def end_pair(k, c):
        at = pl.multiple_of(k * 128, 128)
        v = val_v[:, pl.ds(at, 128)].astype(f32).T
        val_t[pl.ds(at, 128), :] = v.astype(bf)
        for i in range(2):
            h = 2 * k + i
            row = pl.ds(pl.multiple_of(h * HEADDIM, HEADDIM), HEADDIM)
            scaled = (v[i * HEADDIM : (i + 1) * HEADDIM] * steps[pl.ds(h, 1), :]).astype(bf)
            scaled_t[row, :] = scaled
            var0[row, :] = (scaled.astype(f32) * rows_s[0, pl.ds(h, 1), :]).astype(bf)
        return c

    lax.fori_loop(0, heads // 2, end_pair, 0)
    per = SHARD

    def end_dot(m, c):
        n = BLOCK // per
        part = jnp.dot(
            var0[pl.ds(pl.multiple_of(m * BLOCK, BLOCK), BLOCK), :], key_ref[...], preferred_element_type=f32
        ).astype(bf)
        for i in range(n):
            e_buf[m * n + i] = part[i * per : (i + 1) * per]
        return c

    lax.fori_loop(0, ch // BLOCK, end_dot, 0)

    pl.semaphore_wait(barrier, nz + nx + ny - 2)

    ce = remote(e_buf, pe, pair_s.at[0], pair_r.at[0], {"seq_2": other})
    cd = remote(d_buf, pd, pair_s.at[1], pair_r.at[1], {"seq_2": other})
    ce.start()
    cd.start()

    for load in loads[5:9]:
        load.wait()
    picks = jnp.broadcast_to(pick_ref[...], (heads, tok))
    levels, groups, _ = table_ref.shape
    for v in range(levels):
        w = jnp.zeros((heads, tok), f32)
        columns = table_ref[v].T
        for g in range(groups):
            w = jnp.where(picks == g, columns[:, g : g + 1], w)
        rows_t[v] = w

    cd.wait()
    first = my_c == 0
    d_own, d_oth = d_buf[...], pd[...]
    d0 = jnp.where(first, d_own, d_oth)
    d1 = jnp.where(first, d_oth, d_own)
    dc[...] = d0 * d1
    scales = [lane_pick(d1, my_c * half_heads + h) for h in range(half_heads)]
    ce.wait()

    def merge_pair(s, c):
        own = e_buf[my_c * nz + s].astype(f32)
        oth = pe[my_c * nz + s].astype(f32)
        e0 = jnp.where(first, own, oth)
        e1 = jnp.where(first, oth, own)
        a_half[s] = (e1 + scales[s * SHARD // HEADDIM] * e0).astype(bf)
        return c

    for s in range(nz):
        merge_pair(s, 0)

    def send_z(i, c):
        to = lax.rem(my_z + far_first(i, nz), nz)
        remote(a_half.at[place(to)], inz.at[my_z], z_s.at[0], z_r.at[0], {"seq_1": to}).start()
        remote(dc, dz.at[my_z], z_s.at[1], z_r.at[1], {"seq_1": to}).start()
        return c

    lax.fori_loop(0, nz - 1, send_z, 0)
    step_up = remote(a_half, rs.at[0, my_c], lev_s.at[0], lev_r.at[0], {"seq_1": lax.rem(my_z + 1, nz)})

    @pl.when(jnp.logical_not(bit(my_z, 0)))
    def _():
        step_up.start()

    inz[my_z] = a_half[place(my_z)]
    dz[my_z] = dc[...]

    total = cuts[...]
    for v in range(low_bits + 1):
        width = STRETCH << max(v - 1, 0)
        mark, mark_doc = jnp.zeros((heads, tok), f32), jnp.zeros((1, tok), jnp.int32)
        if v == 0:
            for c in range(per_span):
                at = c * STRETCH + STRETCH // 2 - 1
                mark = jnp.where(lane >= c * STRETCH, total[:, at : at + 1], mark)
            rows_s[0] = jnp.exp(mark - total)
            rows_t[0] = rows_t[0] * jnp.exp(total - mark)
        else:
            for c in range(tok // (2 * width)):
                at = (2 * c + 1) * width - 1
                mark = jnp.where(lane >= 2 * c * width, total[:, at : at + 1], mark)
                mark_doc = jnp.where(lane1 >= 2 * c * width, docs[:, at : at + 1], mark_doc)
            upper = lane // width % 2 == 1
            same = (docs == mark_doc).astype(f32)
            rows_s[v] = jnp.where(upper, 0.0, jnp.exp(jnp.minimum(mark - total, 0.0)) * same)
            rows_t[v] = jnp.where(upper, rows_t[v] * jnp.exp(jnp.minimum(total - mark, 0.0)) * same, 0.0)
    reach = jnp.exp(total) * (docs == 0).astype(f32)
    for v in range(low_bits + 1, levels):
        rows_t[v] = rows_t[v] * reach

    source = lax.broadcasted_iota(jnp.int32, (BLOCK, BLOCK), 0)
    reader = lax.broadcasted_iota(jnp.int32, (BLOCK, BLOCK), 1)
    differ = jnp.bitwise_xor(source // STRETCH, reader // STRETCH)
    causal = source <= reader
    for b in range(tok // BLOCK):
        part = slice(b * BLOCK, (b + 1) * BLOCK)
        scores = jnp.where(causal, nt_dot(key_ref[part, :], query_ref[part, :]), 0.0)
        rhs[3 * b] = jnp.where(differ == 0, scores, 0.0).astype(bf)
        rhs[3 * b + 1] = jnp.where(differ == 1, scores, 0.0).astype(bf)
        rhs[3 * b + 2] = jnp.where(differ >= 2, scores, 0.0).astype(bf)
    rhs[6] = nt_dot(key_ref[:BLOCK, :], query_ref[BLOCK:, :]).astype(bf)

    def variants(h, c):
        row = pl.ds(pl.multiple_of(h * HEADDIM, HEADDIM), HEADDIM)
        scaled = scaled_t[row, :].astype(f32)
        var0[row, :] = (scaled * rows_s[0, pl.ds(h, 1), :]).astype(bf)
        var1[row, :] = (scaled * rows_s[1, pl.ds(h, 1), :]).astype(bf)
        var2[row, :] = (scaled * rows_s[2, pl.ds(h, 1), :]).astype(bf)
        var3[row, :] = (scaled[:, :BLOCK] * rows_s[3, pl.ds(h, 1), :BLOCK]).astype(bf)
        return c

    lax.fori_loop(0, heads, variants, 0)
    per_block = BLOCK // HEADDIM

    def inner(m, c):
        row = pl.ds(pl.multiple_of(m * BLOCK, BLOCK), BLOCK)
        for b in range(tok // BLOCK):
            part = slice(b * BLOCK, (b + 1) * BLOCK)
            products = [
                jnp.dot(var[row, part], rhs[3 * b + v], preferred_element_type=f32)
                for v, var in enumerate((var0, var1, var2))
            ]
            if b:
                products.append(jnp.dot(var3[row, :], rhs[6], preferred_element_type=f32))
            for i in range(per_block):
                h = m * per_block + i
                own = slice(i * HEADDIM, (i + 1) * HEADDIM)
                at = pl.ds(pl.multiple_of(h * HEADDIM, HEADDIM), HEADDIM)
                out = skip_ref[h] * val_t[at, part].astype(f32)
                for v, product in enumerate(products):
                    out = out + rows_t[v, pl.ds(h, 1), part] * product[own]
                acc_t[at, part] = out
        return c

    lax.fori_loop(0, ch // BLOCK, inner, 0)

    wait_bytes(dz.at[pl.ds(0, nz - 1)], z_r.at[1])
    my_head = my_c * half_heads + place(my_z) * SHARD // HEADDIM
    rows_d = [dz[z] for z in range(nz)]
    decay = [[lane_pick(r, my_head) for r in rows_d]]
    for j in range(bz):
        decay.append([decay[j][m + 1] * decay[j][m] for m in range(0, nz >> j, 2)])
    row_product = rows_d[0]
    for z in range(1, nz):
        row_product = row_product * rows_d[z]
    drow[...] = row_product

    def send_x_decay(i, c):
        to = lax.rem(my_x + far_first(i, nx), nx)
        remote(drow, dxr.at[my_x], x_s.at[1], x_r.at[1], {"seq_0": to}).start()
        return c

    lax.fori_loop(0, nx - 1, send_x_decay, 0)
    dxr[my_x] = drow[...]
    wait_bytes(inz.at[pl.ds(0, nz - 1)], z_r.at[0])
    state = [[inz[z].astype(f32) for z in range(nz)]]
    for j in range(bz):
        state.append([state[j][m + 1] + decay[j][m + 1] * state[j][m] for m in range(0, nz >> j, 2)])
    outz[total_z] = state[bz][0].astype(bf)
    for j in range(bz):
        for m in range(0, nz >> j, 2):
            outz[base_z[j] + m // 2] = state[j][m].astype(bf)

    def send_x(i, c):
        to = lax.rem(my_x + far_first(i, nx), nx)
        remote(outz.at[total_z], xr.at[my_x], x_s.at[0], x_r.at[0], {"seq_0": to}).start()
        return c

    lax.fori_loop(0, nx - 1, send_x, 0)
    xr[my_x] = outz[total_z]
    near = 2

    def pass_row(j, o):
        shard = rs.at[bz + j, my_c, lax.rem(my_z, 4) * quads + lax.rem(my_z // 4 + quads - o, quads)]
        if o:
            wait_bytes(shard, row_r.at[j * quads + o])
        for to in (2 if j % 2 == 0 else nz - 2, 1, nz - 1):
            remote(shard, shard, two_s.at[j], two_r.at[j], {"seq_1": lax.rem(my_z + to, nz)}).start()
    quarter = my_z // 4

    def send_levels_quad():
        for j in range(near, bz):
            for o in sorted(range(1, quads), key=lambda o: -min(o, quads - o)):
                to = lax.rem(my_z + 4 * o, nz)
                @pl.when(bit(to, j))
                def _():
                    remote(
                        outz.at[base_z[j] + to // (1 << (j + 1))], rs.at[j, my_c, place(my_z)],
                        lev_s.at[j], lev_r.at[j], {"seq_1": to},
                    ).start()

            @pl.when(bit(my_z, j))
            def _():
                rs[j, my_c, place(my_z)] = outz[base_z[j] + my_z // (1 << (j + 1))]

    def pass_levels_quad():
        for j in range(near, bz):
            @pl.when(bit(my_z, j))
            def _():
                wait_bytes(rs.at[j, 0, pl.ds(0, quads - 1)], lev_r.at[j])
                for o in range(1, 4):
                    part = rs.at[j, my_c, pl.ds(lax.rem(my_z, 4) * quads, quads)]
                    to = quarter * 4 + lax.rem(my_z + o, 4)
                    remote(part, part, two_s.at[bx + j - near], two_r.at[bx + j - near], {"seq_1": to}).start()

    def send_levels_z(wanted):
        def step(i, c):
            to = lax.rem(my_z + far_first(i, nz), nz)
            for j in wanted:
                @pl.when(bit(to, j))
                def _():
                    remote(
                        outz.at[base_z[j] + to // (1 << (j + 1))], rs.at[j, my_c, place(my_z)],
                        lev_s.at[j], lev_r.at[j], {"seq_1": to},
                    ).start()
            return c

        lax.fori_loop(0, nz - 1, step, 0)
        for j in wanted:
            @pl.when(bit(my_z, j))
            def _():
                rs[j, my_c, place(my_z)] = outz[base_z[j] + my_z // (1 << (j + 1))]

    send_levels_quad()

    one = jnp.ones_like(d0)
    mine = jnp.where(first, one, d0)

    def weigh(v, lead):
        column = jnp.sum(jnp.where(square_mask, lead, 0.0), axis=1, keepdims=True)
        rows_t[v] = rows_t[v] * column

    for j in range(bz):
        low = my_z // (1 << j) * (1 << j)
        product = mine
        for z in range(nz):
            product = product * jnp.where((z >= low) & (z < my_z), rows_d[z], one)
        weigh(low_bits + 2 + j, product)
    row_lead = mine
    for z in range(nz):
        row_lead = row_lead * jnp.where(z < my_z, rows_d[z], one)

    wait_bytes(dxr.at[pl.ds(0, nx - 1)], x_r.at[1])
    rows_x = [dxr[x] for x in range(nx)]
    decay = [lane_pick(r, my_head) for r in rows_x]
    wait_bytes(xr.at[pl.ds(0, nx - 1)], x_r.at[0])
    state = [xr[x].astype(f32) for x in range(nx)]
    for j in range(bx):
        for m in range(0, nx >> j, 2):
            outx[base_x[j] + m // 2] = state[m].astype(bf)
        state = [state[m + 1] + decay[m + 1] * state[m] for m in range(0, nx >> j, 2)]
        decay = [decay[m + 1] * decay[m] for m in range(0, nx >> j, 2)]
    for o in sorted(range(quads), key=lambda o: -min(o, quads - o)):
        for j in range(bx):
            @pl.when(bit(my_x, j))
            def _():
                at = base_x[j] + my_x // (1 << (j + 1))
                mine_at = rs.at[bz + j, my_c, place(my_z)]
                if o:
                    to = lax.rem(my_z + 4 * o, nz)
                    remote(outx.at[at], mine_at, lev_s.at[bz + j], row_r.at[j * quads + o], {"seq_1": to}).start()
                else:
                    rs[bz + j, my_c, place(my_z)] = outx[at]
                    pass_row(j, 0)

    send_levels_z(range(1, near))
    for j in range(bx):
        low = my_x // (1 << j) * (1 << j)
        product = row_lead
        for x in range(nx):
            product = product * jnp.where((x >= low) & (x < my_x), rows_x[x], one)
        weigh(low_bits + 2 + bz + j, product)

    loads[9].wait()

    def gate_pair(k, c):
        at = pl.multiple_of(k * 128, 128)
        g = gate_v[:, pl.ds(at, 128)].astype(f32)
        silu_t[pl.ds(at, 128), :] = (g / (1.0 + jnp.exp(-g))).T
        return c

    lax.fori_loop(0, heads // 2, gate_pair, 0)

    pass_levels_quad()
    for o in sorted(range(1, quads), key=lambda o: min(o, quads - o)):
        for j in range(bx):
            @pl.when(bit(my_x, j))
            def _():
                pass_row(j, o)

    def apply(v, ref, rows):
        def step(m, c):
            for b in range(tok // BLOCK):
                part = slice(b * BLOCK, (b + 1) * BLOCK)
                block = ref(m)
                product = nt_dot(block, query_ref[part, :])
                for i in range(per_block):
                    h = m * per_block + i
                    at = pl.ds(pl.multiple_of(h * HEADDIM, HEADDIM), HEADDIM)
                    acc_t[at, part] += rows_t[v, pl.ds(h, 1), part] * product[i * HEADDIM : (i + 1) * HEADDIM]
            return c

        lax.fori_loop(rows[0], rows[1], step, 0)

    chunks = ch // BLOCK
    n = BLOCK // SHARD
    half_chunks = chunks // 2

    @pl.when(jnp.logical_not(first))
    def _():
        apply(low_bits + 1, lambda m: pe[pl.ds(m * n, n)].reshape(BLOCK, 128), (0, chunks))

    def swap(v):
        return remote(rs.at[v, my_c], rs.at[v, my_c], fin_s.at[v], fin_r.at[v], {"seq_2": other})

    def level_block(v):
        if half_chunks:
            return lambda m: rs[v, m // half_chunks, pl.ds(lax.rem(m, half_chunks) * n, n)].reshape(BLOCK, 128)
        return lambda m: jnp.concatenate([rs[v, 0].reshape(BLOCK // 2, 128), rs[v, 1].reshape(BLOCK // 2, 128)])

    def arrive_z(j):
        @pl.when(bit(my_z, j))
        def _():
            if j == 0:
                wait_bytes(rs.at[0, 0], lev_r.at[0])
            elif j < near:
                wait_bytes(rs.at[j, 0, pl.ds(0, nz - 1)], lev_r.at[j])
            else:
                wait_bytes(rs.at[j, 0, pl.ds(0, 3 * quads)], two_r.at[bx + j - near])
            swap(j).start()

    def apply_z(j):
        @pl.when(bit(my_z, j))
        def _():
            swap(j).wait()
            apply(low_bits + 2 + j, level_block(j), (0, chunks))

    early = [0] + list(range(near, bz))
    for j in early:
        arrive_z(j)
    for j in early:
        apply_z(j)
    for j in range(bx):
        @pl.when(bit(my_x, j))
        def _():
            wait_bytes(rs.at[bz + j, 0, pl.ds(0, 3 * quads)], two_r.at[j])
            swap(bz + j).start()
    for j in range(1, near):
        arrive_z(j)
    if half_chunks:
        for j in range(bx):
            @pl.when(bit(my_x, j))
            def _():
                v = bz + j
                apply(low_bits + 2 + v, level_block(v), (my_c * half_chunks, (my_c + 1) * half_chunks))
    for j in range(1, near):
        apply_z(j)
    for j in range(bx):
        @pl.when(bit(my_x, j))
        def _():
            v = bz + j
            swap(v).wait()
            if half_chunks:
                apply(low_bits + 2 + v, level_block(v), (other * half_chunks, (other + 1) * half_chunks))
            else:
                apply(low_bits + 2 + v, level_block(v), (0, chunks))

    def gate_rows(k, squares):
        row = pl.ds(pl.multiple_of(k * 128, 128), 128)
        g = acc_t[row, :] * silu_t[row, :]
        acc_t[row, :] = g
        return squares + jnp.sum(g * g, axis=0, keepdims=True)

    sq_own[...] = lax.fori_loop(0, heads // 2, gate_rows, jnp.zeros((1, tok), f32))

    def send_y(o, c):
        remote(sq_own, sq.at[my_y], y_s, y_r, {"head": lax.rem(my_y + o, ny)}).start()
        return c

    lax.fori_loop(1, ny, send_y, 0)
    sq[my_y] = sq_own[...]

    for k in range(heads // 2):
        part = pl.ds(k * 128, 128)
        val_v[:, part] = acc_t[part, :].T.astype(bf)
        if k:
            part = pl.ds(k * 128 - 128, 128)
            pltpu.make_async_copy(val_v.at[:, part], gated_out.at[:, part], out_s).start()

    part = pl.ds(ch - 128, 128)
    pltpu.make_async_copy(val_v.at[:, part], gated_out.at[:, part], out_s).start()

    wait_bytes(a_half.at[pl.ds(0, nz - 1)], z_s.at[0])
    wait_bytes(dz.at[pl.ds(0, nz - 1)], z_s.at[1])
    wait_bytes(xr.at[pl.ds(0, nx - 1)], x_s.at[0])
    wait_bytes(dxr.at[pl.ds(0, nx - 1)], x_s.at[1])
    for j in range(near, bz):
        reached = (bit(my_z, j)).astype(jnp.int32)
        for count in range(quads // 2 - 1, quads // 2 + 1):
            @pl.when((quads // 2 - reached == count) & (count > 0))
            def _():
                wait_bytes(inz.at[pl.ds(0, max(count, 1))], lev_s.at[j])

        @pl.when(bit(my_z, j))
        def _():
            wait_bytes(rs.at[j, 0, pl.ds(0, 3 * quads)], two_s.at[bx + j - near])
    @pl.when(jnp.logical_not(bit(my_z, 0)))
    def _():
        wait_bytes(a_half, lev_s.at[0])

    for j in range(1, near):
        @pl.when(bit(my_z, j))
        def _():
            if nz // 2 > 1:
                wait_bytes(inz.at[pl.ds(0, nz // 2 - 1)], lev_s.at[j])

        @pl.when(jnp.logical_not(bit(my_z, j)))
        def _():
            wait_bytes(inz.at[pl.ds(0, nz // 2)], lev_s.at[j])
    for j in range(bx):
        @pl.when(bit(my_x, j))
        def _():
            if quads > 1:
                wait_bytes(inz.at[pl.ds(0, quads - 1)], lev_s.at[bz + j])
            wait_bytes(rs.at[bz + j, 0, pl.ds(0, 3 * quads)], two_s.at[j])
    if ny > 1:
        wait_bytes(sq.at[pl.ds(0, ny - 1)], y_s)
        wait_bytes(sq.at[pl.ds(0, ny - 1)], y_r)
    squares = sq[0]
    for y in range(1, ny):
        squares = squares + sq[y]
    wait_bytes(val_v, out_s)
    square_out[...] = squares


def finish_kernel(count, gated_hbm, square_hbm, gain_hbm, out_hbm, gated, done, squares, gain, small_s, in_s, out_s):
    tok, ch = gated.shape
    rows = tok // 8
    small = [
        pltpu.make_async_copy(square_hbm, squares, small_s.at[0]), pltpu.make_async_copy(gain_hbm, gain, small_s.at[1]),
    ]
    parts = [pl.ds(k * rows, rows) for k in range(8)]
    loads = [pltpu.make_async_copy(gated_hbm.at[part], gated.at[part], in_s.at[k]) for k, part in enumerate(parts)]
    stores = [pltpu.make_async_copy(done.at[part], out_hbm.at[part], out_s.at[k]) for k, part in enumerate(parts)]
    for copy in small + loads:
        copy.start()
    for copy in small:
        copy.wait()
    scale = lax.rsqrt(squares[...] / count + epsilon)
    column = jnp.broadcast_to(scale, (128, tok)).T[:, :1]
    weight = gain[...]
    for k, part in enumerate(parts):
        loads[k].wait()
        done[part, :] = (gated[part, :].astype(jnp.float32) * column[k * rows : (k + 1) * rows] * weight).astype(jnp.bfloat16)
        if k:
            stores[k - 1].start()
    stores[7].start()
    for copy in stores:
        copy.wait()


def local(
    values_in, gate_in, key_proj, query_proj, step_size, log_decay, skip_weight, norm_gain, level_table, level_pick, doc_start,
):
    nx, nz, ny = lax.axis_size("seq_0"), lax.axis_size("seq_1"), lax.axis_size("head")
    tok, ch = values_in.shape
    heads = step_size.shape[1]
    width = key_proj.shape[1]
    levels_out = nz.bit_length() - 1 + nx.bit_length() - 1
    bx = nx.bit_length() - 1
    table_levels = level_table.shape[2]
    bf, f32 = jnp.bfloat16, jnp.float32
    vmem = pl.BlockSpec(memory_space=pltpu.VMEM)
    hbm = pl.BlockSpec(memory_space=pltpu.HBM)
    dma = pltpu.SemaphoreType.DMA
    V = pltpu.VMEM
    gated, squares = pl.pallas_call(
        functools.partial(layer_kernel, nx, nz, ny),
        name="layer",
        out_shape=(jax.ShapeDtypeStruct((tok, ch), bf), jax.ShapeDtypeStruct((1, tok), f32)),
        in_specs=[hbm] * 10,
        out_specs=(hbm, vmem),
        scratch_shapes=[
            V((tok, width), bf), V((tok, width), bf), V((heads, tok), f32), V((table_levels, level_table.shape[0], heads), f32),
            V((1, tok), jnp.int32), pltpu.SMEM((doc_start.shape[0],), jnp.int32), pltpu.SMEM((heads,), f32),
            V((tok, ch), bf), V((tok, ch), bf), V((ch, tok), bf), V((ch, tok), bf),
            V((ch, tok), bf), V((ch, tok), bf), V((ch, tok), bf), V((ch, BLOCK), bf),
            V((7, BLOCK, BLOCK), bf), V((ch, tok), f32), V((ch, tok), f32),
            V((heads, tok), f32), V((heads, tok), f32), V((4, heads, tok), f32), V((table_levels, heads, tok), f32),
            V((2 * nz, SHARD, width), bf), V((1, 128), f32), V((2 * nz, SHARD, width), bf), V((1, 128), f32),
            V((nz, SHARD, width), bf), V((1, 128), f32), V((nz, SHARD, width), bf), V((nz, 1, 128), f32),
            V((nz, SHARD, width), bf), V((1, 128), f32), V((nx, SHARD, width), bf), V((nx, 1, 128), f32),
            V((nx, SHARD, width), bf), V((levels_out, 2, nz, SHARD, width), bf),
            V((1, tok), f32), V((ny, 1, tok), f32),
            dma((10,)), dma((2,)), dma((2,)), dma((2,)), dma((2,)), dma((2,)), dma((2,)),
            dma((levels_out,)), dma((levels_out,)), dma((2 * levels_out,)), dma((2 * levels_out,)), dma((bx * nz // 4,)), dma((levels_out,)), dma((levels_out,)),
            dma, dma, dma,
        ],
        compiler_params=pltpu.CompilerParams(collective_id=0, has_side_effects=True, vmem_limit_bytes=67043328),
    )(
        values_in, gate_in, key_proj, query_proj, step_size.T, log_decay.T, level_table.transpose(2, 0, 1),
        level_pick.reshape(1, tok), doc_start, skip_weight,
    )
    return pl.pallas_call(
        functools.partial(finish_kernel, ch * ny),
        name="finish",
        out_shape=jax.ShapeDtypeStruct((tok, ch), bf),
        in_specs=[hbm] * 3,
        out_specs=hbm,
        scratch_shapes=[V((tok, ch), bf), V((tok, ch), bf), V((1, tok), f32), V((1, ch), f32), dma((2,)), dma((8,)), dma((8,))],
        compiler_params=pltpu.CompilerParams(vmem_limit_bytes=67043328),
    )(gated, squares, norm_gain.reshape(1, ch))


def solution(mesh):
    split = Mesh(
        mesh.devices.reshape(4, 16, 2, mesh.shape["head"]), ("seq_0", "seq_1", "seq_2", "head")
    )
    return on_mesh(split)


def on_mesh(split):
    placed = (
        P(SEQ, "head"),
        P(SEQ, "head"),
        P(SEQ, None),
        P(SEQ, None),
        P(SEQ, "head"),
        P(SEQ, "head"),
        P("head"),
        P("head"),
        P(None, "head", None),
        P(SEQ),
        P(SEQ),
    )
    return jax.shard_map(local, mesh=split, in_specs=placed, out_specs=P(SEQ, "head"), check_vma=False)
```

```python
import functools

import jax
import jax.numpy as jnp
from jax import lax
from jax.experimental import pallas as pl
from jax.experimental.pallas import tpu as pltpu
from jax.sharding import Mesh
from jax.sharding import PartitionSpec as P

HEADDIM = 64
STRETCH = 64
BLOCK = 256
SEQ = ("seq_0", "seq_1", "seq_2")
epsilon = 1e-06

MESH_ID = pl.DeviceIdType.MESH
SHARD = 32


def remote(src, dst, send, recv, where):
    return pltpu.make_async_remote_copy(
        src_ref=src, dst_ref=dst, send_sem=send, recv_sem=recv, device_id=where, device_id_type=MESH_ID
    )


def wait_bytes(ref, sem):
    pltpu.make_async_copy(ref, ref, sem).wait()


def lane_pick(rows, lane):
    lanes = lax.broadcasted_iota(jnp.int32, rows.shape, 1)
    return jnp.sum(jnp.where(lanes == lane, rows, 0.0), axis=1, keepdims=True)


def levels_base(size, bits):
    base, at = [], 0
    for j in range(bits):
        base.append(at)
        at += size >> (j + 1)
    return base, at


def bit(value, j):
    return lax.rem(value // (1 << j), 2) == 1


def nt_dot(a, b):
    return lax.dot_general(a, b, (((1,), (1,)), ((), ())), preferred_element_type=jnp.float32)


def layer_kernel(
    nx, nz, ny, val_hbm, gate_hbm, key_hbm, query_hbm, step_hbm, log_hbm, table_hbm, pick_hbm, doc_hbm, skip_hbm,
    gated_out, square_out,
    key_ref, query_ref, log_ref, table_ref, pick_ref, doc_ref, skip_ref,
    val_v, gate_v, val_t, scaled_t, var0, var1, var2, var3, rhs, acc_t, silu_t, steps, cuts, rows_s, rows_t,
    e_buf, d_buf, pe, pd, a_half, dc, inz, dz, outz, drow, xr, dxr, outx, rs, sq_own, sq,
    load_s, pair_s, pair_r, z_s, z_r, x_s, x_r, lev_s, lev_r, two_s, two_r, row_r, fin_s, fin_r, y_s, y_r, out_s,
):
    f32, bf = jnp.float32, jnp.bfloat16
    tok, ch = val_v.shape
    heads = ch // HEADDIM
    per_span = tok // STRETCH
    low_bits = per_span.bit_length() - 1
    bz, bx = nz.bit_length() - 1, nx.bit_length() - 1
    quads = nz // 4
    base_z, total_z = levels_base(nz, bz)
    base_x, _ = levels_base(nx, bx)
    my_x, my_z, my_c = lax.axis_index("seq_0"), lax.axis_index("seq_1"), lax.axis_index("seq_2")
    my_y = lax.axis_index("head")
    other = 1 - my_c
    half_heads = heads // 2

    def place(z):
        return lax.rem(z, 4) * quads + z // 4

    def far_first(i, size):
        return size // 2 + (i + 1) // 2 * (1 - 2 * lax.rem(i, 2))

    barrier = pltpu.get_barrier_semaphore()

    def greet(axis, mine, size):
        def step(i, c):
            to = lax.rem(mine + far_first(i, size), size)
            pl.semaphore_signal(barrier, inc=1, device_id={axis: to}, device_id_type=MESH_ID)
            return c

        lax.fori_loop(0, size - 1, step, 0)

    greet("seq_1", my_z, nz)
    greet("seq_0", my_x, nx)
    greet("head", my_y, ny)
    pl.semaphore_signal(barrier, inc=1, device_id={"seq_2": other}, device_id_type=MESH_ID)

    loads = [
        pltpu.make_async_copy(src, dst, load_s.at[i])
        for i, (src, dst) in enumerate((
            (log_hbm, log_ref), (doc_hbm, doc_ref), (val_hbm, val_v), (step_hbm, steps), (key_hbm, key_ref),
            (query_hbm, query_ref), (table_hbm, table_ref), (pick_hbm, pick_ref), (skip_hbm, skip_ref), (gate_hbm, gate_v),
        ))
    ]
    for load in loads:
        load.start()
    loads[0].wait()
    loads[1].wait()

    total = log_ref[...]
    lane = lax.broadcasted_iota(jnp.int32, (heads, tok), 1)
    shift = 1
    while shift < tok:
        total = total + jnp.where(lane >= shift, pltpu.roll(total, shift, 1), 0.0)
        shift *= 2
    cuts[...] = total
    lane1 = lax.broadcasted_iota(jnp.int32, (1, tok), 1)
    count = doc_ref[0]
    docs = jnp.broadcast_to(count, (1, tok))
    for c in range(1, per_span):
        count = count + doc_ref[c]
        docs = jnp.where(lane1 >= c * STRETCH, count, docs)
    last = tok - 1
    end_log = total[:, last:]
    rows_s[0] = jnp.exp(end_log - total) * (docs == docs[:, last:]).astype(f32)
    square_mask = lax.broadcasted_iota(jnp.int32, (heads, 128), 0) == lax.broadcasted_iota(jnp.int32, (heads, 128), 1)
    end_decay = jnp.exp(end_log) * (docs[:, last:] == 0).astype(f32)
    d_buf[...] = jnp.sum(jnp.where(square_mask, end_decay, 0.0), axis=0, keepdims=True)

    for load in loads[2:5]:
        load.wait()

    def end_pair(k, c):
        at = pl.multiple_of(k * 128, 128)
        v = val_v[:, pl.ds(at, 128)].astype(f32).T
        val_t[pl.ds(at, 128), :] = v.astype(bf)
        for i in range(2):
            h = 2 * k + i
            row = pl.ds(pl.multiple_of(h * HEADDIM, HEADDIM), HEADDIM)
            scaled = (v[i * HEADDIM : (i + 1) * HEADDIM] * steps[pl.ds(h, 1), :]).astype(bf)
            scaled_t[row, :] = scaled
            var0[row, :] = (scaled.astype(f32) * rows_s[0, pl.ds(h, 1), :]).astype(bf)
        return c

    lax.fori_loop(0, heads // 2, end_pair, 0)
    per = SHARD

    def end_dot(m, c):
        n = BLOCK // per
        part = jnp.dot(
            var0[pl.ds(pl.multiple_of(m * BLOCK, BLOCK), BLOCK), :], key_ref[...], preferred_element_type=f32
        ).astype(bf)
        for i in range(n):
            e_buf[m * n + i] = part[i * per : (i + 1) * per]
        return c

    lax.fori_loop(0, ch // BLOCK, end_dot, 0)

    pl.semaphore_wait(barrier, nz + nx + ny - 2)

    ce = remote(e_buf, pe, pair_s.at[0], pair_r.at[0], {"seq_2": other})
    cd = remote(d_buf, pd, pair_s.at[1], pair_r.at[1], {"seq_2": other})
    ce.start()
    cd.start()

    for load in loads[5:9]:
        load.wait()
    picks = jnp.broadcast_to(pick_ref[...], (heads, tok))
    levels, groups, _ = table_ref.shape
    for v in range(levels):
        w = jnp.zeros((heads, tok), f32)
        columns = table_ref[v].T
        for g in range(groups):
            w = jnp.where(picks == g, columns[:, g : g + 1], w)
        rows_t[v] = w

    cd.wait()
    first = my_c == 0
    d_own, d_oth = d_buf[...], pd[...]
    d0 = jnp.where(first, d_own, d_oth)
    d1 = jnp.where(first, d_oth, d_own)
    dc[...] = d0 * d1
    scales = [lane_pick(d1, my_c * half_heads + h) for h in range(half_heads)]
    ce.wait()

    def merge_pair(s, c):
        own = e_buf[my_c * nz + s].astype(f32)
        oth = pe[my_c * nz + s].astype(f32)
        e0 = jnp.where(first, own, oth)
        e1 = jnp.where(first, oth, own)
        a_half[s] = (e1 + scales[s * SHARD // HEADDIM] * e0).astype(bf)
        return c

    for s in range(nz):
        merge_pair(s, 0)

    def send_z(i, c):
        to = lax.rem(my_z + far_first(i, nz), nz)
        remote(a_half.at[place(to)], inz.at[my_z], z_s.at[0], z_r.at[0], {"seq_1": to}).start()
        remote(dc, dz.at[my_z], z_s.at[1], z_r.at[1], {"seq_1": to}).start()
        return c

    lax.fori_loop(0, nz - 1, send_z, 0)
    step_up = remote(a_half, rs.at[0, my_c], lev_s.at[0], lev_r.at[0], {"seq_1": lax.rem(my_z + 1, nz)})

    @pl.when(jnp.logical_not(bit(my_z, 0)))
    def _():
        step_up.start()

    inz[my_z] = a_half[place(my_z)]
    dz[my_z] = dc[...]

    total = cuts[...]
    for v in range(low_bits + 1):
        width = STRETCH << max(v - 1, 0)
        mark, mark_doc = jnp.zeros((heads, tok), f32), jnp.zeros((1, tok), jnp.int32)
        if v == 0:
            for c in range(per_span):
                at = c * STRETCH + STRETCH // 2 - 1
                mark = jnp.where(lane >= c * STRETCH, total[:, at : at + 1], mark)
            rows_s[0] = jnp.exp(mark - total)
            rows_t[0] = rows_t[0] * jnp.exp(total - mark)
        else:
            for c in range(tok // (2 * width)):
                at = (2 * c + 1) * width - 1
                mark = jnp.where(lane >= 2 * c * width, total[:, at : at + 1], mark)
                mark_doc = jnp.where(lane1 >= 2 * c * width, docs[:, at : at + 1], mark_doc)
            upper = lane // width % 2 == 1
            same = (docs == mark_doc).astype(f32)
            rows_s[v] = jnp.where(upper, 0.0, jnp.exp(jnp.minimum(mark - total, 0.0)) * same)
            rows_t[v] = jnp.where(upper, rows_t[v] * jnp.exp(jnp.minimum(total - mark, 0.0)) * same, 0.0)
    reach = jnp.exp(total) * (docs == 0).astype(f32)
    for v in range(low_bits + 1, levels):
        rows_t[v] = rows_t[v] * reach

    source = lax.broadcasted_iota(jnp.int32, (BLOCK, BLOCK), 0)
    reader = lax.broadcasted_iota(jnp.int32, (BLOCK, BLOCK), 1)
    differ = jnp.bitwise_xor(source // STRETCH, reader // STRETCH)
    causal = source <= reader
    for b in range(tok // BLOCK):
        part = slice(b * BLOCK, (b + 1) * BLOCK)
        scores = jnp.where(causal, nt_dot(key_ref[part, :], query_ref[part, :]), 0.0)
        rhs[3 * b] = jnp.where(differ == 0, scores, 0.0).astype(bf)
        rhs[3 * b + 1] = jnp.where(differ == 1, scores, 0.0).astype(bf)
        rhs[3 * b + 2] = jnp.where(differ >= 2, scores, 0.0).astype(bf)
    rhs[6] = nt_dot(key_ref[:BLOCK, :], query_ref[BLOCK:, :]).astype(bf)

    def variants(h, c):
        row = pl.ds(pl.multiple_of(h * HEADDIM, HEADDIM), HEADDIM)
        scaled = scaled_t[row, :].astype(f32)
        var0[row, :] = (scaled * rows_s[0, pl.ds(h, 1), :]).astype(bf)
        var1[row, :] = (scaled * rows_s[1, pl.ds(h, 1), :]).astype(bf)
        var2[row, :] = (scaled * rows_s[2, pl.ds(h, 1), :]).astype(bf)
        var3[row, :] = (scaled[:, :BLOCK] * rows_s[3, pl.ds(h, 1), :BLOCK]).astype(bf)
        return c

    lax.fori_loop(0, heads, variants, 0)
    per_block = BLOCK // HEADDIM

    def inner(m, c):
        row = pl.ds(pl.multiple_of(m * BLOCK, BLOCK), BLOCK)
        for b in range(tok // BLOCK):
            part = slice(b * BLOCK, (b + 1) * BLOCK)
            products = [
                jnp.dot(var[row, part], rhs[3 * b + v], preferred_element_type=f32)
                for v, var in enumerate((var0, var1, var2))
            ]
            if b:
                products.append(jnp.dot(var3[row, :], rhs[6], preferred_element_type=f32))
            for i in range(per_block):
                h = m * per_block + i
                own = slice(i * HEADDIM, (i + 1) * HEADDIM)
                at = pl.ds(pl.multiple_of(h * HEADDIM, HEADDIM), HEADDIM)
                out = skip_ref[h] * val_t[at, part].astype(f32)
                for v, product in enumerate(products):
                    out = out + rows_t[v, pl.ds(h, 1), part] * product[own]
                acc_t[at, part] = out
        return c

    lax.fori_loop(0, ch // BLOCK, inner, 0)

    wait_bytes(dz.at[pl.ds(0, nz - 1)], z_r.at[1])
    my_head = my_c * half_heads + place(my_z) * SHARD // HEADDIM
    rows_d = [dz[z] for z in range(nz)]
    decay = [[lane_pick(r, my_head) for r in rows_d]]
    for j in range(bz):
        decay.append([decay[j][m + 1] * decay[j][m] for m in range(0, nz >> j, 2)])
    row_product = rows_d[0]
    for z in range(1, nz):
        row_product = row_product * rows_d[z]
    drow[...] = row_product

    def send_x_decay(i, c):
        to = lax.rem(my_x + far_first(i, nx), nx)
        remote(drow, dxr.at[my_x], x_s.at[1], x_r.at[1], {"seq_0": to}).start()
        return c

    lax.fori_loop(0, nx - 1, send_x_decay, 0)
    dxr[my_x] = drow[...]
    wait_bytes(inz.at[pl.ds(0, nz - 1)], z_r.at[0])
    state = [[inz[z].astype(f32) for z in range(nz)]]
    for j in range(bz):
        state.append([state[j][m + 1] + decay[j][m + 1] * state[j][m] for m in range(0, nz >> j, 2)])
    outz[total_z] = state[bz][0].astype(bf)
    for j in range(bz):
        for m in range(0, nz >> j, 2):
            outz[base_z[j] + m // 2] = state[j][m].astype(bf)

    def send_x(i, c):
        to = lax.rem(my_x + far_first(i, nx), nx)
        remote(outz.at[total_z], xr.at[my_x], x_s.at[0], x_r.at[0], {"seq_0": to}).start()
        return c

    lax.fori_loop(0, nx - 1, send_x, 0)
    xr[my_x] = outz[total_z]
    near = 2

    def pass_row(j, o):
        shard = rs.at[bz + j, my_c, lax.rem(my_z, 4) * quads + lax.rem(my_z // 4 + quads - o, quads)]
        if o:
            wait_bytes(shard, row_r.at[j * quads + o])
        for to in (2 if j % 2 == 0 else nz - 2, 1, nz - 1):
            remote(shard, shard, two_s.at[j], two_r.at[j], {"seq_1": lax.rem(my_z + to, nz)}).start()
    quarter = my_z // 4

    def send_levels_quad():
        for o in sorted(range(1, quads), key=lambda o: -min(o, quads - o)):
            for j in range(near, bz):
                to = lax.rem(my_z + 4 * o, nz)
                @pl.when(bit(to, j))
                def _():
                    remote(
                        outz.at[base_z[j] + to // (1 << (j + 1))], rs.at[j, my_c, place(my_z)],
                        lev_s.at[j], lev_r.at[j], {"seq_1": to},
                    ).start()

        for j in range(near, bz):
            @pl.when(bit(my_z, j))
            def _():
                rs[j, my_c, place(my_z)] = outz[base_z[j] + my_z // (1 << (j + 1))]

    def pass_levels_quad():
        for j in range(near, bz):
            @pl.when(bit(my_z, j))
            def _():
                wait_bytes(rs.at[j, 0, pl.ds(0, quads - 1)], lev_r.at[j])
                for o in range(1, 4):
                    part = rs.at[j, my_c, pl.ds(lax.rem(my_z, 4) * quads, quads)]
                    to = quarter * 4 + lax.rem(my_z + o, 4)
                    remote(part, part, two_s.at[bx + j - near], two_r.at[bx + j - near], {"seq_1": to}).start()

    def send_levels_z(wanted):
        def step(i, c):
            to = lax.rem(my_z + far_first(i, nz), nz)
            for j in wanted:
                @pl.when(bit(to, j))
                def _():
                    remote(
                        outz.at[base_z[j] + to // (1 << (j + 1))], rs.at[j, my_c, place(my_z)],
                        lev_s.at[j], lev_r.at[j], {"seq_1": to},
                    ).start()
            return c

        lax.fori_loop(0, nz - 1, step, 0)
        for j in wanted:
            @pl.when(bit(my_z, j))
            def _():
                rs[j, my_c, place(my_z)] = outz[base_z[j] + my_z // (1 << (j + 1))]

    send_levels_quad()

    one = jnp.ones_like(d0)
    mine = jnp.where(first, one, d0)

    def weigh(v, lead):
        column = jnp.sum(jnp.where(square_mask, lead, 0.0), axis=1, keepdims=True)
        rows_t[v] = rows_t[v] * column

    for j in range(bz):
        low = my_z // (1 << j) * (1 << j)
        product = mine
        for z in range(nz):
            product = product * jnp.where((z >= low) & (z < my_z), rows_d[z], one)
        weigh(low_bits + 2 + j, product)
    row_lead = mine
    for z in range(nz):
        row_lead = row_lead * jnp.where(z < my_z, rows_d[z], one)

    wait_bytes(dxr.at[pl.ds(0, nx - 1)], x_r.at[1])
    rows_x = [dxr[x] for x in range(nx)]
    decay = [lane_pick(r, my_head) for r in rows_x]
    wait_bytes(xr.at[pl.ds(0, nx - 1)], x_r.at[0])
    state = [xr[x].astype(f32) for x in range(nx)]
    for j in range(bx):
        for m in range(0, nx >> j, 2):
            outx[base_x[j] + m // 2] = state[m].astype(bf)
        state = [state[m + 1] + decay[m + 1] * state[m] for m in range(0, nx >> j, 2)]
        decay = [decay[m + 1] * decay[m] for m in range(0, nx >> j, 2)]
    for o in sorted(range(quads), key=lambda o: -min(o, quads - o)):
        for j in range(bx):
            @pl.when(bit(my_x, j))
            def _():
                at = base_x[j] + my_x // (1 << (j + 1))
                mine_at = rs.at[bz + j, my_c, place(my_z)]
                if o:
                    to = lax.rem(my_z + 4 * o, nz)
                    remote(outx.at[at], mine_at, lev_s.at[bz + j], row_r.at[j * quads + o], {"seq_1": to}).start()
                else:
                    rs[bz + j, my_c, place(my_z)] = outx[at]
                    pass_row(j, 0)

    send_levels_z(range(1, near))
    for j in range(bx):
        low = my_x // (1 << j) * (1 << j)
        product = row_lead
        for x in range(nx):
            product = product * jnp.where((x >= low) & (x < my_x), rows_x[x], one)
        weigh(low_bits + 2 + bz + j, product)

    loads[9].wait()

    def gate_pair(k, c):
        at = pl.multiple_of(k * 128, 128)
        g = gate_v[:, pl.ds(at, 128)].astype(f32)
        silu_t[pl.ds(at, 128), :] = (g / (1.0 + jnp.exp(-g))).T
        return c

    lax.fori_loop(0, heads // 2, gate_pair, 0)

    pass_levels_quad()
    for o in sorted(range(1, quads), key=lambda o: min(o, quads - o)):
        for j in range(bx):
            @pl.when(bit(my_x, j))
            def _():
                pass_row(j, o)

    def apply(v, ref, rows):
        def step(m, c):
            for b in range(tok // BLOCK):
                part = slice(b * BLOCK, (b + 1) * BLOCK)
                block = ref(m)
                product = nt_dot(block, query_ref[part, :])
                for i in range(per_block):
                    h = m * per_block + i
                    at = pl.ds(pl.multiple_of(h * HEADDIM, HEADDIM), HEADDIM)
                    acc_t[at, part] += rows_t[v, pl.ds(h, 1), part] * product[i * HEADDIM : (i + 1) * HEADDIM]
            return c

        lax.fori_loop(rows[0], rows[1], step, 0)

    chunks = ch // BLOCK
    n = BLOCK // SHARD
    half_chunks = chunks // 2

    @pl.when(jnp.logical_not(first))
    def _():
        apply(low_bits + 1, lambda m: pe[pl.ds(m * n, n)].reshape(BLOCK, 128), (0, chunks))

    def swap(v):
        return remote(rs.at[v, my_c], rs.at[v, my_c], fin_s.at[v], fin_r.at[v], {"seq_2": other})

    def level_block(v):
        if half_chunks:
            return lambda m: rs[v, m // half_chunks, pl.ds(lax.rem(m, half_chunks) * n, n)].reshape(BLOCK, 128)
        return lambda m: jnp.concatenate([rs[v, 0].reshape(BLOCK // 2, 128), rs[v, 1].reshape(BLOCK // 2, 128)])

    def arrive_z(j):
        @pl.when(bit(my_z, j))
        def _():
            if j == 0:
                wait_bytes(rs.at[0, 0], lev_r.at[0])
            elif j < near:
                wait_bytes(rs.at[j, 0, pl.ds(0, nz - 1)], lev_r.at[j])
            else:
                wait_bytes(rs.at[j, 0, pl.ds(0, 3 * quads)], two_r.at[bx + j - near])
            swap(j).start()

    def apply_z(j):
        @pl.when(bit(my_z, j))
        def _():
            swap(j).wait()
            apply(low_bits + 2 + j, level_block(j), (0, chunks))

    early = [0] + list(range(near, bz))
    for j in early:
        arrive_z(j)
    for j in early:
        apply_z(j)
    for j in range(bx):
        @pl.when(bit(my_x, j))
        def _():
            wait_bytes(rs.at[bz + j, 0, pl.ds(0, 3 * quads)], two_r.at[j])
            swap(bz + j).start()
    for j in range(1, near):
        arrive_z(j)
    if half_chunks:
        for j in range(bx):
            @pl.when(bit(my_x, j))
            def _():
                v = bz + j
                apply(low_bits + 2 + v, level_block(v), (my_c * half_chunks, (my_c + 1) * half_chunks))
    for j in range(1, near):
        apply_z(j)
    for j in range(bx):
        @pl.when(bit(my_x, j))
        def _():
            v = bz + j
            swap(v).wait()
            if half_chunks:
                apply(low_bits + 2 + v, level_block(v), (other * half_chunks, (other + 1) * half_chunks))
            else:
                apply(low_bits + 2 + v, level_block(v), (0, chunks))

    def gate_rows(k, squares):
        row = pl.ds(pl.multiple_of(k * 128, 128), 128)
        g = acc_t[row, :] * silu_t[row, :]
        acc_t[row, :] = g
        return squares + jnp.sum(g * g, axis=0, keepdims=True)

    sq_own[...] = lax.fori_loop(0, heads // 2, gate_rows, jnp.zeros((1, tok), f32))

    def send_y(i, c):
        remote(sq_own, sq.at[my_y], y_s, y_r, {"head": lax.rem(my_y + far_first(i, ny), ny)}).start()
        return c

    lax.fori_loop(0, ny - 1, send_y, 0)
    sq[my_y] = sq_own[...]

    for k in range(heads // 2):
        part = pl.ds(k * 128, 128)
        val_v[:, part] = acc_t[part, :].T.astype(bf)
        if k:
            part = pl.ds(k * 128 - 128, 128)
            pltpu.make_async_copy(val_v.at[:, part], gated_out.at[:, part], out_s).start()

    part = pl.ds(ch - 128, 128)
    pltpu.make_async_copy(val_v.at[:, part], gated_out.at[:, part], out_s).start()

    wait_bytes(a_half.at[pl.ds(0, nz - 1)], z_s.at[0])
    wait_bytes(dz.at[pl.ds(0, nz - 1)], z_s.at[1])
    wait_bytes(xr.at[pl.ds(0, nx - 1)], x_s.at[0])
    wait_bytes(dxr.at[pl.ds(0, nx - 1)], x_s.at[1])
    for j in range(near, bz):
        reached = (bit(my_z, j)).astype(jnp.int32)
        for count in range(quads // 2 - 1, quads // 2 + 1):
            @pl.when((quads // 2 - reached == count) & (count > 0))
            def _():
                wait_bytes(inz.at[pl.ds(0, max(count, 1))], lev_s.at[j])

        @pl.when(bit(my_z, j))
        def _():
            wait_bytes(rs.at[j, 0, pl.ds(0, 3 * quads)], two_s.at[bx + j - near])
    @pl.when(jnp.logical_not(bit(my_z, 0)))
    def _():
        wait_bytes(a_half, lev_s.at[0])

    for j in range(1, near):
        @pl.when(bit(my_z, j))
        def _():
            if nz // 2 > 1:
                wait_bytes(inz.at[pl.ds(0, nz // 2 - 1)], lev_s.at[j])

        @pl.when(jnp.logical_not(bit(my_z, j)))
        def _():
            wait_bytes(inz.at[pl.ds(0, nz // 2)], lev_s.at[j])
    for j in range(bx):
        @pl.when(bit(my_x, j))
        def _():
            if quads > 1:
                wait_bytes(inz.at[pl.ds(0, quads - 1)], lev_s.at[bz + j])
            wait_bytes(rs.at[bz + j, 0, pl.ds(0, 3 * quads)], two_s.at[j])
    if ny > 1:
        wait_bytes(sq.at[pl.ds(0, ny - 1)], y_s)
        wait_bytes(sq.at[pl.ds(0, ny - 1)], y_r)
    squares = sq[0]
    for y in range(1, ny):
        squares = squares + sq[y]
    wait_bytes(val_v, out_s)
    square_out[...] = squares


def finish_kernel(count, gated_hbm, square_hbm, gain_hbm, out_hbm, gated, done, squares, gain, small_s, in_s, out_s):
    tok, ch = gated.shape
    rows = tok // 8
    small = [
        pltpu.make_async_copy(square_hbm, squares, small_s.at[0]), pltpu.make_async_copy(gain_hbm, gain, small_s.at[1]),
    ]
    parts = [pl.ds(k * rows, rows) for k in range(8)]
    loads = [pltpu.make_async_copy(gated_hbm.at[part], gated.at[part], in_s.at[k]) for k, part in enumerate(parts)]
    stores = [pltpu.make_async_copy(done.at[part], out_hbm.at[part], out_s.at[k]) for k, part in enumerate(parts)]
    for copy in small + loads:
        copy.start()
    for copy in small:
        copy.wait()
    scale = lax.rsqrt(squares[...] / count + epsilon)
    column = jnp.broadcast_to(scale, (128, tok)).T[:, :1]
    weight = gain[...]
    for k, part in enumerate(parts):
        loads[k].wait()
        done[part, :] = (gated[part, :].astype(jnp.float32) * column[k * rows : (k + 1) * rows] * weight).astype(jnp.bfloat16)
        if k:
            stores[k - 1].start()
    stores[7].start()
    for copy in stores:
        copy.wait()


def local(
    values_in, gate_in, key_proj, query_proj, step_size, log_decay, skip_weight, norm_gain, level_table, level_pick, doc_start,
):
    nx, nz, ny = lax.axis_size("seq_0"), lax.axis_size("seq_1"), lax.axis_size("head")
    tok, ch = values_in.shape
    heads = step_size.shape[1]
    width = key_proj.shape[1]
    levels_out = nz.bit_length() - 1 + nx.bit_length() - 1
    bx = nx.bit_length() - 1
    table_levels = level_table.shape[2]
    bf, f32 = jnp.bfloat16, jnp.float32
    vmem = pl.BlockSpec(memory_space=pltpu.VMEM)
    hbm = pl.BlockSpec(memory_space=pltpu.HBM)
    dma = pltpu.SemaphoreType.DMA
    V = pltpu.VMEM
    gated, squares = pl.pallas_call(
        functools.partial(layer_kernel, nx, nz, ny),
        name="layer",
        out_shape=(jax.ShapeDtypeStruct((tok, ch), bf), jax.ShapeDtypeStruct((1, tok), f32)),
        in_specs=[hbm] * 10,
        out_specs=(hbm, vmem),
        scratch_shapes=[
            V((tok, width), bf), V((tok, width), bf), V((heads, tok), f32), V((table_levels, level_table.shape[0], heads), f32),
            V((1, tok), jnp.int32), pltpu.SMEM((doc_start.shape[0],), jnp.int32), pltpu.SMEM((heads,), f32),
            V((tok, ch), bf), V((tok, ch), bf), V((ch, tok), bf), V((ch, tok), bf),
            V((ch, tok), bf), V((ch, tok), bf), V((ch, tok), bf), V((ch, BLOCK), bf),
            V((7, BLOCK, BLOCK), bf), V((ch, tok), f32), V((ch, tok), f32),
            V((heads, tok), f32), V((heads, tok), f32), V((4, heads, tok), f32), V((table_levels, heads, tok), f32),
            V((2 * nz, SHARD, width), bf), V((1, 128), f32), V((2 * nz, SHARD, width), bf), V((1, 128), f32),
            V((nz, SHARD, width), bf), V((1, 128), f32), V((nz, SHARD, width), bf), V((nz, 1, 128), f32),
            V((nz, SHARD, width), bf), V((1, 128), f32), V((nx, SHARD, width), bf), V((nx, 1, 128), f32),
            V((nx, SHARD, width), bf), V((levels_out, 2, nz, SHARD, width), bf),
            V((1, tok), f32), V((ny, 1, tok), f32),
            dma((10,)), dma((2,)), dma((2,)), dma((2,)), dma((2,)), dma((2,)), dma((2,)),
            dma((levels_out,)), dma((levels_out,)), dma((2 * levels_out,)), dma((2 * levels_out,)), dma((bx * nz // 4,)), dma((levels_out,)), dma((levels_out,)),
            dma, dma, dma,
        ],
        compiler_params=pltpu.CompilerParams(collective_id=0, has_side_effects=True, vmem_limit_bytes=67043328),
    )(
        values_in, gate_in, key_proj, query_proj, step_size.T, log_decay.T, level_table.transpose(2, 0, 1),
        level_pick.reshape(1, tok), doc_start, skip_weight,
    )
    return pl.pallas_call(
        functools.partial(finish_kernel, ch * ny),
        name="finish",
        out_shape=jax.ShapeDtypeStruct((tok, ch), bf),
        in_specs=[hbm] * 3,
        out_specs=hbm,
        scratch_shapes=[V((tok, ch), bf), V((tok, ch), bf), V((1, tok), f32), V((1, ch), f32), dma((2,)), dma((8,)), dma((8,))],
        compiler_params=pltpu.CompilerParams(vmem_limit_bytes=67043328),
    )(gated, squares, norm_gain.reshape(1, ch))


def solution(mesh):
    split = Mesh(
        mesh.devices.reshape(4, 16, 2, mesh.shape["head"]), ("seq_0", "seq_1", "seq_2", "head")
    )
    return on_mesh(split)


def on_mesh(split):
    placed = (
        P(SEQ, "head"),
        P(SEQ, "head"),
        P(SEQ, None),
        P(SEQ, None),
        P(SEQ, "head"),
        P(SEQ, "head"),
        P("head"),
        P("head"),
        P(None, "head", None),
        P(SEQ),
        P(SEQ),
    )
    return jax.shard_map(local, mesh=split, in_specs=placed, out_specs=P(SEQ, "head"), check_vma=False)
```
